32 devices in a mesh: rep: 1 (over z), kv: 32 (over y, x, core).
Axes of the slice: x: 4, y: 4, z: 1, core: 2. Of those that a mesh axis runs over, the one named last changes fastest.
The devices are a block of a 4x4x8 slice.
Arguments:
- embeds: bfloat16 [2, 128, 2048], P(None, ('rep', 'kv'))
- w_query: bfloat16 [2, 2048, 2048], replicated
- w_key: bfloat16 [2, 2048, 2048], replicated
- w_value: bfloat16 [2, 2048, 2048], replicated
- w_out: bfloat16 [2, 2048, 2048], replicated
- w_up: bfloat16 [2, 2048, 8192], replicated
- w_down: bfloat16 [2, 8192, 2048], replicated
- k_pool: bfloat16 [2304, 2, 16, 16, 128], P(('rep', 'kv'))
- v_pool: bfloat16 [2304, 2, 16, 16, 128], P(('rep', 'kv'))
- old_table: int32 [128, 12], P('rep')
- new_table: int32 [128, 12], P('rep')
- seq_len: int32 [128], P('rep')
- finished: int32 [128], P('rep')
- mig_src: int32 [768], P('rep')
- mig_dst: int32 [768], P('rep')
Outputs:
- output 1: bfloat16 [2, 128, 2048], P(None, ('rep', 'kv'))
- output 2: bfloat16 [2304, 2, 16, 16, 128], P(('rep', 'kv'))
- output 3: bfloat16 [2304, 2, 16, 16, 128], P(('rep', 'kv'))
All inputs are finite; a program needn't handle non-finite values.
Results may differ from the reference program's by a relative error of at most 0.0188525.
Values are sent between devices in bfloat16 or wider.
A program may use at most 768 MiB of HBM per device.

```python
import jax
import jax.numpy as jnp
from jax import lax

D_MODEL = 2048
Q_HEADS = 16
KV_HEADS = 16
HEAD_DIM = 128
FF_DIM = 8192
PAGE_SIZE = 16
SEQ_DEV = 4
PAGES_SEQ = 12
PAIR_CAP = 3
GROUP_DEVS = 32
N_LAYERS = 2

Q_WIDTH = Q_HEADS * HEAD_DIM
KV_WIDTH = KV_HEADS * HEAD_DIM
HALF_DEVS = GROUP_DEVS // 2
N_BATCH = GROUP_DEVS * SEQ_DEV
DONE_SEQS = N_BATCH // 4
SLOTS_DEV = 3 * SEQ_DEV * PAGES_SEQ // 2
TOTAL_SLOTS = GROUP_DEVS * SLOTS_DEV
COLD_PAGES = PAGES_SEQ // 4
HOT_PAGES = PAGES_SEQ - COLD_PAGES
PER_DEV = N_BATCH // HALF_DEVS
DONE_PER = DONE_SEQS // HALF_DEVS
ACTIVE_PER = PER_DEV - DONE_PER
DONE_COLD = COLD_PAGES * DONE_PER
N_MIG = HALF_DEVS * HALF_DEVS * PAIR_CAP
CONTEXT = PAGES_SEQ * PAGE_SIZE


def slot_order(one_key):
    return jax.random.permutation(one_key, SLOTS_DEV)


def draw_layout(layout_key):
    key_list = jax.random.split(layout_key, 5)
    dev_perm = jax.random.permutation(key_list[0], GROUP_DEVS)
    seq_perm = jax.random.permutation(key_list[1], N_BATCH)
    slot_perm = jax.vmap(slot_order)(jax.random.split(key_list[2], GROUP_DEVS))
    entry_perm = jax.random.permutation(key_list[3], N_MIG)
    hot_devs = dev_perm[:HALF_DEVS]
    cold_devs = dev_perm[HALF_DEVS:]
    seq_ids = jnp.arange(N_BATCH)[:, None]
    page_ids = jnp.arange(PAGES_SEQ)[None, :]
    is_cold = page_ids < COLD_PAGES
    page_level = jnp.where(is_cold, page_ids, page_ids - COLD_PAGES)
    dev_pos = (seq_ids + page_level) % HALF_DEVS
    device = jnp.where(is_cold, cold_devs[dev_pos], hot_devs[dev_pos])
    slot_rank = page_level * PER_DEV + seq_ids // HALF_DEVS
    slot_ids = device * SLOTS_DEV + slot_perm[device, slot_rank]
    entry_ids = jnp.arange(N_MIG)
    src_pos = entry_ids // (HALF_DEVS * PAIR_CAP)
    dst_pos = (entry_ids // PAIR_CAP) % HALF_DEVS
    within = entry_ids % PAIR_CAP
    src_rank = dst_pos * PAIR_CAP + within
    dst_rank = src_pos * PAIR_CAP + within
    hot_level = HOT_PAGES - 1 - src_rank // ACTIVE_PER
    src_seq = DONE_SEQS + (src_pos - hot_level) % HALF_DEVS + HALF_DEVS * (src_rank % ACTIVE_PER)
    src_page = COLD_PAGES + hot_level
    src_slot = slot_ids[src_seq, src_page]
    cold_level = jnp.minimum(dst_rank // DONE_PER, COLD_PAGES - 1)
    done_seq = (dst_pos - cold_level) % HALF_DEVS + HALF_DEVS * (dst_rank % DONE_PER)
    reuse_slot = slot_ids[done_seq, cold_level]
    cold_dev = cold_devs[dst_pos]
    free_rank = jnp.clip(COLD_PAGES * PER_DEV + dst_rank - DONE_COLD, 0, SLOTS_DEV - 1)
    free_slot = cold_dev * SLOTS_DEV + slot_perm[cold_dev, free_rank]
    dst_slot = jnp.where(dst_rank < DONE_COLD, reuse_slot, free_slot)
    new_ids = slot_ids.at[src_seq, src_page].set(dst_slot)
    done_flag = (jnp.arange(N_BATCH) < DONE_SEQS).astype(jnp.int32)
    seq_len = jax.random.randint(key_list[4], (N_BATCH,), (PAGES_SEQ - 1) * PAGE_SIZE, CONTEXT - 1)
    seq_len = seq_len.at[seq_perm[N_BATCH - 1]].set(CONTEXT - 2)
    seq_len = seq_len.at[seq_perm[N_BATCH - 2]].set((PAGES_SEQ - 1) * PAGE_SIZE)
    blank_table = jnp.zeros((N_BATCH, PAGES_SEQ), jnp.int32)
    return {
        'old_table': blank_table.at[seq_perm].set(slot_ids.astype(jnp.int32)),
        'new_table': blank_table.at[seq_perm].set(new_ids.astype(jnp.int32)),
        'seq_len': seq_len.astype(jnp.int32),
        'finished': jnp.zeros((N_BATCH,), jnp.int32).at[seq_perm].set(done_flag),
        'mig_src': jnp.zeros((N_MIG,), jnp.int32).at[entry_perm].set(src_slot.astype(jnp.int32)),
        'mig_dst': jnp.zeros((N_MIG,), jnp.int32).at[entry_perm].set(dst_slot.astype(jnp.int32)),
    }


def draw_weight(one_key, fan_in, fan_out, gain):
    values = jax.random.normal(one_key, (N_LAYERS, fan_in, fan_out), jnp.float32)
    return (values * (gain * fan_in ** -0.5)).astype(jnp.bfloat16)


def setup_inputs(seed: int = 0, part: int = 0) -> dict:
    shared = jax.random.split(jax.random.key(seed), 6)
    part_keys = jax.random.split(jax.random.fold_in(jax.random.key(seed + 1), part), 5)
    layout = draw_layout(part_keys[0])
    pool_shape = (TOTAL_SLOTS, N_LAYERS, PAGE_SIZE, KV_HEADS, HEAD_DIM)
    page_mean = jax.random.normal(part_keys[3], (TOTAL_SLOTS, N_LAYERS, 1, KV_HEADS, HEAD_DIM), jnp.float32)
    v_noise = jax.random.normal(part_keys[4], pool_shape, jnp.float32)
    return {
        'embeds': jax.random.normal(part_keys[1], (2, N_BATCH, D_MODEL), jnp.float32).astype(jnp.bfloat16),
        'w_query': draw_weight(shared[0], D_MODEL, Q_WIDTH, 1.0),
        'w_key': draw_weight(shared[1], D_MODEL, KV_WIDTH, 1.0),
        'w_value': draw_weight(shared[2], D_MODEL, KV_WIDTH, 1.0),
        'w_out': draw_weight(shared[3], Q_WIDTH, D_MODEL, (0.5 * PAGES_SEQ) ** 0.5),
        'w_up': draw_weight(shared[4], D_MODEL, FF_DIM, 1.0),
        'w_down': draw_weight(shared[5], FF_DIM, D_MODEL, 1.0),
        'k_pool': jax.random.normal(part_keys[2], pool_shape, jnp.float32).astype(jnp.bfloat16),
        'v_pool': (page_mean + 0.5 * v_noise).astype(jnp.bfloat16),
        'old_table': layout['old_table'],
        'new_table': layout['new_table'],
        'seq_len': layout['seq_len'],
        'finished': layout['finished'],
        'mig_src': layout['mig_src'],
        'mig_dst': layout['mig_dst'],
    }


def project(hidden, w_mat):
    return jnp.dot(hidden, w_mat, preferred_element_type=jnp.float32).astype(jnp.bfloat16)


def attend(query_rows, k_layer, v_layer, table, lengths):
    def one_seq(operands):
        q_row, table_row, length = operands
        page_keys = k_layer[table_row].astype(jnp.float32).reshape(CONTEXT, KV_HEADS, HEAD_DIM)
        page_vals = v_layer[table_row].astype(jnp.float32).reshape(CONTEXT, KV_HEADS, HEAD_DIM)
        q_grouped = q_row.astype(jnp.float32).reshape(KV_HEADS, Q_HEADS // KV_HEADS, HEAD_DIM)
        scores = jnp.einsum('grd,tgd->grt', q_grouped, page_keys) * (HEAD_DIM ** -0.5)
        valid_pos = jnp.arange(CONTEXT) <= length
        scores = jnp.where(valid_pos, scores, -jnp.inf)
        weights = jax.nn.softmax(scores, axis=-1)
        mixed = jnp.einsum('grt,tgd->grd', weights, page_vals)
        return mixed.reshape(Q_WIDTH).astype(jnp.bfloat16)
    return lax.map(one_seq, (query_rows, table, lengths))


def finish_block(hidden, attn_rows, w_out, w_up, w_down):
    mixed_rows = (hidden.astype(jnp.float32) + jnp.dot(attn_rows, w_out, preferred_element_type=jnp.float32)).astype(jnp.bfloat16)
    inner_act = jax.nn.gelu(jnp.dot(mixed_rows, w_up, preferred_element_type=jnp.float32)).astype(jnp.bfloat16)
    return (mixed_rows.astype(jnp.float32) + jnp.dot(inner_act, w_down, preferred_element_type=jnp.float32)).astype(jnp.bfloat16)


def reference(embeds, w_query, w_key, w_value, w_out, w_up, w_down, k_pool, v_pool, old_table, new_table, seq_len, finished, mig_src, mig_dst):
    seq_ids = jnp.arange(N_BATCH)
    active = finished == 0
    len_next = seq_len + 1
    slot_zero = old_table[seq_ids, seq_len // PAGE_SIZE]
    slot_one = jnp.where(active, new_table[seq_ids, len_next // PAGE_SIZE], TOTAL_SLOTS)
    hid_zero = embeds[0]
    hid_one = embeds[1]
    k_layers = []
    v_layers = []
    for layer_idx in range(N_LAYERS):
        k_layer = k_pool[:, layer_idx]
        v_layer = v_pool[:, layer_idx]
        query_rows = project(hid_zero, w_query[layer_idx])
        k_new = project(hid_zero, w_key[layer_idx]).reshape(N_BATCH, KV_HEADS, HEAD_DIM)
        v_new = project(hid_zero, w_value[layer_idx]).reshape(N_BATCH, KV_HEADS, HEAD_DIM)
        k_layer = k_layer.at[slot_zero, seq_len % PAGE_SIZE].set(k_new)
        v_layer = v_layer.at[slot_zero, seq_len % PAGE_SIZE].set(v_new)
        attn_rows = attend(query_rows, k_layer, v_layer, old_table, seq_len)
        hid_zero = finish_block(hid_zero, attn_rows, w_out[layer_idx], w_up[layer_idx], w_down[layer_idx])
        k_layer = k_layer.at[mig_dst].set(k_layer[mig_src])
        v_layer = v_layer.at[mig_dst].set(v_layer[mig_src])
        query_rows = project(hid_one, w_query[layer_idx])
        k_new = project(hid_one, w_key[layer_idx]).reshape(N_BATCH, KV_HEADS, HEAD_DIM)
        v_new = project(hid_one, w_value[layer_idx]).reshape(N_BATCH, KV_HEADS, HEAD_DIM)
        k_layer = k_layer.at[slot_one, len_next % PAGE_SIZE].set(k_new, mode='drop')
        v_layer = v_layer.at[slot_one, len_next % PAGE_SIZE].set(v_new, mode='drop')
        attn_rows = attend(query_rows, k_layer, v_layer, new_table, len_next)
        hid_one = finish_block(hid_one, attn_rows, w_out[layer_idx], w_up[layer_idx], w_down[layer_idx])
        k_layers.append(k_layer)
        v_layers.append(v_layer)
    hid_one = jnp.where(active[:, None], hid_one, jnp.zeros_like(hid_one))
    return jnp.stack([hid_zero, hid_one]), jnp.stack(k_layers, axis=1), jnp.stack(v_layers, axis=1)
```

```python
import functools

import jax
import jax.numpy as jnp
from jax import lax
from jax.experimental import pallas as pl
from jax.experimental.pallas import tpu as pltpu
from jax.sharding import PartitionSpec as P

MESH = pl.DeviceIdType.MESH
ANY = pl.BlockSpec(memory_space=pl.ANY)
VMEM = pl.BlockSpec(memory_space=pltpu.VMEM)
SMEM = pl.BlockSpec(memory_space=pltpu.SMEM)
LOW = -1e30


def ring(count, depth, lead, start_in, wait_in, middle, start_out, wait_out):
    def body(i, carry):
        @pl.when(i < count)
        def _():
            @pl.when(i >= depth)
            def _():
                wait_out(i - depth)

            start_in(i)

        @pl.when(i >= lead)
        def _():
            wait_in(i - lead)
            middle(i - lead)
            start_out(i - lead)

        return carry

    lax.fori_loop(0, count + lead, body, 0)

    def drain(i, carry):
        wait_out(i)
        return carry

    lax.fori_loop(jnp.maximum(count - depth, 0), count, drain, 0)


def compact(total, flag, value, listed):
    def body(i, count):
        @pl.when(flag(i))
        def _():
            listed[count] = value(i)

        return count + flag(i).astype(jnp.int32)

    return lax.fori_loop(0, total, body, jnp.int32(0))


def pack_kernel(depth, lead, slot_ref, k_ref, v_ref, *rest):
    outs, (buf, listed, sems_in, sems_out) = rest[:-4], rest[-4:]
    peers = slot_ref.shape[0] // len(outs)
    for r, out in enumerate(outs):
        count = compact(peers, lambda i: slot_ref[r * peers + i] >= 0, lambda i: i, listed)

        def ins(i):
            at = lax.rem(i, depth)
            slot = slot_ref[r * peers + listed[i]]
            return [pltpu.make_async_copy(ref.at[slot], buf.at[at, h], sems_in.at[at, h]) for h, ref in enumerate((k_ref, v_ref))]

        def put(i):
            at = lax.rem(i, depth)
            return pltpu.make_async_copy(buf.at[at], out.at[listed[i]], sems_out.at[at])

        ring(
            count, depth, lead,
            lambda i: [c.start() for c in ins(i)],
            lambda i: [c.wait() for c in ins(i)],
            lambda i: None,
            lambda i: put(i).start(),
            lambda i: put(i).wait(),
        )


def pack_pages(send_slot, k_pool, v_pool, rounds, peers):
    page = k_pool.shape[1:]
    depth, lead = 16, 8
    return pl.pallas_call(
        functools.partial(pack_kernel, depth, lead),
        out_shape=[jax.ShapeDtypeStruct((peers, 2) + page, k_pool.dtype)] * rounds,
        in_specs=[SMEM, ANY, ANY],
        out_specs=[ANY] * rounds,
        scratch_shapes=[
            pltpu.VMEM((depth, 2) + page, k_pool.dtype),
            pltpu.SMEM((peers,), jnp.int32),
            pltpu.SemaphoreType.DMA((depth, 2)),
            pltpu.SemaphoreType.DMA((depth,)),
        ],
        name="pack_pages",
    )(send_slot, k_pool, v_pool)


def patch_rows(buf, at, slot, first_ref, second_ref, offset_ref, rows):
    seq_dev = rows[0].shape[2]
    for step, ref in enumerate((first_ref, second_ref)):
        seq = ref[slot]

        @pl.when(seq >= 0)
        def _():
            offset = offset_ref[seq] + step
            home, place = seq // seq_dev, lax.rem(seq, seq_dev)
            for layer, row in enumerate(rows):
                for h in range(2):
                    buf[at, h, layer, offset] = row[home, h, place, step]


def keep_kernel(depth, lead, from_ref, first_ref, second_ref, offset_ref, k_ref, v_ref, *rest):
    n_layers = k_ref.shape[1]
    rows = rest[:n_layers]
    k_out, v_out, buf, listed, sems_in, sems_out = rest[n_layers:]
    count = compact(from_ref.shape[0], lambda i: from_ref[i] < 0, lambda i: i, listed)

    def ins(i):
        at = lax.rem(i, depth)
        return [pltpu.make_async_copy(ref.at[listed[i]], buf.at[at, h], sems_in.at[at, h]) for h, ref in enumerate((k_ref, v_ref))]

    def outs(i):
        at = lax.rem(i, depth)
        return [pltpu.make_async_copy(buf.at[at, h], ref.at[listed[i]], sems_out.at[at, h]) for h, ref in enumerate((k_out, v_out))]

    ring(
        count, depth, lead,
        lambda i: [c.start() for c in ins(i)],
        lambda i: [c.wait() for c in ins(i)],
        lambda i: patch_rows(buf, lax.rem(i, depth), listed[i], first_ref, second_ref, offset_ref, rows),
        lambda i: [c.start() for c in outs(i)],
        lambda i: [c.wait() for c in outs(i)],
    )


def keep_pages(from_page, first_seq, second_seq, offsets, k_pool, v_pool, rows):
    depth, lead = 16, 8
    return pl.pallas_call(
        functools.partial(keep_kernel, depth, lead),
        out_shape=[jax.ShapeDtypeStruct(k_pool.shape, k_pool.dtype)] * 2,
        in_specs=[SMEM] * 4 + [ANY] * 2 + [VMEM] * len(rows),
        out_specs=[ANY] * 2,
        scratch_shapes=[
            pltpu.VMEM((depth, 2) + k_pool.shape[1:], k_pool.dtype),
            pltpu.SMEM((k_pool.shape[0],), jnp.int32),
            pltpu.SemaphoreType.DMA((depth, 2)),
            pltpu.SemaphoreType.DMA((depth, 2)),
        ],
        name="keep_pages",
    )(from_page, first_seq, second_seq, offsets, k_pool, v_pool, *rows)


def place_kernel(depth, lead, n_layers, rounds, from_ref, first_ref, second_ref, offset_ref, *rest):
    arrived = rest[:rounds]
    rows = rest[rounds:rounds + n_layers]
    k_out, v_out, buf, listed, sems_in, sems_out = rest[rounds + n_layers + 2:]
    peers = arrived[0].shape[0]
    for r in range(rounds):
        count = compact(
            from_ref.shape[0],
            lambda i: (from_ref[i] >= r * peers) & (from_ref[i] < (r + 1) * peers),
            lambda i: i,
            listed,
        )

        def take(i):
            at = lax.rem(i, depth)
            return pltpu.make_async_copy(arrived[r].at[from_ref[listed[i]] - r * peers], buf.at[at], sems_in.at[at])

        def outs(i):
            at = lax.rem(i, depth)
            return [pltpu.make_async_copy(buf.at[at, h], ref.at[listed[i]], sems_out.at[at, h]) for h, ref in enumerate((k_out, v_out))]

        ring(
            count, depth, lead,
            lambda i: take(i).start(),
            lambda i: take(i).wait(),
            lambda i: patch_rows(buf, lax.rem(i, depth), listed[i], first_ref, second_ref, offset_ref, rows),
            lambda i: [c.start() for c in outs(i)],
            lambda i: [c.wait() for c in outs(i)],
        )


def place_pages(from_page, first_seq, second_seq, offsets, arrived, rows, k_out, v_out):
    depth, lead = 16, 8
    rounds, n_layers = len(arrived), len(rows)
    first_pool = 4 + rounds + n_layers
    return pl.pallas_call(
        functools.partial(place_kernel, depth, lead, n_layers, rounds),
        out_shape=[jax.ShapeDtypeStruct(k_out.shape, k_out.dtype)] * 2,
        in_specs=[SMEM] * 4 + [ANY] * rounds + [VMEM] * n_layers + [ANY] * 2,
        out_specs=[ANY] * 2,
        scratch_shapes=[
            pltpu.VMEM((depth, 2) + k_out.shape[1:], k_out.dtype),
            pltpu.SMEM((k_out.shape[0],), jnp.int32),
            pltpu.SemaphoreType.DMA((depth,)),
            pltpu.SemaphoreType.DMA((depth, 2)),
        ],
        input_output_aliases={first_pool: 0, first_pool + 1: 1},
        name="place_pages",
    )(from_page, first_seq, second_seq, offsets, *arrived, *rows, k_out, v_out)


def attend_kernel(block, pages_seq, seq_dev, page_size, scale, code_ref, q_ref, k_ref, v_ref, acc_ref):
    rows, head_dim = q_ref.shape[-2:]
    heads = k_ref.shape[3]
    step = pl.program_id(0)

    @pl.when(step == 0)
    def _():
        acc_ref[:, :seq_dev] = jnp.zeros((acc_ref.shape[0], seq_dev, rows, head_dim), jnp.float32)
        lane = lax.broadcasted_iota(jnp.int32, (acc_ref.shape[0], 1, rows, head_dim), 3)
        acc_ref[:, seq_dev:] = jnp.where(lax.rem(lane, 2) == 0, LOW, 0.0)

    row = lax.broadcasted_iota(jnp.int32, (rows, page_size * heads), 0)
    column = lax.broadcasted_iota(jnp.int32, (rows, page_size * heads), 1)
    same_head = lax.rem(row, heads) == lax.rem(column, heads)
    position = column // heads
    lane = lax.broadcasted_iota(jnp.int32, (rows, head_dim), 1)
    for s in range(block):
        code = code_ref[step * block + s]

        @pl.when(code >= 0)
        def _():
            seen = lax.rem(code, 2 * page_size)
            seq = code // (2 * page_size * pages_seq)
            home, place = seq // seq_dev, lax.rem(seq, seq_dev)
            q = q_ref[lax.rem(home, 2), home // 2, place]
            keys = k_ref[s, 0].reshape(page_size * heads, head_dim)
            values = v_ref[s, 0].reshape(page_size * heads, head_dim)
            scores = lax.dot_general(q, keys, (((1,), (1,)), ((), ())), preferred_element_type=jnp.float32) * scale
            mask = same_head & (position < seen)
            scores = jnp.where(mask, scores, LOW)
            top = jnp.max(scores, axis=1, keepdims=True)
            stats = acc_ref[home, seq_dev]
            old_top = jnp.max(jnp.where(lane == 2 * place, stats, LOW), axis=1, keepdims=True)
            old_sum = jnp.sum(jnp.where(lane == 2 * place + 1, stats, 0.0), axis=1, keepdims=True)
            new_top = jnp.maximum(top, old_top)
            weights = jnp.where(mask, jnp.exp(scores - new_top), 0.0)
            factor = jnp.exp(old_top - new_top)
            new_sum = old_sum * factor + jnp.sum(weights, axis=1, keepdims=True)
            high = weights.astype(jnp.bfloat16)
            low = (weights - high.astype(jnp.float32)).astype(jnp.bfloat16)
            mixed = jnp.dot(high, values, preferred_element_type=jnp.float32) + jnp.dot(low, values, preferred_element_type=jnp.float32)
            acc_ref[home, place] = acc_ref[home, place] * factor + mixed
            acc_ref[home, seq_dev] = jnp.where(lane == 2 * place, new_top, jnp.where(lane == 2 * place + 1, new_sum, stats))


def attend_pages(code, q_all, k_pool, v_pool, layer, pages_seq, seq_dev):
    slots, _, page_size, heads, head_dim = k_pool.shape
    rows = q_all.shape[-2]
    groups = q_all.shape[0] * q_all.shape[1]
    block = 8
    page_spec = pl.BlockSpec((block, 1, page_size, heads, head_dim), lambda i, c: (i, layer, 0, 0, 0))
    acc_shape = (groups, seq_dev + 1, rows, head_dim)
    return pl.pallas_call(
        functools.partial(attend_kernel, block, pages_seq, seq_dev, page_size, head_dim ** -0.5),
        out_shape=jax.ShapeDtypeStruct(acc_shape, jnp.float32),
        grid_spec=pltpu.PrefetchScalarGridSpec(
            num_scalar_prefetch=1,
            grid=(slots // block,),
            in_specs=[pl.BlockSpec(q_all.shape, lambda i, c: (0,) * q_all.ndim), page_spec, page_spec],
            out_specs=pl.BlockSpec(acc_shape, lambda i, c: (0, 0, 0, 0)),
        ),
        compiler_params=pltpu.CompilerParams(dimension_semantics=("arbitrary",)),
        cost_estimate=pl.CostEstimate(flops=4 * 10 ** 8, bytes_accessed=2 * slots * page_size * heads * head_dim * 2, transcendentals=0),
        name="attend_pages",
    )(code, q_all, k_pool, v_pool)


def spread_kernel(n, x_ref, out_ref, held, send_sem, recv_sem, pass_sem, got_sem, copy_sem):
    me = lax.axis_index("kv")
    chips = n // 2
    core, chip = lax.rem(me, 2), me // 2
    other = me + 1 - 2 * core

    def peer(j):
        return 2 * lax.rem(chip + j, chips) + core

    barrier = pltpu.get_barrier_semaphore()

    def greet(j, carry):
        pl.semaphore_signal(barrier, inc=1, device_id={"kv": peer(j)}, device_id_type=MESH)
        return carry

    lax.fori_loop(1, chips, greet, 0)
    pl.semaphore_signal(barrier, inc=1, device_id={"kv": other}, device_id_type=MESH)
    pl.semaphore_wait(barrier, chips)

    def send(j):
        return pltpu.make_async_remote_copy(
            src_ref=x_ref, dst_ref=held.at[core, chip], send_sem=send_sem.at[j], recv_sem=recv_sem.at[chip],
            device_id={"kv": peer(j)}, device_id_type=MESH,
        )

    def forward(source, at):
        return pltpu.make_async_remote_copy(
            src_ref=source, dst_ref=held.at[core, at], send_sem=pass_sem.at[at], recv_sem=got_sem.at[at],
            device_id={"kv": other}, device_id_type=MESH,
        )

    def start(j, carry):
        send(j).start()
        return carry

    lax.fori_loop(1, chips, start, 0)
    own = forward(x_ref, chip)
    own.start()
    mine = pltpu.make_async_copy(x_ref, out_ref.at[core, chip], copy_sem.at[0])
    mine.start()

    def arrive(j, carry):
        at = lax.rem(chip + chips - j, chips)
        pltpu.make_async_remote_copy(
            src_ref=x_ref, dst_ref=held.at[core, at], send_sem=send_sem.at[j], recv_sem=recv_sem.at[at],
            device_id={"kv": other}, device_id_type=MESH,
        ).wait_recv()
        forward(held.at[core, at], at).start()
        pltpu.make_async_copy(held.at[core, at], out_ref.at[core, at], copy_sem.at[j]).start()
        return carry

    lax.fori_loop(1, chips, arrive, 0)

    def passed(j, carry):
        at = lax.rem(chip + j, chips)
        pltpu.make_async_remote_copy(
            src_ref=x_ref, dst_ref=held.at[1 - core, at], send_sem=pass_sem.at[at], recv_sem=got_sem.at[at],
            device_id={"kv": other}, device_id_type=MESH,
        ).wait_recv()
        pltpu.make_async_copy(held.at[1 - core, at], out_ref.at[1 - core, at], copy_sem.at[chips + j]).start()
        return carry

    lax.fori_loop(0, chips, passed, 0)

    own.wait_send()
    mine.wait()

    def finish(j, carry):
        at = lax.rem(chip + chips - j, chips)
        send(j).wait_send()
        forward(held.at[core, at], at).wait_send()
        pltpu.make_async_copy(held.at[core, at], out_ref.at[core, at], copy_sem.at[j]).wait()
        return carry

    lax.fori_loop(1, chips, finish, 0)

    def written(j, carry):
        at = lax.rem(chip + j, chips)
        pltpu.make_async_copy(held.at[1 - core, at], out_ref.at[1 - core, at], copy_sem.at[chips + j]).wait()
        return carry

    lax.fori_loop(0, chips, written, 0)


def spread(x, n):
    chips = n // 2
    return pl.pallas_call(
        functools.partial(spread_kernel, n),
        out_shape=jax.ShapeDtypeStruct((2, chips) + x.shape, x.dtype),
        in_specs=[VMEM],
        out_specs=ANY,
        scratch_shapes=[
            pltpu.VMEM((2, chips) + x.shape, x.dtype),
            pltpu.SemaphoreType.DMA((chips,)),
            pltpu.SemaphoreType.DMA((chips,)),
            pltpu.SemaphoreType.DMA((chips,)),
            pltpu.SemaphoreType.DMA((chips,)),
            pltpu.SemaphoreType.DMA((n,)),
        ],
        compiler_params=pltpu.CompilerParams(collective_id=0, has_side_effects=True),
        name="spread_queries",
    )(x)


def gather_home_kernel(n, scale, acc_ref, q_ref, k_ref, v_ref, o_ref, held, send_sem, recv_sem):
    me = lax.axis_index("kv")
    seq_dev, rows, head_dim = q_ref.shape
    heads = k_ref.shape[2]

    def peer(j):
        return lax.rem(me + j, n)

    barrier = pltpu.get_barrier_semaphore()

    def greet(j, carry):
        pl.semaphore_signal(barrier, inc=1, device_id={"kv": peer(j)}, device_id_type=MESH)
        return carry

    lax.fori_loop(1, n, greet, 0)
    pl.semaphore_wait(barrier, n - 1)

    def send(j):
        return pltpu.make_async_remote_copy(
            src_ref=acc_ref.at[peer(j)], dst_ref=held.at[me], send_sem=send_sem.at[j], recv_sem=recv_sem.at[me],
            device_id={"kv": peer(j)}, device_id_type=MESH,
        )

    def start(j, carry):
        send(j).start()
        return carry

    lax.fori_loop(1, n, start, 0)
    held[me] = acc_ref[me]

    queries = [q_ref[i].astype(jnp.float32) for i in range(seq_dev)]
    second_row = lax.broadcasted_iota(jnp.int32, (rows, 1), 0) >= heads

    def twice(x):
        x = x.astype(jnp.float32)
        return jnp.concatenate([x, x], axis=0)

    first = [jnp.sum(queries[i] * twice(k_ref[i, 0]), axis=1, keepdims=True) * scale for i in range(seq_dev)]
    second = [
        jnp.where(second_row, jnp.sum(queries[i] * twice(k_ref[i, 1]), axis=1, keepdims=True) * scale, LOW)
        for i in range(seq_dev)
    ]

    def arrive(j, carry):
        at = lax.rem(me + n - j, n)
        pltpu.make_async_remote_copy(
            src_ref=acc_ref.at[at], dst_ref=held.at[at], send_sem=send_sem.at[j], recv_sem=recv_sem.at[at],
            device_id={"kv": peer(j)}, device_id_type=MESH,
        ).wait_recv()
        return carry

    lax.fori_loop(1, n, arrive, 0)

    def highest(j, top):
        return jnp.maximum(top, held[j, seq_dev])

    top_all = lax.fori_loop(0, n, highest, jnp.full((rows, head_dim), LOW, jnp.float32))
    tops, sums, mixed = [], [], []
    for i in range(seq_dev):
        top = jnp.maximum(jnp.maximum(top_all[:, 2 * i:2 * i + 1], first[i]), second[i])
        p_first, p_second = jnp.exp(first[i] - top), jnp.exp(second[i] - top)
        tops.append(top)
        sums.append(p_first + p_second)
        mixed.append(p_first * twice(v_ref[i, 0]) + p_second * twice(v_ref[i, 1]))

    def merge(j, carry):
        sums, mixed = carry
        stats = held[j, seq_dev]
        new_sums, new_mixed = [], []
        for i in range(seq_dev):
            weight = jnp.exp(stats[:, 2 * i:2 * i + 1] - tops[i])
            new_sums.append(sums[i] + weight * stats[:, 2 * i + 1:2 * i + 2])
            new_mixed.append(mixed[i] + weight * held[j, i])
        return tuple(new_sums), tuple(new_mixed)

    sums, mixed = lax.fori_loop(0, n, merge, (tuple(sums), tuple(mixed)))
    for i in range(seq_dev):
        o_ref[i] = (mixed[i] / sums[i]).astype(o_ref.dtype)

    def finish(j, carry):
        send(j).wait_send()
        return carry

    lax.fori_loop(1, n, finish, 0)


def gather_home(acc, q, k_new, v_new, n):
    return pl.pallas_call(
        functools.partial(gather_home_kernel, n, q.shape[-1] ** -0.5),
        out_shape=jax.ShapeDtypeStruct(q.shape, jnp.bfloat16),
        in_specs=[VMEM] * 4,
        out_specs=VMEM,
        scratch_shapes=[
            pltpu.VMEM(acc.shape, acc.dtype),
            pltpu.SemaphoreType.DMA((n,)),
            pltpu.SemaphoreType.DMA((n,)),
        ],
        compiler_params=pltpu.CompilerParams(collective_id=1, has_side_effects=True),
        name="gather_home",
    )(acc, q, k_new, v_new)


def solution(mesh):
    groups = mesh.shape['kv']
    rows_spec = P(None, ('rep', 'kv'), None)
    pool_spec = P(('rep', 'kv'))
    table_spec = P('rep', None)
    vec_spec = P('rep')
    full_spec = P()

    def device_fn(embeds, w_query, w_key, w_value, w_out, w_up, w_down, k_pool, v_pool, old_table, new_table, seq_len, finished, mig_src, mig_dst):
        me = lax.axis_index('kv')
        slots, n_layers, page_size, heads, head_dim = k_pool.shape
        steps, seq_dev, width = embeds.shape
        n_batch, pages_seq = old_table.shape
        n_mig = mig_src.shape[0]
        rounds = 4 * n_mig // (groups * groups)
        base = me * slots
        local = jnp.arange(slots, dtype=jnp.int32)
        active = finished == 0
        last = pages_seq - 1

        def find(match, value):
            return jnp.max(jnp.where(match, value, -1), axis=1)

        flat = old_table.reshape(-1)
        place = jnp.arange(n_batch * pages_seq, dtype=jnp.int32)
        seen = jnp.clip(seq_len[:, None] - jnp.arange(pages_seq, dtype=jnp.int32)[None, :] * page_size, 0, page_size).reshape(-1)
        code = find(flat[None, :] - base == local[:, None], (place * (2 * page_size) + seen)[None, :])

        src_dev, dst_dev = mig_src // slots, mig_dst // slots
        pair = src_dev * groups + dst_dev
        entry = jnp.arange(n_mig, dtype=jnp.int32)
        rank = jnp.sum((pair[None, :] == pair[:, None]) & (entry[None, :] < entry[:, None]), axis=1, dtype=jnp.int32)
        lines = jnp.arange(rounds * groups, dtype=jnp.int32)
        send_slot = find(
            ((rank * groups + dst_dev)[None, :] == lines[:, None]) & (src_dev == me)[None, :], (mig_src - src_dev * slots)[None, :]
        )
        from_page = find((mig_dst - base)[None, :] == local[:, None], (rank * groups + src_dev)[None, :])

        seq_ids = jnp.arange(n_batch, dtype=jnp.int32)
        owner_old = find((old_table[:, last] - base)[None, :] == local[:, None], seq_ids[None, :])
        owner_new = find(((new_table[:, last] - base)[None, :] == local[:, None]) & active[None, :], seq_ids[None, :])
        first_seq = jnp.where(from_page >= 0, owner_new, owner_old)
        second_seq = owner_new
        offsets = lax.rem(seq_len, page_size)

        packed = pack_pages(send_slot, k_pool, v_pool, rounds, groups)

        def exchange(block):
            return lax.all_to_all(block, 'kv', 0, 0, tiled=True)

        hidden = jnp.transpose(embeds, (1, 0, 2)).reshape(seq_dev * steps, width)
        arrived = []
        rows = []
        for layer in range(n_layers):
            query = jnp.dot(hidden, w_query[layer], preferred_element_type=jnp.float32).astype(jnp.bfloat16)
            key = jnp.dot(hidden, w_key[layer], preferred_element_type=jnp.float32).astype(jnp.bfloat16)
            value = jnp.dot(hidden, w_value[layer], preferred_element_type=jnp.float32).astype(jnp.bfloat16)
            query = query.reshape(seq_dev, steps * heads, head_dim)
            key = key.reshape(seq_dev, steps, heads, head_dim)
            value = value.reshape(seq_dev, steps, heads, head_dim)
            q_all = spread(query, groups)
            if layer == 0:
                block, q_all = lax.optimization_barrier((packed[0], q_all))
                arrived.append(exchange(block))
            acc = attend_pages(code, q_all, k_pool, v_pool, layer, pages_seq, seq_dev)
            mixed = gather_home(acc, query, key, value, groups)
            if layer + 1 < rounds:
                block, mixed = lax.optimization_barrier((packed[layer + 1], mixed))
                arrived.append(exchange(block))
            rows.append(lax.all_gather(jnp.stack([key, value])[None], 'kv', axis=0, tiled=True))
            mixed = mixed.reshape(seq_dev * steps, heads * head_dim)
            hidden = (hidden.astype(jnp.float32) + jnp.dot(mixed, w_out[layer], preferred_element_type=jnp.float32)).astype(jnp.bfloat16)
            inner = jax.nn.gelu(jnp.dot(hidden, w_up[layer], preferred_element_type=jnp.float32)).astype(jnp.bfloat16)
            hidden = (hidden.astype(jnp.float32) + jnp.dot(inner, w_down[layer], preferred_element_type=jnp.float32)).astype(jnp.bfloat16)
        for r in range(len(arrived), rounds):
            arrived.append(exchange(packed[r]))
        k_out, v_out = keep_pages(from_page, first_seq, second_seq, offsets, k_pool, v_pool, rows)
        k_out, v_out = place_pages(from_page, first_seq, second_seq, offsets, arrived, rows, k_out, v_out)
        hidden = jnp.transpose(hidden.reshape(seq_dev, steps, width), (1, 0, 2))
        done = lax.dynamic_slice(finished, (me * seq_dev,), (seq_dev,)) != 0
        live = jnp.stack([jnp.ones_like(done), ~done])
        hidden = jnp.where(live[:, :, None], hidden, jnp.zeros_like(hidden))
        return hidden, k_out, v_out

    in_specs = (rows_spec, full_spec, full_spec, full_spec, full_spec, full_spec, full_spec, pool_spec, pool_spec, table_spec, table_spec, vec_spec, vec_spec, vec_spec, vec_spec)
    return jax.shard_map(device_fn, mesh=mesh, in_specs=in_specs, out_specs=(rows_spec, pool_spec, pool_spec), check_vma=False)
```

```python
import functools

import jax
import jax.numpy as jnp
from jax import lax
from jax.experimental import pallas as pl
from jax.experimental.pallas import tpu as pltpu
from jax.sharding import PartitionSpec as P

MESH = pl.DeviceIdType.MESH
ANY = pl.BlockSpec(memory_space=pl.ANY)
VMEM = pl.BlockSpec(memory_space=pltpu.VMEM)
SMEM = pl.BlockSpec(memory_space=pltpu.SMEM)
LOW = -1e30


def ring(count, depth, lead, start_in, wait_in, start_out, wait_out):
    def body(i, carry):
        @pl.when(i < count)
        def _():
            @pl.when(i >= depth)
            def _():
                wait_out(i - depth)

            start_in(i)

        @pl.when(i >= lead)
        def _():
            wait_in(i - lead)
            start_out(i - lead)

        return carry

    lax.fori_loop(0, count + lead, body, 0)

    def drain(i, carry):
        wait_out(i)
        return carry

    lax.fori_loop(jnp.maximum(count - depth, 0), count, drain, 0)


def compact(total, flag, value, listed):
    def body(i, count):
        @pl.when(flag(i))
        def _():
            listed[count] = value(i)

        return count + flag(i).astype(jnp.int32)

    return lax.fori_loop(0, total, body, jnp.int32(0))


def pack_kernel(depth, lead, plan, slot_ref, *rest):
    pools = rest[:2]
    outs = rest[2:-4]
    buf, listed, sems_in, sems_out = rest[-4:]
    peers = outs[0].shape[0]
    for r, halves in plan:
        mine, outs = outs[:len(halves)], outs[len(halves):]
        count = compact(peers, lambda i: slot_ref[r * peers + i] >= 0, lambda i: i, listed)

        def ins(i):
            at = lax.rem(i, depth)
            slot = slot_ref[r * peers + listed[i]]
            return [pltpu.make_async_copy(pools[h].at[slot], buf.at[at, h], sems_in.at[at, h]) for h in halves]

        def puts(i):
            at = lax.rem(i, depth)
            return [pltpu.make_async_copy(buf.at[at, h], out.at[listed[i]], sems_out.at[at, h]) for h, out in zip(halves, mine)]

        ring(
            count, depth, lead,
            lambda i: [c.start() for c in ins(i)],
            lambda i: [c.wait() for c in ins(i)],
            lambda i: [c.start() for c in puts(i)],
            lambda i: [c.wait() for c in puts(i)],
        )


def pack_pages(plan, send_slot, k_pool, v_pool, peers):
    page = k_pool.shape[1:]
    depth, lead = 24, 12
    total = sum(len(halves) for _, halves in plan)
    return pl.pallas_call(
        functools.partial(pack_kernel, depth, lead, plan),
        out_shape=[jax.ShapeDtypeStruct((peers,) + page, k_pool.dtype)] * total,
        in_specs=[SMEM, ANY, ANY],
        out_specs=[ANY] * total,
        scratch_shapes=[
            pltpu.VMEM((depth, 2) + page, k_pool.dtype),
            pltpu.SMEM((peers,), jnp.int32),
            pltpu.SemaphoreType.DMA((depth, 2)),
            pltpu.SemaphoreType.DMA((depth, 2)),
        ],
        cost_estimate=pl.CostEstimate(flops=10 ** 8 * total, bytes_accessed=2 ** 21 * total, transcendentals=0),
        name="pack_pages",
    )(send_slot, k_pool, v_pool)


def keep_kernel(depth, lead, from_ref, k_ref, v_ref, k_out, v_out, buf, listed, sems_in, sems_out):
    count = compact(from_ref.shape[0], lambda i: from_ref[i] < 0, lambda i: i, listed)

    def ins(i):
        at = lax.rem(i, depth)
        return [pltpu.make_async_copy(ref.at[listed[i]], buf.at[at, h], sems_in.at[at, h]) for h, ref in enumerate((k_ref, v_ref))]

    def outs(i):
        at = lax.rem(i, depth)
        return [pltpu.make_async_copy(buf.at[at, h], ref.at[listed[i]], sems_out.at[at, h]) for h, ref in enumerate((k_out, v_out))]

    ring(
        count, depth, lead,
        lambda i: [c.start() for c in ins(i)],
        lambda i: [c.wait() for c in ins(i)],
        lambda i: [c.start() for c in outs(i)],
        lambda i: [c.wait() for c in outs(i)],
    )


def keep_pages(from_page, k_pool, v_pool):
    depth, lead = 24, 12
    return pl.pallas_call(
        functools.partial(keep_kernel, depth, lead),
        out_shape=[jax.ShapeDtypeStruct(k_pool.shape, k_pool.dtype)] * 2,
        in_specs=[SMEM] + [ANY] * 2,
        out_specs=[ANY] * 2,
        scratch_shapes=[
            pltpu.VMEM((depth, 2) + k_pool.shape[1:], k_pool.dtype),
            pltpu.SMEM((k_pool.shape[0],), jnp.int32),
            pltpu.SemaphoreType.DMA((depth, 2)),
            pltpu.SemaphoreType.DMA((depth, 2)),
        ],
        cost_estimate=pl.CostEstimate(flops=10 ** 9, bytes_accessed=2 ** 25, transcendentals=0),
        name="keep_pages",
    )(from_page, k_pool, v_pool)


def place_kernel(depth, lead, plan, seq_dev, n_rows, from_ref, first_ref, second_ref, offset_ref, *rest):
    arrived = rest[:sum(len(halves) for _, halves in plan)]
    rest = rest[len(arrived):]
    rows = rest[:n_rows]
    k_out, v_out, buf, listed, sems_in, sems_out, sem_row = rest[n_rows + 2:]
    pools = (k_out, v_out)
    peers = arrived[0].shape[0]
    slots = from_ref.shape[0]
    heads = k_out.shape[3]

    def row_copies(slot, step, seq, halves):
        home, place = seq // seq_dev, lax.rem(seq, seq_dev)
        return [
            pltpu.make_async_copy(
                x.at[lax.rem(home, 2), home // 2, 1 + h, place, pl.ds(step * heads, heads)],
                pools[h].at[slot, layer, offset_ref[seq] + step],
                sem_row.at[0],
            )
            for layer, x in enumerate(rows) for h in halves
        ]

    def patch(action, halves, chosen):
        def body(slot, carry):
            for step, ref in enumerate((first_ref, second_ref)):
                @pl.when((ref[slot] >= 0) & chosen(slot))
                def _():
                    for c in row_copies(slot, step, ref[slot], halves):
                        action(c)
            return carry
        lax.fori_loop(0, slots, body, 0)

    late = [(r, h) for r, halves in plan for h in halves]

    def is_late(h):
        def chosen(slot):
            hit = jnp.bool_(False)
            for r, g in late:
                if g == h:
                    hit = hit | ((from_ref[slot] >= r * peers) & (from_ref[slot] < (r + 1) * peers))
            return hit
        return chosen

    def is_early(h):
        return lambda slot: jnp.logical_not(is_late(h)(slot))

    if n_rows:
        for h in range(2):
            patch(lambda c: c.start(), (h,), is_early(h))
    for r, halves in plan:
        mine, arrived = arrived[:len(halves)], arrived[len(halves):]
        count = compact(slots, lambda i: (from_ref[i] >= r * peers) & (from_ref[i] < (r + 1) * peers), lambda i: i, listed)

        def ins(i):
            at = lax.rem(i, depth)
            line = from_ref[listed[i]] - r * peers
            return [pltpu.make_async_copy(ref.at[line], buf.at[at, h], sems_in.at[at, h]) for h, ref in zip(halves, mine)]

        def outs(i):
            at = lax.rem(i, depth)
            return [pltpu.make_async_copy(buf.at[at, h], pools[h].at[listed[i]], sems_out.at[at, h]) for h in halves]

        ring(
            count, depth, lead,
            lambda i: [c.start() for c in ins(i)],
            lambda i: [c.wait() for c in ins(i)],
            lambda i: [c.start() for c in outs(i)],
            lambda i: [c.wait() for c in outs(i)],
        )
    if n_rows:
        for h in range(2):
            patch(lambda c: c.start(), (h,), is_late(h))
        patch(lambda c: c.wait(), (0, 1), lambda slot: jnp.bool_(True))


def place_pages(plan, seq_dev, from_page, first_seq, second_seq, offsets, arrived, rows, k_out, v_out):
    depth, lead = 24, 12
    first_pool = 4 + len(arrived) + len(rows)
    return pl.pallas_call(
        functools.partial(place_kernel, depth, lead, plan, seq_dev, len(rows)),
        out_shape=[jax.ShapeDtypeStruct(k_out.shape, k_out.dtype)] * 2,
        in_specs=[SMEM] * 4 + [ANY] * (len(arrived) + len(rows) + 2),
        out_specs=[ANY] * 2,
        scratch_shapes=[
            pltpu.VMEM((depth, 2) + k_out.shape[1:], k_out.dtype),
            pltpu.SMEM((k_out.shape[0],), jnp.int32),
            pltpu.SemaphoreType.DMA((depth, 2)),
            pltpu.SemaphoreType.DMA((depth, 2)),
            pltpu.SemaphoreType.DMA((1,)),
        ],
        input_output_aliases={first_pool: 0, first_pool + 1: 1},
        cost_estimate=pl.CostEstimate(flops=10 ** 8 * len(arrived), bytes_accessed=2 ** 22 * len(arrived), transcendentals=0),
        name="place_pages",
    )(from_page, first_seq, second_seq, offsets, *arrived, *rows, k_out, v_out)


def attend_kernel(block, pages_seq, seq_dev, page_size, scale, code_ref, x_ref, k_ref, v_ref, acc_ref):
    rows, head_dim = x_ref.shape[-2:]
    heads = k_ref.shape[3]
    chips = acc_ref.shape[1]
    step = pl.program_id(0)

    @pl.when(step == 0)
    def _():
        for core in range(2):
            acc_ref[core, :, :seq_dev] = jnp.zeros((chips, seq_dev, rows, head_dim), jnp.float32)
            lane = lax.broadcasted_iota(jnp.int32, (chips, 1, rows, head_dim), 3)
            acc_ref[core, :, seq_dev:] = jnp.where(lax.rem(lane, 2) == 0, LOW, 0.0)

    row = lax.broadcasted_iota(jnp.int32, (rows, page_size * heads), 0)
    column = lax.broadcasted_iota(jnp.int32, (rows, page_size * heads), 1)
    same_head = lax.rem(row, heads) == lax.rem(column, heads)
    position = jnp.where(same_head, column // heads, page_size)
    lane = lax.broadcasted_iota(jnp.int32, (rows, head_dim), 1)
    found = []
    for s in range(block):
        code = code_ref[step * block + s]
        held = jnp.maximum(code, 0)
        seen = jnp.where(code >= 0, lax.rem(held, 2 * page_size), 0)
        seq = held // (2 * page_size * pages_seq)
        home, place = seq // seq_dev, lax.rem(seq, seq_dev)
        core, chip = lax.rem(home, 2), home // 2
        q = x_ref[core, chip, 0, place]
        keys = k_ref[s, 0].reshape(page_size * heads, head_dim)
        values = v_ref[s, 0].reshape(page_size * heads, head_dim)
        scores = lax.dot_general(q, keys, (((1,), (1,)), ((), ())), preferred_element_type=jnp.float32) * scale
        mask = position < seen
        scores = jnp.where(mask, scores, LOW)
        top = jnp.max(scores, axis=1, keepdims=True)
        weights = jnp.where(mask, jnp.exp(scores - top), 0.0)
        total = jnp.sum(weights, axis=1, keepdims=True)
        high = weights.astype(jnp.bfloat16)
        low = (weights - high.astype(jnp.float32)).astype(jnp.bfloat16)
        mixed = jnp.dot(high, values, preferred_element_type=jnp.float32) + jnp.dot(low, values, preferred_element_type=jnp.float32)
        found.append((core, chip, place, top, total, mixed))
    for core, chip, place, top, total, mixed in found:
        stats = acc_ref[core, chip, seq_dev]
        old_top = jnp.max(jnp.where(lane == 2 * place, stats, LOW), axis=1, keepdims=True)
        old_total = jnp.sum(jnp.where(lane == 2 * place + 1, stats, 0.0), axis=1, keepdims=True)
        new_top = jnp.maximum(top, old_top)
        old_part, new_part = jnp.exp(old_top - new_top), jnp.exp(top - new_top)
        acc_ref[core, chip, place] = acc_ref[core, chip, place] * old_part + mixed * new_part
        new_total = old_total * old_part + total * new_part
        acc_ref[core, chip, seq_dev] = jnp.where(lane == 2 * place, new_top, jnp.where(lane == 2 * place + 1, new_total, stats))


def attend_pages(code, x_all, k_pool, v_pool, layer, pages_seq):
    slots, _, page_size, heads, head_dim = k_pool.shape
    cores, chips, _, seq_dev, rows, _ = x_all.shape
    block = 8
    page_spec = pl.BlockSpec((block, 1, page_size, heads, head_dim), lambda i, c: (i, layer, 0, 0, 0))
    query_spec = pl.BlockSpec((cores, chips, 1, seq_dev, rows, head_dim), lambda i, c: (0,) * 6)
    acc_shape = (cores, chips, seq_dev + 1, rows, head_dim)
    return pl.pallas_call(
        functools.partial(attend_kernel, block, pages_seq, seq_dev, page_size, head_dim ** -0.5),
        out_shape=jax.ShapeDtypeStruct(acc_shape, jnp.float32),
        grid_spec=pltpu.PrefetchScalarGridSpec(
            num_scalar_prefetch=1,
            grid=(slots // block,),
            in_specs=[query_spec, page_spec, page_spec],
            out_specs=pl.BlockSpec(acc_shape, lambda i, c: (0,) * 5),
        ),
        compiler_params=pltpu.CompilerParams(dimension_semantics=("arbitrary",)),
        cost_estimate=pl.CostEstimate(flops=10 ** 9, bytes_accessed=2 * slots * page_size * heads * head_dim * 2, transcendentals=0),
        name="attend_pages",
    )(code, x_all, k_pool, v_pool)


def spread_kernel(n, x_ref, out_ref, held, send_sem, recv_sem, pass_sem, got_sem, copy_sem):
    me = lax.axis_index("kv")
    chips = n // 2
    core, chip = lax.rem(me, 2), me // 2
    other = me + 1 - 2 * core

    def peer(j):
        return 2 * lax.rem(chip + j, chips) + core

    barrier = pltpu.get_barrier_semaphore()

    def greet(j, carry):
        pl.semaphore_signal(barrier, inc=1, device_id={"kv": peer(j)}, device_id_type=MESH)
        return carry

    lax.fori_loop(1, chips, greet, 0)
    pl.semaphore_signal(barrier, inc=1, device_id={"kv": other}, device_id_type=MESH)
    pl.semaphore_wait(barrier, chips)

    def send(j):
        return pltpu.make_async_remote_copy(
            src_ref=x_ref, dst_ref=held.at[core, chip], send_sem=send_sem.at[j], recv_sem=recv_sem.at[chip],
            device_id={"kv": peer(j)}, device_id_type=MESH,
        )

    def forward(source, at):
        return pltpu.make_async_remote_copy(
            src_ref=source, dst_ref=held.at[core, at], send_sem=pass_sem.at[at], recv_sem=got_sem.at[at],
            device_id={"kv": other}, device_id_type=MESH,
        )

    def start(j, carry):
        send(j).start()
        return carry

    lax.fori_loop(1, chips, start, 0)
    own = forward(x_ref, chip)
    own.start()
    mine = pltpu.make_async_copy(x_ref, out_ref.at[core, chip], copy_sem.at[0])
    mine.start()

    def arrive(j, carry):
        at = lax.rem(chip + chips - j, chips)
        pltpu.make_async_remote_copy(
            src_ref=x_ref, dst_ref=held.at[core, at], send_sem=send_sem.at[j], recv_sem=recv_sem.at[at],
            device_id={"kv": other}, device_id_type=MESH,
        ).wait_recv()
        forward(held.at[core, at], at).start()
        pltpu.make_async_copy(held.at[core, at], out_ref.at[core, at], copy_sem.at[j]).start()
        return carry

    lax.fori_loop(1, chips, arrive, 0)

    def passed(j, carry):
        at = lax.rem(chip + j, chips)
        pltpu.make_async_remote_copy(
            src_ref=x_ref, dst_ref=held.at[1 - core, at], send_sem=pass_sem.at[at], recv_sem=got_sem.at[at],
            device_id={"kv": other}, device_id_type=MESH,
        ).wait_recv()
        pltpu.make_async_copy(held.at[1 - core, at], out_ref.at[1 - core, at], copy_sem.at[chips + j]).start()
        return carry

    lax.fori_loop(0, chips, passed, 0)

    own.wait_send()
    mine.wait()

    def finish(j, carry):
        at = lax.rem(chip + chips - j, chips)
        send(j).wait_send()
        forward(held.at[core, at], at).wait_send()
        pltpu.make_async_copy(held.at[core, at], out_ref.at[core, at], copy_sem.at[j]).wait()
        return carry

    lax.fori_loop(1, chips, finish, 0)

    def written(j, carry):
        at = lax.rem(chip + j, chips)
        pltpu.make_async_copy(held.at[1 - core, at], out_ref.at[1 - core, at], copy_sem.at[chips + j]).wait()
        return carry

    lax.fori_loop(0, chips, written, 0)


def spread(x, n):
    chips = n // 2
    return pl.pallas_call(
        functools.partial(spread_kernel, n),
        out_shape=jax.ShapeDtypeStruct((2, chips) + x.shape, x.dtype),
        in_specs=[VMEM],
        out_specs=ANY,
        scratch_shapes=[
            pltpu.VMEM((2, chips) + x.shape, x.dtype),
            pltpu.SemaphoreType.DMA((chips,)),
            pltpu.SemaphoreType.DMA((chips,)),
            pltpu.SemaphoreType.DMA((chips,)),
            pltpu.SemaphoreType.DMA((chips,)),
            pltpu.SemaphoreType.DMA((n,)),
        ],
        compiler_params=pltpu.CompilerParams(collective_id=0, has_side_effects=True),
        name="spread_queries",
    )(x)


def lane_before(x):
    return pltpu.roll(x, x.shape[1] - 1, 1)


def gather_home_kernel(n, scale, acc_ref, x_ref, o_ref, near, sums, held, near_send, near_recv, send_sem, recv_sem):
    me = lax.axis_index("kv")
    _, seq_dev, rows, head_dim = x_ref.shape
    heads = rows // 2
    chips = n // 2
    core, chip = lax.rem(me, 2), me // 2
    other = me + 1 - 2 * core

    def peer(j):
        return 2 * lax.rem(chip + j, chips) + core

    barrier = pltpu.get_barrier_semaphore()

    def greet(j, carry):
        pl.semaphore_signal(barrier, inc=1, device_id={"kv": peer(j)}, device_id_type=MESH)
        return carry

    lax.fori_loop(1, chips, greet, 0)
    pl.semaphore_signal(barrier, inc=1, device_id={"kv": other}, device_id_type=MESH)
    pl.semaphore_wait(barrier, chips)

    swap = pltpu.make_async_remote_copy(
        src_ref=acc_ref.at[1 - core], dst_ref=near, send_sem=near_send.at[0], recv_sem=near_recv.at[0],
        device_id={"kv": other}, device_id_type=MESH,
    )
    swap.start()

    queries = [x_ref[0, i].astype(jnp.float32) for i in range(seq_dev)]
    second_row = lax.broadcasted_iota(jnp.int32, (rows, 1), 0) >= heads

    def twice(h, i, step):
        x = x_ref[1 + h, i, step * heads:(step + 1) * heads].astype(jnp.float32)
        return jnp.concatenate([x, x], axis=0)

    first = [jnp.sum(queries[i] * twice(0, i, 0), axis=1, keepdims=True) * scale for i in range(seq_dev)]
    second = [
        jnp.where(second_row, jnp.sum(queries[i] * twice(0, i, 1), axis=1, keepdims=True) * scale, LOW)
        for i in range(seq_dev)
    ]
    even = lax.rem(lax.broadcasted_iota(jnp.int32, (rows, head_dim), 1), 2) == 0

    def send(j):
        return pltpu.make_async_remote_copy(
            src_ref=sums.at[lax.rem(chip + j, chips)], dst_ref=held.at[chip], send_sem=send_sem.at[j], recv_sem=recv_sem.at[chip],
            device_id={"kv": peer(j)}, device_id_type=MESH,
        )

    def merge_near(at):
        mine, theirs = acc_ref[core, at, seq_dev], near[at, seq_dev]
        top = jnp.maximum(mine, theirs)
        a, b = jnp.exp(mine - top), jnp.exp(theirs - top)
        total = a * lane_before(mine) + b * lane_before(theirs)
        stats = jnp.where(even, top, pltpu.roll(total, 1, 1))
        return stats, [
            a[:, 2 * i:2 * i + 1] * acc_ref[core, at, i] + b[:, 2 * i:2 * i + 1] * near[at, i] for i in range(seq_dev)
        ]

    swap.wait_recv()

    def far(j, carry):
        at = lax.rem(chip + j, chips)
        stats, mixed = merge_near(at)
        sums[at, seq_dev] = stats
        for i in range(seq_dev):
            sums[at, i] = mixed[i]
        send(j).start()
        return carry

    lax.fori_loop(1, chips, far, 0)
    stats, mixed = merge_near(chip)
    held[chip, seq_dev] = stats
    for i in range(seq_dev):
        held[chip, i] = mixed[i]

    def arrive(j, carry):
        at = lax.rem(chip + chips - j, chips)
        pltpu.make_async_remote_copy(
            src_ref=sums.at[at], dst_ref=held.at[at], send_sem=send_sem.at[j], recv_sem=recv_sem.at[at],
            device_id={"kv": peer(j)}, device_id_type=MESH,
        ).wait_recv()
        return carry

    lax.fori_loop(1, chips, arrive, 0)

    def highest(j, top):
        return jnp.maximum(top, held[j, seq_dev])

    top_all = lax.fori_loop(0, chips, highest, jnp.full((rows, head_dim), LOW, jnp.float32))
    tops, totals, mixed = [], [], []
    for i in range(seq_dev):
        top = jnp.maximum(jnp.maximum(top_all[:, 2 * i:2 * i + 1], first[i]), second[i])
        p_first, p_second = jnp.exp(first[i] - top), jnp.exp(second[i] - top)
        tops.append(top)
        totals.append(p_first + p_second)
        mixed.append(p_first * twice(1, i, 0) + p_second * twice(1, i, 1))

    def merge(j, carry):
        totals, mixed = carry
        stats = held[j, seq_dev]
        new_totals, new_mixed = [], []
        for i in range(seq_dev):
            weight = jnp.exp(stats[:, 2 * i:2 * i + 1] - tops[i])
            new_totals.append(totals[i] + weight * stats[:, 2 * i + 1:2 * i + 2])
            new_mixed.append(mixed[i] + weight * held[j, i])
        return tuple(new_totals), tuple(new_mixed)

    totals, mixed = lax.fori_loop(0, chips, merge, (tuple(totals), tuple(mixed)))
    for i in range(seq_dev):
        o_ref[i] = (mixed[i] / totals[i]).astype(o_ref.dtype)

    swap.wait_send()

    def finish(j, carry):
        send(j).wait_send()
        return carry

    lax.fori_loop(1, chips, finish, 0)


def gather_home(acc, x, n):
    chips = n // 2
    blocks = acc.shape[1:]
    return pl.pallas_call(
        functools.partial(gather_home_kernel, n, x.shape[-1] ** -0.5),
        out_shape=jax.ShapeDtypeStruct(x.shape[1:], jnp.bfloat16),
        in_specs=[VMEM] * 2,
        out_specs=VMEM,
        scratch_shapes=[
            pltpu.VMEM(blocks, acc.dtype),
            pltpu.VMEM(blocks, acc.dtype),
            pltpu.VMEM(blocks, acc.dtype),
            pltpu.SemaphoreType.DMA((1,)),
            pltpu.SemaphoreType.DMA((1,)),
            pltpu.SemaphoreType.DMA((chips,)),
            pltpu.SemaphoreType.DMA((chips,)),
        ],
        compiler_params=pltpu.CompilerParams(collective_id=1, has_side_effects=True),
        name="gather_home",
    )(acc, x)


def solution(mesh):
    groups = mesh.shape['kv']
    rows_spec = P(None, ('rep', 'kv'), None)
    pool_spec = P(('rep', 'kv'))
    table_spec = P('rep', None)
    vec_spec = P('rep')
    full_spec = P()

    def device_fn(embeds, w_query, w_key, w_value, w_out, w_up, w_down, k_pool, v_pool, old_table, new_table, seq_len, finished, mig_src, mig_dst):
        me = lax.axis_index('kv')
        slots, n_layers, page_size, heads, head_dim = k_pool.shape
        steps, seq_dev, width = embeds.shape
        n_batch, pages_seq = old_table.shape
        n_mig = mig_src.shape[0]
        rounds = 4 * n_mig // (groups * groups)
        base = me * slots
        local = jnp.arange(slots, dtype=jnp.int32)
        active = finished == 0
        last = pages_seq - 1

        def find(match, value):
            return jnp.max(jnp.where(match, value, -1), axis=1)

        flat = old_table.reshape(-1)
        place = jnp.arange(n_batch * pages_seq, dtype=jnp.int32)
        seen = jnp.clip(seq_len[:, None] - jnp.arange(pages_seq, dtype=jnp.int32)[None, :] * page_size, 0, page_size).reshape(-1)
        code = find(flat[None, :] - base == local[:, None], (place * (2 * page_size) + seen)[None, :])

        src_dev, dst_dev = mig_src // slots, mig_dst // slots
        pair = src_dev * groups + dst_dev
        entry = jnp.arange(n_mig, dtype=jnp.int32)
        rank = jnp.sum((pair[None, :] == pair[:, None]) & (entry[None, :] < entry[:, None]), axis=1, dtype=jnp.int32)
        lines = jnp.arange(rounds * groups, dtype=jnp.int32)
        send_slot = find(
            ((rank * groups + dst_dev)[None, :] == lines[:, None]) & (src_dev == me)[None, :], (mig_src - src_dev * slots)[None, :]
        )
        from_page = find((mig_dst - base)[None, :] == local[:, None], (rank * groups + src_dev)[None, :])

        seq_ids = jnp.arange(n_batch, dtype=jnp.int32)
        owner_old = find((old_table[:, last] - base)[None, :] == local[:, None], seq_ids[None, :])
        owner_new = find(((new_table[:, last] - base)[None, :] == local[:, None]) & active[None, :], seq_ids[None, :])
        first_seq = jnp.where(from_page >= 0, owner_new, owner_old)
        second_seq = owner_new
        offsets = lax.rem(seq_len, page_size)

        def exchange(block):
            return lax.all_to_all(block, 'kv', 0, 0, tiled=True)

        def after(blocks, value):
            out = lax.optimization_barrier((tuple(blocks), value))
            return [exchange(block) for block in out[0]], out[1]

        (k_packed,) = pack_pages(((0, (0,)),), send_slot, k_pool, v_pool, groups)
        plan = ((0, (1,)),) + tuple((r, (0, 1)) for r in range(1, rounds))
        packed = [k_packed] + list(pack_pages(plan, send_slot, k_pool, v_pool, groups))
        got = [exchange(packed[0])]
        split = [packed[1:2], packed[2:4], packed[4:5], packed[5:]]
        tables = (from_page, first_seq, second_seq, offsets)
        k_out, v_out = keep_pages(from_page, k_pool, v_pool)

        hidden = jnp.transpose(embeds, (1, 0, 2)).reshape(seq_dev * steps, width)
        rows = []
        for layer in range(n_layers):
            x = jnp.stack([
                jnp.dot(hidden, w[layer], preferred_element_type=jnp.float32).astype(jnp.bfloat16).reshape(seq_dev, steps * heads, head_dim)
                for w in (w_query, w_key, w_value)
            ])
            x, k_out, v_out = lax.optimization_barrier((x, k_out, v_out))
            x_all = spread(x, groups)
            rows.append(x_all)
            if split:
                more, x_all = after(split.pop(0), x_all)
                got += more
            acc = attend_pages(code, x_all, k_pool, v_pool, layer, pages_seq)
            mixed = gather_home(acc, x, groups)
            if split:
                more, mixed = after(split.pop(0), mixed)
                got += more
            if layer == 0:
                k_out, v_out = place_pages(((0, (0, 1)),), seq_dev, *tables, got[:2], [], k_out, v_out)
            mixed = mixed.reshape(seq_dev * steps, heads * head_dim)
            hidden = (hidden.astype(jnp.float32) + jnp.dot(mixed, w_out[layer], preferred_element_type=jnp.float32)).astype(jnp.bfloat16)
            inner = jax.nn.gelu(jnp.dot(hidden, w_up[layer], preferred_element_type=jnp.float32)).astype(jnp.bfloat16)
            hidden = (hidden.astype(jnp.float32) + jnp.dot(inner, w_down[layer], preferred_element_type=jnp.float32)).astype(jnp.bfloat16)
        for blocks in split:
            got += [exchange(block) for block in blocks]
        early = tuple((r, (0, 1)) for r in range(1, rounds - 1)) + ((rounds - 1, (0,)),)
        k_out, v_out = place_pages(early, seq_dev, *tables, got[2:-1], [], k_out, v_out)
        k_out, v_out = place_pages(((rounds - 1, (1,)),), seq_dev, *tables, got[-1:], rows, k_out, v_out)
        hidden = jnp.transpose(hidden.reshape(seq_dev, steps, width), (1, 0, 2))
        done = lax.dynamic_slice(finished, (me * seq_dev,), (seq_dev,)) != 0
        live = jnp.stack([jnp.ones_like(done), ~done])
        hidden = jnp.where(live[:, :, None], hidden, jnp.zeros_like(hidden))
        return hidden, k_out, v_out

    in_specs = (rows_spec, full_spec, full_spec, full_spec, full_spec, full_spec, full_spec, pool_spec, pool_spec, table_spec, table_spec, vec_spec, vec_spec, vec_spec, vec_spec)
    return jax.shard_map(device_fn, mesh=mesh, in_specs=in_specs, out_specs=(rows_spec, pool_spec, pool_spec), check_vma=False)
```

```python
import functools

import jax
import jax.numpy as jnp
from jax import lax
from jax.experimental import pallas as pl
from jax.experimental.pallas import tpu as pltpu
from jax.sharding import PartitionSpec as P

MESH = pl.DeviceIdType.MESH
ANY = pl.BlockSpec(memory_space=pl.ANY)
VMEM = pl.BlockSpec(memory_space=pltpu.VMEM)
SMEM = pl.BlockSpec(memory_space=pltpu.SMEM)
LOW = -1e30


def ring(count, depth, lead, start_in, wait_in, start_out, wait_out):
    def body(i, carry):
        @pl.when(i < count)
        def _():
            @pl.when(i >= depth)
            def _():
                wait_out(i - depth)

            start_in(i)

        @pl.when(i >= lead)
        def _():
            wait_in(i - lead)
            start_out(i - lead)

        return carry

    lax.fori_loop(0, count + lead, body, 0)

    def drain(i, carry):
        wait_out(i)
        return carry

    lax.fori_loop(jnp.maximum(count - depth, 0), count, drain, 0)


def compact(total, flag, value, listed):
    def body(i, count):
        @pl.when(flag(i))
        def _():
            listed[count] = value(i)

        return count + flag(i).astype(jnp.int32)

    return lax.fori_loop(0, total, body, jnp.int32(0))


def pack_kernel(depth, lead, plan, slot_ref, *rest):
    pools = rest[:2]
    outs = rest[2:-4]
    buf, listed, sems_in, sems_out = rest[-4:]
    peers = outs[0].shape[0]
    for r, halves in plan:
        mine, outs = outs[0], outs[1:]
        count = compact(peers, lambda i: slot_ref[r * peers + i] >= 0, lambda i: i, listed)

        def ins(i):
            at = lax.rem(i, depth)
            slot = slot_ref[r * peers + listed[i]]
            return [pltpu.make_async_copy(pools[h].at[slot], buf.at[at, h], sems_in.at[at, h]) for h in halves]

        def puts(i):
            at = lax.rem(i, depth)
            return [pltpu.make_async_copy(buf.at[at, h], mine.at[listed[i], k], sems_out.at[at, h]) for k, h in enumerate(halves)]

        ring(
            count, depth, lead,
            lambda i: [c.start() for c in ins(i)],
            lambda i: [c.wait() for c in ins(i)],
            lambda i: [c.start() for c in puts(i)],
            lambda i: [c.wait() for c in puts(i)],
        )


def pack_pages(plan, send_slot, k_pool, v_pool, peers):
    page = k_pool.shape[1:]
    depth, lead = 24, 12
    total = sum(len(halves) for _, halves in plan)
    return pl.pallas_call(
        functools.partial(pack_kernel, depth, lead, plan),
        out_shape=[jax.ShapeDtypeStruct((peers, len(halves)) + page, k_pool.dtype) for _, halves in plan],
        in_specs=[SMEM, ANY, ANY],
        out_specs=[ANY] * len(plan),
        scratch_shapes=[
            pltpu.VMEM((depth, 2) + page, k_pool.dtype),
            pltpu.SMEM((peers,), jnp.int32),
            pltpu.SemaphoreType.DMA((depth, 2)),
            pltpu.SemaphoreType.DMA((depth, 2)),
        ],
        cost_estimate=pl.CostEstimate(flops=10 ** 8 * total, bytes_accessed=2 ** 21 * total, transcendentals=0),
        name="pack_pages",
    )(send_slot, k_pool, v_pool)


def keep_kernel(depth, lead, from_ref, k_ref, v_ref, k_out, v_out, buf, listed, sems_in, sems_out):
    count = compact(from_ref.shape[0], lambda i: from_ref[i] < 0, lambda i: i, listed)

    def ins(i):
        at = lax.rem(i, depth)
        return [pltpu.make_async_copy(ref.at[listed[i]], buf.at[at, h], sems_in.at[at, h]) for h, ref in enumerate((k_ref, v_ref))]

    def outs(i):
        at = lax.rem(i, depth)
        return [pltpu.make_async_copy(buf.at[at, h], ref.at[listed[i]], sems_out.at[at, h]) for h, ref in enumerate((k_out, v_out))]

    ring(
        count, depth, lead,
        lambda i: [c.start() for c in ins(i)],
        lambda i: [c.wait() for c in ins(i)],
        lambda i: [c.start() for c in outs(i)],
        lambda i: [c.wait() for c in outs(i)],
    )


def keep_pages(from_page, k_pool, v_pool):
    depth, lead = 24, 12
    return pl.pallas_call(
        functools.partial(keep_kernel, depth, lead),
        out_shape=[jax.ShapeDtypeStruct(k_pool.shape, k_pool.dtype)] * 2,
        in_specs=[SMEM] + [ANY] * 2,
        out_specs=[ANY] * 2,
        scratch_shapes=[
            pltpu.VMEM((depth, 2) + k_pool.shape[1:], k_pool.dtype),
            pltpu.SMEM((k_pool.shape[0],), jnp.int32),
            pltpu.SemaphoreType.DMA((depth, 2)),
            pltpu.SemaphoreType.DMA((depth, 2)),
        ],
        cost_estimate=pl.CostEstimate(flops=10 ** 9, bytes_accessed=2 ** 25, transcendentals=0),
        name="keep_pages",
    )(from_page, k_pool, v_pool)


def place_kernel(depth, lead, plan, patches, seq_dev, n_rows, from_ref, first_ref, second_ref, offset_ref, *rest):
    arrived, rest = rest[:len(plan)], rest[len(plan):]
    rows = rest[:n_rows]
    k_out, v_out, buf, listed, sems_in, sems_out, staged, entries, sem_row = rest[n_rows + 2:]
    pools = (k_out, v_out)
    peers = arrived[0].shape[0]
    slots, n_batch = from_ref.shape[0], offset_ref.shape[0]
    heads = k_out.shape[3]

    def came(slot, r):
        return (from_ref[slot] >= r * peers) & (from_ref[slot] < (r + 1) * peers)

    def fetch(at, seq, step, h):
        home, place = seq // seq_dev, lax.rem(seq, seq_dev)
        return [
            pltpu.make_async_copy(
                x.at[lax.rem(home, 2), home // 2, 1 + h, place, pl.ds(step * heads, heads)], staged.at[at, layer], sem_row.at[0]
            )
            for layer, x in enumerate(rows)
        ]

    ends = []
    found = jnp.int32(0)
    for h, rounds, inside in patches:
        def collect(slot, count):
            hit = jnp.bool_(False)
            for r in rounds:
                hit = hit | came(slot, r)
            for step, ref in enumerate((first_ref, second_ref)):
                seq = ref[slot]
                take = (seq >= 0) & (hit == inside)

                @pl.when(take)
                def _():
                    entries[count] = (slot * 2 + step) * n_batch + seq
                    for c in fetch(count, seq, step, h):
                        c.start()

                count = count + take.astype(jnp.int32)
            return count

        found = lax.fori_loop(0, slots, collect, found)
        ends.append(found)

    for part, (r, halves) in enumerate(plan):
        count = compact(slots, lambda i: came(i, r), lambda i: i, listed)

        def ins(i):
            at = lax.rem(i, depth)
            line = from_ref[listed[i]] - r * peers
            return [pltpu.make_async_copy(arrived[part].at[line, k], buf.at[at, h], sems_in.at[at, h]) for k, h in enumerate(halves)]

        def outs(i):
            at = lax.rem(i, depth)
            return [pltpu.make_async_copy(buf.at[at, h], pools[h].at[listed[i]], sems_out.at[at, h]) for h in halves]

        ring(
            count, depth, lead,
            lambda i: [c.start() for c in ins(i)],
            lambda i: [c.wait() for c in ins(i)],
            lambda i: [c.start() for c in outs(i)],
            lambda i: [c.wait() for c in outs(i)],
        )

    if patches:
        def fetched(i, carry):
            for c in fetch(i, 0, 0, 0):
                c.wait()
            return carry

        lax.fori_loop(0, found, fetched, 0)
        begin = jnp.int32(0)
        for (h, _, _), end in zip(patches, ends):
            def row_outs(i):
                entry = entries[i]
                seq, at = lax.rem(entry, n_batch), entry // n_batch
                slot, step = at // 2, lax.rem(at, 2)
                return [
                    pltpu.make_async_copy(staged.at[i, layer], pools[h].at[slot, layer, offset_ref[seq] + step], sem_row.at[1])
                    for layer in range(n_rows)
                ]

            def start(i, carry):
                for c in row_outs(i):
                    c.start()
                return carry

            lax.fori_loop(begin, end, start, 0)
            begin = end

        def written(i, carry):
            for layer in range(n_rows):
                pltpu.make_async_copy(staged.at[i, layer], k_out.at[0, layer, 0], sem_row.at[1]).wait()
            return carry

        lax.fori_loop(0, found, written, 0)


def place_pages(plan, patches, seq_dev, from_page, first_seq, second_seq, offsets, arrived, rows, k_out, v_out):
    depth, lead = 24, 12
    first_pool = 4 + len(arrived) + len(rows)
    most = max(2 * len(patches) * k_out.shape[0], 1)
    return pl.pallas_call(
        functools.partial(place_kernel, depth, lead, plan, patches, seq_dev, len(rows)),
        out_shape=[jax.ShapeDtypeStruct(k_out.shape, k_out.dtype)] * 2,
        in_specs=[SMEM] * 4 + [ANY] * (len(arrived) + len(rows) + 2),
        out_specs=[ANY] * 2,
        scratch_shapes=[
            pltpu.VMEM((depth, 2) + k_out.shape[1:], k_out.dtype),
            pltpu.SMEM((k_out.shape[0],), jnp.int32),
            pltpu.SemaphoreType.DMA((depth, 2)),
            pltpu.SemaphoreType.DMA((depth, 2)),
            pltpu.VMEM((most, max(len(rows), 1)) + k_out.shape[3:], k_out.dtype),
            pltpu.SMEM((most,), jnp.int32),
            pltpu.SemaphoreType.DMA((2,)),
        ],
        input_output_aliases={first_pool: 0, first_pool + 1: 1},
        cost_estimate=pl.CostEstimate(flops=2 * 10 ** 8 * len(arrived), bytes_accessed=2 ** 22 * len(arrived), transcendentals=0),
        name="place_pages",
    )(from_page, first_seq, second_seq, offsets, *arrived, *rows, k_out, v_out)


def attend_kernel(block, pages_seq, seq_dev, page_size, scale, code_ref, x_ref, k_ref, v_ref, acc_ref):
    rows, head_dim = x_ref.shape[-2:]
    heads = k_ref.shape[3]
    chips = acc_ref.shape[1]
    step = pl.program_id(0)

    @pl.when(step == 0)
    def _():
        for core in range(2):
            acc_ref[core, :, :seq_dev] = jnp.zeros((chips, seq_dev, rows, head_dim), jnp.float32)
            lane = lax.broadcasted_iota(jnp.int32, (chips, 1, rows, head_dim), 3)
            acc_ref[core, :, seq_dev:] = jnp.where(lax.rem(lane, 2) == 0, LOW, 0.0)

    row = lax.broadcasted_iota(jnp.int32, (rows, page_size * heads), 0)
    column = lax.broadcasted_iota(jnp.int32, (rows, page_size * heads), 1)
    same_head = lax.rem(row, heads) == lax.rem(column, heads)
    position = jnp.where(same_head, column // heads, page_size)
    lane = lax.broadcasted_iota(jnp.int32, (rows, head_dim), 1)
    found = []
    for s in range(block):
        code = code_ref[step * block + s]
        held = jnp.maximum(code, 0)
        seen = jnp.where(code >= 0, lax.rem(held, 2 * page_size), 0)
        seq = held // (2 * page_size * pages_seq)
        home, place = seq // seq_dev, lax.rem(seq, seq_dev)
        core, chip = lax.rem(home, 2), home // 2
        q = x_ref[core, chip, 0, place]
        keys = k_ref[s, 0].reshape(page_size * heads, head_dim)
        values = v_ref[s, 0].reshape(page_size * heads, head_dim)
        scores = lax.dot_general(q, keys, (((1,), (1,)), ((), ())), preferred_element_type=jnp.float32) * scale
        mask = position < seen
        scores = jnp.where(mask, scores, LOW)
        top = jnp.max(scores, axis=1, keepdims=True)
        weights = jnp.where(mask, jnp.exp(scores - top), 0.0)
        total = jnp.sum(weights, axis=1, keepdims=True)
        high = weights.astype(jnp.bfloat16)
        low = (weights - high.astype(jnp.float32)).astype(jnp.bfloat16)
        mixed = jnp.dot(high, values, preferred_element_type=jnp.float32) + jnp.dot(low, values, preferred_element_type=jnp.float32)
        found.append((core, chip, place, top, total, mixed))
    for core, chip, place, top, total, mixed in found:
        stats = acc_ref[core, chip, seq_dev]
        old_top = jnp.max(jnp.where(lane == 2 * place, stats, LOW), axis=1, keepdims=True)
        old_total = jnp.sum(jnp.where(lane == 2 * place + 1, stats, 0.0), axis=1, keepdims=True)
        new_top = jnp.maximum(top, old_top)
        old_part, new_part = jnp.exp(old_top - new_top), jnp.exp(top - new_top)
        acc_ref[core, chip, place] = acc_ref[core, chip, place] * old_part + mixed * new_part
        new_total = old_total * old_part + total * new_part
        acc_ref[core, chip, seq_dev] = jnp.where(lane == 2 * place, new_top, jnp.where(lane == 2 * place + 1, new_total, stats))


def attend_pages(code, x_all, k_pool, v_pool, layer, pages_seq):
    slots, _, page_size, heads, head_dim = k_pool.shape
    cores, chips, _, seq_dev, rows, _ = x_all.shape
    block = 8
    page_spec = pl.BlockSpec((block, 1, page_size, heads, head_dim), lambda i, c: (i, layer, 0, 0, 0))
    query_spec = pl.BlockSpec((cores, chips, 1, seq_dev, rows, head_dim), lambda i, c: (0,) * 6)
    acc_shape = (cores, chips, seq_dev + 1, rows, head_dim)
    return pl.pallas_call(
        functools.partial(attend_kernel, block, pages_seq, seq_dev, page_size, head_dim ** -0.5),
        out_shape=jax.ShapeDtypeStruct(acc_shape, jnp.float32),
        grid_spec=pltpu.PrefetchScalarGridSpec(
            num_scalar_prefetch=1,
            grid=(slots // block,),
            in_specs=[query_spec, page_spec, page_spec],
            out_specs=pl.BlockSpec(acc_shape, lambda i, c: (0,) * 5),
        ),
        compiler_params=pltpu.CompilerParams(dimension_semantics=("arbitrary",)),
        cost_estimate=pl.CostEstimate(flops=10 ** 9, bytes_accessed=2 * slots * page_size * heads * head_dim * 2, transcendentals=0),
        name="attend_pages",
    )(code, x_all, k_pool, v_pool)


def spread_kernel(n, x_ref, out_ref, held, send_sem, recv_sem, pass_sem, got_sem, copy_sem):
    me = lax.axis_index("kv")
    chips = n // 2
    core, chip = lax.rem(me, 2), me // 2
    other = me + 1 - 2 * core

    def peer(j):
        return 2 * lax.rem(chip + j, chips) + core

    barrier = pltpu.get_barrier_semaphore()

    def greet(j, carry):
        pl.semaphore_signal(barrier, inc=1, device_id={"kv": peer(j)}, device_id_type=MESH)
        return carry

    lax.fori_loop(1, chips, greet, 0)
    pl.semaphore_signal(barrier, inc=1, device_id={"kv": other}, device_id_type=MESH)
    pl.semaphore_wait(barrier, chips)

    def send(j):
        return pltpu.make_async_remote_copy(
            src_ref=x_ref, dst_ref=held.at[core, chip], send_sem=send_sem.at[j], recv_sem=recv_sem.at[chip],
            device_id={"kv": peer(j)}, device_id_type=MESH,
        )

    def forward(source, at):
        return pltpu.make_async_remote_copy(
            src_ref=source, dst_ref=held.at[core, at], send_sem=pass_sem.at[at], recv_sem=got_sem.at[at],
            device_id={"kv": other}, device_id_type=MESH,
        )

    def start(j, carry):
        send(j).start()
        return carry

    lax.fori_loop(1, chips, start, 0)
    own = forward(x_ref, chip)
    own.start()
    mine = pltpu.make_async_copy(x_ref, out_ref.at[core, chip], copy_sem.at[0])
    mine.start()

    def arrive(j, carry):
        at = lax.rem(chip + chips - j, chips)
        pltpu.make_async_remote_copy(
            src_ref=x_ref, dst_ref=held.at[core, at], send_sem=send_sem.at[j], recv_sem=recv_sem.at[at],
            device_id={"kv": other}, device_id_type=MESH,
        ).wait_recv()
        forward(held.at[core, at], at).start()
        pltpu.make_async_copy(held.at[core, at], out_ref.at[core, at], copy_sem.at[j]).start()
        return carry

    lax.fori_loop(1, chips, arrive, 0)

    def passed(j, carry):
        at = lax.rem(chip + j, chips)
        pltpu.make_async_remote_copy(
            src_ref=x_ref, dst_ref=held.at[1 - core, at], send_sem=pass_sem.at[at], recv_sem=got_sem.at[at],
            device_id={"kv": other}, device_id_type=MESH,
        ).wait_recv()
        pltpu.make_async_copy(held.at[1 - core, at], out_ref.at[1 - core, at], copy_sem.at[chips + j]).start()
        return carry

    lax.fori_loop(0, chips, passed, 0)

    own.wait_send()
    mine.wait()

    def finish(j, carry):
        at = lax.rem(chip + chips - j, chips)
        send(j).wait_send()
        forward(held.at[core, at], at).wait_send()
        pltpu.make_async_copy(held.at[core, at], out_ref.at[core, at], copy_sem.at[j]).wait()
        return carry

    lax.fori_loop(1, chips, finish, 0)

    def written(j, carry):
        at = lax.rem(chip + j, chips)
        pltpu.make_async_copy(held.at[1 - core, at], out_ref.at[1 - core, at], copy_sem.at[chips + j]).wait()
        return carry

    lax.fori_loop(0, chips, written, 0)


def spread(x, n):
    chips = n // 2
    return pl.pallas_call(
        functools.partial(spread_kernel, n),
        out_shape=jax.ShapeDtypeStruct((2, chips) + x.shape, x.dtype),
        in_specs=[VMEM],
        out_specs=ANY,
        scratch_shapes=[
            pltpu.VMEM((2, chips) + x.shape, x.dtype),
            pltpu.SemaphoreType.DMA((chips,)),
            pltpu.SemaphoreType.DMA((chips,)),
            pltpu.SemaphoreType.DMA((chips,)),
            pltpu.SemaphoreType.DMA((chips,)),
            pltpu.SemaphoreType.DMA((n,)),
        ],
        compiler_params=pltpu.CompilerParams(collective_id=0, has_side_effects=True),
        name="spread_queries",
    )(x)


def lane_before(x):
    return pltpu.roll(x, x.shape[1] - 1, 1)


def merge_chip_kernel(acc_ref, sums_ref, near, send_sem, recv_sem):
    me = lax.axis_index("kv")
    core = lax.rem(me, 2)
    other = me + 1 - 2 * core
    chips, blocks, rows, head_dim = near.shape
    seq_dev = blocks - 1

    barrier = pltpu.get_barrier_semaphore()
    pl.semaphore_signal(barrier, inc=1, device_id={"kv": other}, device_id_type=MESH)
    pl.semaphore_wait(barrier, 1)

    swap = pltpu.make_async_remote_copy(
        src_ref=acc_ref.at[1 - core], dst_ref=near, send_sem=send_sem.at[0], recv_sem=recv_sem.at[0],
        device_id={"kv": other}, device_id_type=MESH,
    )
    swap.start()
    even = lax.rem(lax.broadcasted_iota(jnp.int32, (rows, head_dim), 1), 2) == 0
    swap.wait_recv()

    def merge(at, carry):
        mine, theirs = acc_ref[core, at, seq_dev], near[at, seq_dev]
        top = jnp.maximum(mine, theirs)
        a, b = jnp.exp(mine - top), jnp.exp(theirs - top)
        total = a * lane_before(mine) + b * lane_before(theirs)
        sums_ref[at, seq_dev] = jnp.where(even, top, pltpu.roll(total, 1, 1))
        for i in range(seq_dev):
            sums_ref[at, i] = a[:, 2 * i:2 * i + 1] * acc_ref[core, at, i] + b[:, 2 * i:2 * i + 1] * near[at, i]
        return carry

    lax.fori_loop(0, chips, merge, 0)
    swap.wait_send()


def merge_chip(acc):
    blocks = acc.shape[1:]
    return pl.pallas_call(
        merge_chip_kernel,
        out_shape=jax.ShapeDtypeStruct(blocks, acc.dtype),
        in_specs=[VMEM],
        out_specs=VMEM,
        scratch_shapes=[
            pltpu.VMEM(blocks, acc.dtype),
            pltpu.SemaphoreType.DMA((1,)),
            pltpu.SemaphoreType.DMA((1,)),
        ],
        compiler_params=pltpu.CompilerParams(collective_id=2, has_side_effects=True),
        cost_estimate=pl.CostEstimate(flops=10 ** 9, bytes_accessed=2 ** 23, transcendentals=0),
        name="merge_chip",
    )(acc)


def gather_home_kernel(n, scale, sums_ref, x_ref, o_ref, held, send_sem, recv_sem):
    me = lax.axis_index("kv")
    _, seq_dev, rows, head_dim = x_ref.shape
    heads = rows // 2
    chips = n // 2
    core, chip = lax.rem(me, 2), me // 2

    def peer(j):
        return 2 * lax.rem(chip + j, chips) + core

    barrier = pltpu.get_barrier_semaphore()

    def greet(j, carry):
        pl.semaphore_signal(barrier, inc=1, device_id={"kv": peer(j)}, device_id_type=MESH)
        return carry

    lax.fori_loop(1, chips, greet, 0)
    pl.semaphore_wait(barrier, chips - 1)

    def send(j):
        return pltpu.make_async_remote_copy(
            src_ref=sums_ref.at[lax.rem(chip + j, chips)], dst_ref=held.at[chip], send_sem=send_sem.at[j], recv_sem=recv_sem.at[chip],
            device_id={"kv": peer(j)}, device_id_type=MESH,
        )

    def start(j, carry):
        send(j).start()
        return carry

    lax.fori_loop(1, chips, start, 0)
    held[chip] = sums_ref[chip]

    queries = [x_ref[0, i].astype(jnp.float32) for i in range(seq_dev)]
    second_row = lax.broadcasted_iota(jnp.int32, (rows, 1), 0) >= heads

    def twice(h, i, step):
        x = x_ref[1 + h, i, step * heads:(step + 1) * heads].astype(jnp.float32)
        return jnp.concatenate([x, x], axis=0)

    first = [jnp.sum(queries[i] * twice(0, i, 0), axis=1, keepdims=True) * scale for i in range(seq_dev)]
    second = [
        jnp.where(second_row, jnp.sum(queries[i] * twice(0, i, 1), axis=1, keepdims=True) * scale, LOW)
        for i in range(seq_dev)
    ]
    def arrive(j, carry):
        at = lax.rem(chip + chips - j, chips)
        pltpu.make_async_remote_copy(
            src_ref=sums_ref.at[at], dst_ref=held.at[at], send_sem=send_sem.at[j], recv_sem=recv_sem.at[at],
            device_id={"kv": peer(j)}, device_id_type=MESH,
        ).wait_recv()
        return carry

    lax.fori_loop(1, chips, arrive, 0)

    def highest(j, top):
        return jnp.maximum(top, held[j, seq_dev])

    top_all = lax.fori_loop(0, chips, highest, jnp.full((rows, head_dim), LOW, jnp.float32))
    tops, totals, mixed = [], [], []
    for i in range(seq_dev):
        top = jnp.maximum(jnp.maximum(top_all[:, 2 * i:2 * i + 1], first[i]), second[i])
        p_first, p_second = jnp.exp(first[i] - top), jnp.exp(second[i] - top)
        tops.append(top)
        totals.append(p_first + p_second)
        mixed.append(p_first * twice(1, i, 0) + p_second * twice(1, i, 1))

    def merge(j, carry):
        totals, mixed = carry
        stats = held[j, seq_dev]
        new_totals, new_mixed = [], []
        for i in range(seq_dev):
            weight = jnp.exp(stats[:, 2 * i:2 * i + 1] - tops[i])
            new_totals.append(totals[i] + weight * stats[:, 2 * i + 1:2 * i + 2])
            new_mixed.append(mixed[i] + weight * held[j, i])
        return tuple(new_totals), tuple(new_mixed)

    totals, mixed = lax.fori_loop(0, chips, merge, (tuple(totals), tuple(mixed)))
    for i in range(seq_dev):
        o_ref[i] = (mixed[i] / totals[i]).astype(o_ref.dtype)

    def finish(j, carry):
        send(j).wait_send()
        return carry

    lax.fori_loop(1, chips, finish, 0)


def gather_home(sums, x, n):
    chips = n // 2
    return pl.pallas_call(
        functools.partial(gather_home_kernel, n, x.shape[-1] ** -0.5),
        out_shape=jax.ShapeDtypeStruct(x.shape[1:], jnp.bfloat16),
        in_specs=[VMEM] * 2,
        out_specs=VMEM,
        scratch_shapes=[
            pltpu.VMEM(sums.shape, sums.dtype),
            pltpu.SemaphoreType.DMA((chips,)),
            pltpu.SemaphoreType.DMA((chips,)),
        ],
        compiler_params=pltpu.CompilerParams(collective_id=1, has_side_effects=True),
        name="gather_home",
    )(sums, x)


def solution(mesh):
    groups = mesh.shape['kv']
    rows_spec = P(None, ('rep', 'kv'), None)
    pool_spec = P(('rep', 'kv'))
    table_spec = P('rep', None)
    vec_spec = P('rep')
    full_spec = P()

    def device_fn(embeds, w_query, w_key, w_value, w_out, w_up, w_down, k_pool, v_pool, old_table, new_table, seq_len, finished, mig_src, mig_dst):
        me = lax.axis_index('kv')
        slots, n_layers, page_size, heads, head_dim = k_pool.shape
        steps, seq_dev, width = embeds.shape
        n_batch, pages_seq = old_table.shape
        n_mig = mig_src.shape[0]
        rounds = 4 * n_mig // (groups * groups)
        base = me * slots
        local = jnp.arange(slots, dtype=jnp.int32)
        active = finished == 0
        last = pages_seq - 1

        def find(match, value):
            return jnp.max(jnp.where(match, value, -1), axis=1)

        flat = old_table.reshape(-1)
        place = jnp.arange(n_batch * pages_seq, dtype=jnp.int32)
        seen = jnp.clip(seq_len[:, None] - jnp.arange(pages_seq, dtype=jnp.int32)[None, :] * page_size, 0, page_size).reshape(-1)
        code = find(flat[None, :] - base == local[:, None], (place * (2 * page_size) + seen)[None, :])

        src_dev, dst_dev = mig_src // slots, mig_dst // slots
        pair = src_dev * groups + dst_dev
        entry = jnp.arange(n_mig, dtype=jnp.int32)
        rank = jnp.sum((pair[None, :] == pair[:, None]) & (entry[None, :] < entry[:, None]), axis=1, dtype=jnp.int32)
        lines = jnp.arange(rounds * groups, dtype=jnp.int32)
        send_slot = find(
            ((rank * groups + dst_dev)[None, :] == lines[:, None]) & (src_dev == me)[None, :], (mig_src - src_dev * slots)[None, :]
        )
        from_page = find((mig_dst - base)[None, :] == local[:, None], (rank * groups + src_dev)[None, :])

        seq_ids = jnp.arange(n_batch, dtype=jnp.int32)
        owner_old = find((old_table[:, last] - base)[None, :] == local[:, None], seq_ids[None, :])
        owner_new = find(((new_table[:, last] - base)[None, :] == local[:, None]) & active[None, :], seq_ids[None, :])
        first_seq = jnp.where(from_page >= 0, owner_new, owner_old)
        second_seq = owner_new
        offsets = lax.rem(seq_len, page_size)

        def exchange(block):
            return lax.all_to_all(block, 'kv', 0, 0, tiled=True)

        def send_next(value, count):
            for block in packed[len(got):len(got) + count]:
                block, value = lax.optimization_barrier((block, value))
                got.append(exchange(block))
            return value

        plan = ((0, (0,)), (0, (1,))) + tuple((r, (0, 1)) for r in range(1, rounds - 1)) + ((rounds - 1, (0,)), (rounds - 1, (1,)))
        packed = list(pack_pages(plan[:1], send_slot, k_pool, v_pool, groups))
        got = [exchange(packed[0])]
        packed += list(pack_pages(plan[1:], send_slot, k_pool, v_pool, groups))
        tables = (from_page, first_seq, second_seq, offsets)
        k_out, v_out = keep_pages(from_page, k_pool, v_pool)

        hidden = jnp.transpose(embeds, (1, 0, 2)).reshape(seq_dev * steps, width)
        rows = []
        for layer in range(n_layers):
            x = jnp.stack([
                jnp.dot(hidden, w[layer], preferred_element_type=jnp.float32).astype(jnp.bfloat16).reshape(seq_dev, steps * heads, head_dim)
                for w in (w_query, w_key, w_value)
            ])
            x, k_out, v_out, packed = lax.optimization_barrier((x, k_out, v_out, packed))
            x_all = spread(x, groups)
            rows.append(x_all)
            x_all = send_next(x_all, 1)
            acc = attend_pages(code, x_all, k_pool, v_pool, layer, pages_seq)
            mixed = gather_home(merge_chip(acc), x, groups)
            mixed = send_next(mixed, 1 if layer + 1 < n_layers else len(plan))
            if layer == 0:
                k_out, v_out = place_pages(plan[:2], (), seq_dev, *tables, got[:2], [], k_out, v_out)
            mixed = mixed.reshape(seq_dev * steps, heads * head_dim)
            hidden = (hidden.astype(jnp.float32) + jnp.dot(mixed, w_out[layer], preferred_element_type=jnp.float32)).astype(jnp.bfloat16)
            inner = jax.nn.gelu(jnp.dot(hidden, w_up[layer], preferred_element_type=jnp.float32)).astype(jnp.bfloat16)
            hidden = (hidden.astype(jnp.float32) + jnp.dot(inner, w_down[layer], preferred_element_type=jnp.float32)).astype(jnp.bfloat16)
        last_round = (rounds - 1,)
        k_out, v_out = place_pages(
            plan[2:-1], ((0, (), False), (1, last_round, False)), seq_dev, *tables, got[2:-1], rows, k_out, v_out
        )
        k_out, v_out = place_pages(plan[-1:], ((1, last_round, True),), seq_dev, *tables, got[-1:], rows, k_out, v_out)
        hidden = jnp.transpose(hidden.reshape(seq_dev, steps, width), (1, 0, 2))
        done = lax.dynamic_slice(finished, (me * seq_dev,), (seq_dev,)) != 0
        live = jnp.stack([jnp.ones_like(done), ~done])
        hidden = jnp.where(live[:, :, None], hidden, jnp.zeros_like(hidden))
        return hidden, k_out, v_out

    in_specs = (rows_spec, full_spec, full_spec, full_spec, full_spec, full_spec, full_spec, pool_spec, pool_spec, table_spec, table_spec, vec_spec, vec_spec, vec_spec, vec_spec)
    return jax.shard_map(device_fn, mesh=mesh, in_specs=in_specs, out_specs=(rows_spec, pool_spec, pool_spec), check_vma=False)
```

```python
import functools

import jax
import jax.numpy as jnp
from jax import lax
from jax.experimental import pallas as pl
from jax.experimental.pallas import tpu as pltpu
from jax.sharding import PartitionSpec as P

MESH = pl.DeviceIdType.MESH
ANY = pl.BlockSpec(memory_space=pl.ANY)
VMEM = pl.BlockSpec(memory_space=pltpu.VMEM)
SMEM = pl.BlockSpec(memory_space=pltpu.SMEM)
LOW = -1e30


def ring(count, depth, lead, start_in, wait_in, start_out, wait_out):
    def body(i, carry):
        @pl.when(i < count)
        def _():
            @pl.when(i >= depth)
            def _():
                wait_out(i - depth)

            start_in(i)

        @pl.when(i >= lead)
        def _():
            wait_in(i - lead)
            start_out(i - lead)

        return carry

    lax.fori_loop(0, count + lead, body, 0)

    def drain(i, carry):
        wait_out(i)
        return carry

    lax.fori_loop(jnp.maximum(count - depth, 0), count, drain, 0)


def compact(total, flag, value, listed):
    def body(i, count):
        @pl.when(flag(i))
        def _():
            listed[count] = value(i)

        return count + flag(i).astype(jnp.int32)

    return lax.fori_loop(0, total, body, jnp.int32(0))


def pack_kernel(depth, lead, plan, slot_ref, *rest):
    pools = rest[:2]
    outs = rest[2:-4]
    buf, listed, sems_in, sems_out = rest[-4:]
    peers = outs[0].shape[0]
    for r, halves in plan:
        mine, outs = outs[0], outs[1:]
        count = compact(peers, lambda i: slot_ref[r * peers + i] >= 0, lambda i: i, listed)

        def ins(i):
            at = lax.rem(i, depth)
            slot = slot_ref[r * peers + listed[i]]
            return [pltpu.make_async_copy(pools[h].at[slot], buf.at[at, h], sems_in.at[at, h]) for h in halves]

        def puts(i):
            at = lax.rem(i, depth)
            return [pltpu.make_async_copy(buf.at[at, h], mine.at[listed[i], k], sems_out.at[at, h]) for k, h in enumerate(halves)]

        ring(
            count, depth, lead,
            lambda i: [c.start() for c in ins(i)],
            lambda i: [c.wait() for c in ins(i)],
            lambda i: [c.start() for c in puts(i)],
            lambda i: [c.wait() for c in puts(i)],
        )


def pack_pages(plan, send_slot, k_pool, v_pool, peers):
    page = k_pool.shape[1:]
    depth, lead = 24, 12
    total = sum(len(halves) for _, halves in plan)
    return pl.pallas_call(
        functools.partial(pack_kernel, depth, lead, plan),
        out_shape=[jax.ShapeDtypeStruct((peers, len(halves)) + page, k_pool.dtype) for _, halves in plan],
        in_specs=[SMEM, ANY, ANY],
        out_specs=[ANY] * len(plan),
        scratch_shapes=[
            pltpu.VMEM((depth, 2) + page, k_pool.dtype),
            pltpu.SMEM((peers,), jnp.int32),
            pltpu.SemaphoreType.DMA((depth, 2)),
            pltpu.SemaphoreType.DMA((depth, 2)),
        ],
        cost_estimate=pl.CostEstimate(flops=10 ** 8 * total, bytes_accessed=2 ** 21 * total, transcendentals=0),
        name="pack_pages",
    )(send_slot, k_pool, v_pool)


def keep_kernel(depth, lead, from_ref, k_ref, v_ref, k_out, v_out, buf, listed, sems_in, sems_out):
    count = compact(from_ref.shape[0], lambda i: from_ref[i] < 0, lambda i: i, listed)

    def ins(i):
        at = lax.rem(i, depth)
        return [pltpu.make_async_copy(ref.at[listed[i]], buf.at[at, h], sems_in.at[at, h]) for h, ref in enumerate((k_ref, v_ref))]

    def outs(i):
        at = lax.rem(i, depth)
        return [pltpu.make_async_copy(buf.at[at, h], ref.at[listed[i]], sems_out.at[at, h]) for h, ref in enumerate((k_out, v_out))]

    ring(
        count, depth, lead,
        lambda i: [c.start() for c in ins(i)],
        lambda i: [c.wait() for c in ins(i)],
        lambda i: [c.start() for c in outs(i)],
        lambda i: [c.wait() for c in outs(i)],
    )


def keep_pages(from_page, k_pool, v_pool):
    depth, lead = 24, 12
    return pl.pallas_call(
        functools.partial(keep_kernel, depth, lead),
        out_shape=[jax.ShapeDtypeStruct(k_pool.shape, k_pool.dtype)] * 2,
        in_specs=[SMEM] + [ANY] * 2,
        out_specs=[ANY] * 2,
        scratch_shapes=[
            pltpu.VMEM((depth, 2) + k_pool.shape[1:], k_pool.dtype),
            pltpu.SMEM((k_pool.shape[0],), jnp.int32),
            pltpu.SemaphoreType.DMA((depth, 2)),
            pltpu.SemaphoreType.DMA((depth, 2)),
        ],
        cost_estimate=pl.CostEstimate(flops=10 ** 9, bytes_accessed=2 ** 25, transcendentals=0),
        name="keep_pages",
    )(from_page, k_pool, v_pool)


def place_kernel(depth, lead, plan, patches, seq_dev, n_rows, from_ref, first_ref, second_ref, offset_ref, *rest):
    arrived, rest = rest[:len(plan)], rest[len(plan):]
    rows = rest[:n_rows]
    k_out, v_out, buf, listed, sems_in, sems_out, staged, entries, sem_row = rest[n_rows + 2:]
    pools = (k_out, v_out)
    peers = arrived[0].shape[0]
    slots, n_batch = from_ref.shape[0], offset_ref.shape[0]
    heads = k_out.shape[3]

    def came(slot, r):
        return (from_ref[slot] >= r * peers) & (from_ref[slot] < (r + 1) * peers)

    def fetch(at, seq, step, h):
        home, place = seq // seq_dev, lax.rem(seq, seq_dev)
        return [
            pltpu.make_async_copy(
                x.at[lax.rem(home, 2), home // 2, 1 + h, place, pl.ds(step * heads, heads)], staged.at[at, layer], sem_row.at[0]
            )
            for layer, x in enumerate(rows)
        ]

    ends = []
    found = jnp.int32(0)
    for h, rounds, inside in patches:
        def collect(slot, count):
            hit = jnp.bool_(False)
            for r in rounds:
                hit = hit | came(slot, r)
            for step, ref in enumerate((first_ref, second_ref)):
                seq = ref[slot]
                take = (seq >= 0) & (hit == inside)

                @pl.when(take)
                def _():
                    entries[count] = (slot * 2 + step) * n_batch + seq
                    for c in fetch(count, seq, step, h):
                        c.start()

                count = count + take.astype(jnp.int32)
            return count

        found = lax.fori_loop(0, slots, collect, found)
        ends.append(found)

    for part, (r, halves) in enumerate(plan):
        count = compact(slots, lambda i: came(i, r), lambda i: i, listed)

        def ins(i):
            at = lax.rem(i, depth)
            line = from_ref[listed[i]] - r * peers
            return [pltpu.make_async_copy(arrived[part].at[line, k], buf.at[at, h], sems_in.at[at, h]) for k, h in enumerate(halves)]

        def outs(i):
            at = lax.rem(i, depth)
            return [pltpu.make_async_copy(buf.at[at, h], pools[h].at[listed[i]], sems_out.at[at, h]) for h in halves]

        ring(
            count, depth, lead,
            lambda i: [c.start() for c in ins(i)],
            lambda i: [c.wait() for c in ins(i)],
            lambda i: [c.start() for c in outs(i)],
            lambda i: [c.wait() for c in outs(i)],
        )

    if patches:
        def fetched(i, carry):
            for c in fetch(i, 0, 0, 0):
                c.wait()
            return carry

        lax.fori_loop(0, found, fetched, 0)
        begin = jnp.int32(0)
        for (h, _, _), end in zip(patches, ends):
            def row_outs(i):
                entry = entries[i]
                seq, at = lax.rem(entry, n_batch), entry // n_batch
                slot, step = at // 2, lax.rem(at, 2)
                return [
                    pltpu.make_async_copy(staged.at[i, layer], pools[h].at[slot, layer, offset_ref[seq] + step], sem_row.at[1])
                    for layer in range(n_rows)
                ]

            def start(i, carry):
                for c in row_outs(i):
                    c.start()
                return carry

            lax.fori_loop(begin, end, start, 0)
            begin = end

        def written(i, carry):
            for layer in range(n_rows):
                pltpu.make_async_copy(staged.at[i, layer], k_out.at[0, layer, 0], sem_row.at[1]).wait()
            return carry

        lax.fori_loop(0, found, written, 0)


def place_pages(plan, patches, seq_dev, from_page, first_seq, second_seq, offsets, arrived, rows, k_out, v_out):
    depth, lead = 24, 12
    first_pool = 4 + len(arrived) + len(rows)
    most = max(2 * len(patches) * k_out.shape[0], 1)
    return pl.pallas_call(
        functools.partial(place_kernel, depth, lead, plan, patches, seq_dev, len(rows)),
        out_shape=[jax.ShapeDtypeStruct(k_out.shape, k_out.dtype)] * 2,
        in_specs=[SMEM] * 4 + [ANY] * (len(arrived) + len(rows) + 2),
        out_specs=[ANY] * 2,
        scratch_shapes=[
            pltpu.VMEM((depth, 2) + k_out.shape[1:], k_out.dtype),
            pltpu.SMEM((k_out.shape[0],), jnp.int32),
            pltpu.SemaphoreType.DMA((depth, 2)),
            pltpu.SemaphoreType.DMA((depth, 2)),
            pltpu.VMEM((most, max(len(rows), 1)) + k_out.shape[3:], k_out.dtype),
            pltpu.SMEM((most,), jnp.int32),
            pltpu.SemaphoreType.DMA((2,)),
        ],
        input_output_aliases={first_pool: 0, first_pool + 1: 1},
        cost_estimate=pl.CostEstimate(flops=2 * 10 ** 8 * len(arrived), bytes_accessed=2 ** 22 * len(arrived), transcendentals=0),
        name="place_pages",
    )(from_page, first_seq, second_seq, offsets, *arrived, *rows, k_out, v_out)


def attend_kernel(block, pages_seq, seq_dev, page_size, scale, code_ref, x_ref, k_ref, v_ref, acc_ref):
    rows, head_dim = x_ref.shape[-2:]
    heads = k_ref.shape[3]
    chips = acc_ref.shape[1]
    step = pl.program_id(0)

    @pl.when(step == 0)
    def _():
        for core in range(2):
            acc_ref[core, :, :seq_dev] = jnp.zeros((chips, seq_dev, rows, head_dim), jnp.float32)
            lane = lax.broadcasted_iota(jnp.int32, (chips, 1, rows, head_dim), 3)
            acc_ref[core, :, seq_dev:] = jnp.where(lax.rem(lane, 2) == 0, LOW, 0.0)

    row = lax.broadcasted_iota(jnp.int32, (rows, page_size * heads), 0)
    column = lax.broadcasted_iota(jnp.int32, (rows, page_size * heads), 1)
    same_head = lax.rem(row, heads) == lax.rem(column, heads)
    position = jnp.where(same_head, column // heads, page_size)
    lane = lax.broadcasted_iota(jnp.int32, (rows, head_dim), 1)
    found = []
    for s in range(block):
        code = code_ref[step * block + s]
        held = jnp.maximum(code, 0)
        seen = jnp.where(code >= 0, lax.rem(held, 2 * page_size), 0)
        seq = held // (2 * page_size * pages_seq)
        home, place = seq // seq_dev, lax.rem(seq, seq_dev)
        core, chip = lax.rem(home, 2), home // 2
        q = x_ref[core, chip, 0, place]
        keys = k_ref[s, 0].reshape(page_size * heads, head_dim)
        values = v_ref[s, 0].reshape(page_size * heads, head_dim)
        scores = lax.dot_general(q, keys, (((1,), (1,)), ((), ())), preferred_element_type=jnp.float32) * scale
        mask = position < seen
        scores = jnp.where(mask, scores, LOW)
        top = jnp.max(scores, axis=1, keepdims=True)
        weights = jnp.where(mask, jnp.exp(scores - top), 0.0)
        total = jnp.sum(weights, axis=1, keepdims=True)
        high = weights.astype(jnp.bfloat16)
        low = (weights - high.astype(jnp.float32)).astype(jnp.bfloat16)
        mixed = jnp.dot(high, values, preferred_element_type=jnp.float32) + jnp.dot(low, values, preferred_element_type=jnp.float32)
        found.append((core, chip, place, top, total, mixed))
    for core, chip, place, top, total, mixed in found:
        stats = acc_ref[core, chip, seq_dev]
        old_top = jnp.max(jnp.where(lane == 2 * place, stats, LOW), axis=1, keepdims=True)
        old_total = jnp.sum(jnp.where(lane == 2 * place + 1, stats, 0.0), axis=1, keepdims=True)
        new_top = jnp.maximum(top, old_top)
        old_part, new_part = jnp.exp(old_top - new_top), jnp.exp(top - new_top)
        acc_ref[core, chip, place] = acc_ref[core, chip, place] * old_part + mixed * new_part
        new_total = old_total * old_part + total * new_part
        acc_ref[core, chip, seq_dev] = jnp.where(lane == 2 * place, new_top, jnp.where(lane == 2 * place + 1, new_total, stats))


def attend_pages(code, x_all, k_pool, v_pool, layer, pages_seq):
    slots, _, page_size, heads, head_dim = k_pool.shape
    cores, chips, _, seq_dev, rows, _ = x_all.shape
    block = 8
    page_spec = pl.BlockSpec((block, 1, page_size, heads, head_dim), lambda i, c: (i, layer, 0, 0, 0))
    query_spec = pl.BlockSpec((cores, chips, 1, seq_dev, rows, head_dim), lambda i, c: (0,) * 6)
    acc_shape = (cores, chips, seq_dev + 1, rows, head_dim)
    return pl.pallas_call(
        functools.partial(attend_kernel, block, pages_seq, seq_dev, page_size, head_dim ** -0.5),
        out_shape=jax.ShapeDtypeStruct(acc_shape, jnp.float32),
        grid_spec=pltpu.PrefetchScalarGridSpec(
            num_scalar_prefetch=1,
            grid=(slots // block,),
            in_specs=[query_spec, page_spec, page_spec],
            out_specs=pl.BlockSpec(acc_shape, lambda i, c: (0,) * 5),
        ),
        compiler_params=pltpu.CompilerParams(dimension_semantics=("arbitrary",)),
        cost_estimate=pl.CostEstimate(flops=10 ** 9, bytes_accessed=2 * slots * page_size * heads * head_dim * 2, transcendentals=0),
        name="attend_pages",
    )(code, x_all, k_pool, v_pool)


def spread_kernel(n, x_ref, out_ref, held, send_sem, recv_sem, pass_sem, got_sem, copy_sem):
    me = lax.axis_index("kv")
    chips = n // 2
    core, chip = lax.rem(me, 2), me // 2
    barrier = pltpu.get_barrier_semaphore()

    def greet(j, carry):
        pl.semaphore_signal(barrier, inc=1, device_id={"kv": 2 * lax.rem(chip + j, chips) + core}, device_id_type=MESH)
        return carry

    lax.fori_loop(1, chips, greet, 0)
    pl.semaphore_signal(barrier, inc=1, device_id={"kv": me + 1 - 2 * core}, device_id_type=MESH)
    pl.semaphore_wait(barrier, chips)
    spread_body(n, x_ref, out_ref, held, send_sem, recv_sem, pass_sem, got_sem, copy_sem)


def spread_body(n, x_ref, out_ref, held, send_sem, recv_sem, pass_sem, got_sem, copy_sem):
    me = lax.axis_index("kv")
    chips = n // 2
    core, chip = lax.rem(me, 2), me // 2
    other = me + 1 - 2 * core

    def peer(j):
        return 2 * lax.rem(chip + j, chips) + core

    def send(j):
        return pltpu.make_async_remote_copy(
            src_ref=x_ref, dst_ref=held.at[core, chip], send_sem=send_sem.at[j], recv_sem=recv_sem.at[chip],
            device_id={"kv": peer(j)}, device_id_type=MESH,
        )

    def forward(source, at):
        return pltpu.make_async_remote_copy(
            src_ref=source, dst_ref=held.at[core, at], send_sem=pass_sem.at[at], recv_sem=got_sem.at[at],
            device_id={"kv": other}, device_id_type=MESH,
        )

    def start(j, carry):
        send(j).start()
        return carry

    lax.fori_loop(1, chips, start, 0)
    own = forward(x_ref, chip)
    own.start()
    mine = pltpu.make_async_copy(x_ref, out_ref.at[core, chip], copy_sem.at[0])
    mine.start()

    def arrive(j, carry):
        at = lax.rem(chip + chips - j, chips)
        pltpu.make_async_remote_copy(
            src_ref=x_ref, dst_ref=held.at[core, at], send_sem=send_sem.at[j], recv_sem=recv_sem.at[at],
            device_id={"kv": other}, device_id_type=MESH,
        ).wait_recv()
        forward(held.at[core, at], at).start()
        pltpu.make_async_copy(held.at[core, at], out_ref.at[core, at], copy_sem.at[j]).start()
        return carry

    lax.fori_loop(1, chips, arrive, 0)

    def passed(j, carry):
        at = lax.rem(chip + j, chips)
        pltpu.make_async_remote_copy(
            src_ref=x_ref, dst_ref=held.at[1 - core, at], send_sem=pass_sem.at[at], recv_sem=got_sem.at[at],
            device_id={"kv": other}, device_id_type=MESH,
        ).wait_recv()
        pltpu.make_async_copy(held.at[1 - core, at], out_ref.at[1 - core, at], copy_sem.at[chips + j]).start()
        return carry

    lax.fori_loop(0, chips, passed, 0)

    own.wait_send()
    mine.wait()

    def finish(j, carry):
        at = lax.rem(chip + chips - j, chips)
        send(j).wait_send()
        forward(held.at[core, at], at).wait_send()
        pltpu.make_async_copy(held.at[core, at], out_ref.at[core, at], copy_sem.at[j]).wait()
        return carry

    lax.fori_loop(1, chips, finish, 0)

    def written(j, carry):
        at = lax.rem(chip + j, chips)
        pltpu.make_async_copy(held.at[1 - core, at], out_ref.at[1 - core, at], copy_sem.at[chips + j]).wait()
        return carry

    lax.fori_loop(0, chips, written, 0)


def spread(x, n):
    chips = n // 2
    return pl.pallas_call(
        functools.partial(spread_kernel, n),
        out_shape=jax.ShapeDtypeStruct((2, chips) + x.shape, x.dtype),
        in_specs=[VMEM],
        out_specs=ANY,
        scratch_shapes=[
            pltpu.VMEM((2, chips) + x.shape, x.dtype),
            pltpu.SemaphoreType.DMA((chips,)),
            pltpu.SemaphoreType.DMA((chips,)),
            pltpu.SemaphoreType.DMA((chips,)),
            pltpu.SemaphoreType.DMA((chips,)),
            pltpu.SemaphoreType.DMA((n,)),
        ],
        compiler_params=pltpu.CompilerParams(collective_id=0, has_side_effects=True),
        name="spread_queries",
    )(x)


def lane_before(x):
    return pltpu.roll(x, x.shape[1] - 1, 1)


def merge_chip_kernel(acc_ref, sums_ref, near, send_sem, recv_sem):
    me = lax.axis_index("kv")
    core = lax.rem(me, 2)
    other = me + 1 - 2 * core
    chips, blocks, rows, head_dim = near.shape
    seq_dev = blocks - 1

    barrier = pltpu.get_barrier_semaphore()
    pl.semaphore_signal(barrier, inc=1, device_id={"kv": other}, device_id_type=MESH)
    pl.semaphore_wait(barrier, 1)

    swap = pltpu.make_async_remote_copy(
        src_ref=acc_ref.at[1 - core], dst_ref=near, send_sem=send_sem.at[0], recv_sem=recv_sem.at[0],
        device_id={"kv": other}, device_id_type=MESH,
    )
    swap.start()
    even = lax.rem(lax.broadcasted_iota(jnp.int32, (rows, head_dim), 1), 2) == 0
    swap.wait_recv()

    def merge(at, carry):
        mine, theirs = acc_ref[core, at, seq_dev], near[at, seq_dev]
        top = jnp.maximum(mine, theirs)
        a, b = jnp.exp(mine - top), jnp.exp(theirs - top)
        total = a * lane_before(mine) + b * lane_before(theirs)
        sums_ref[at, seq_dev] = jnp.where(even, top, pltpu.roll(total, 1, 1))
        for i in range(seq_dev):
            sums_ref[at, i] = a[:, 2 * i:2 * i + 1] * acc_ref[core, at, i] + b[:, 2 * i:2 * i + 1] * near[at, i]
        return carry

    lax.fori_loop(0, chips, merge, 0)
    swap.wait_send()


def merge_chip(acc):
    blocks = acc.shape[1:]
    return pl.pallas_call(
        merge_chip_kernel,
        out_shape=jax.ShapeDtypeStruct(blocks, acc.dtype),
        in_specs=[VMEM],
        out_specs=VMEM,
        scratch_shapes=[
            pltpu.VMEM(blocks, acc.dtype),
            pltpu.SemaphoreType.DMA((1,)),
            pltpu.SemaphoreType.DMA((1,)),
        ],
        compiler_params=pltpu.CompilerParams(collective_id=2, has_side_effects=True),
        cost_estimate=pl.CostEstimate(flops=10 ** 9, bytes_accessed=2 ** 23, transcendentals=0),
        name="merge_chip",
    )(acc)


def layer_kernel(n, scale, layer, follow, *refs):
    sums_ref, x_ref, hid_ref, chunk_ref, wo_ref, wu_ref, wd_ref = refs[:7]
    refs = refs[7:]
    if follow:
        proj, refs = refs[:3], refs[3:]
    hid_out, got_ref = refs[:2]
    refs = refs[2:]
    if follow:
        x_out, all_out = refs[:2]
        refs = refs[2:]
    held, o_scr, rows_scr, mid_scr, acc_scr, wide, up, down, wide_sem, up_sem, down_sem, send_sem, recv_sem, page_send, page_recv = refs[:15]
    refs = refs[15:]
    me = lax.axis_index("kv")
    _, seq_dev, rows, head_dim = x_ref.shape
    heads = rows // 2
    chips = n // 2
    core, chip = lax.rem(me, 2), me // 2
    hid_rows, width = hid_ref.shape
    tile, up_tile = wide.shape[2], up.shape[2]
    wide_slots, up_slots = wide.shape[0], up.shape[0]
    n_wide, n_up = width // tile, wu_ref.shape[2] // up_tile

    def peer(j):
        return 2 * lax.rem(chip + j, chips) + core

    def anyone(j):
        return lax.rem(me + j, n)

    barrier = pltpu.get_barrier_semaphore()

    def greet(j, carry):
        pl.semaphore_signal(barrier, inc=1, device_id={"kv": anyone(j)}, device_id_type=MESH)
        return carry

    lax.fori_loop(1, n, greet, 0)

    def wide_copy(w, at, t, slot):
        return pltpu.make_async_copy(w.at[at, :, pl.ds(pl.multiple_of(t * tile, tile), tile)], wide.at[slot], wide_sem.at[slot])

    def up_copy(t):
        slot = lax.rem(t, up_slots)
        return pltpu.make_async_copy(wu_ref.at[layer, :, pl.ds(pl.multiple_of(t * up_tile, up_tile), up_tile)], up.at[slot], up_sem.at[slot])

    def down_copy(t):
        slot = lax.rem(t, up_slots)
        return pltpu.make_async_copy(wd_ref.at[layer, pl.ds(pl.multiple_of(t * up_tile, up_tile), up_tile)], down.at[slot], down_sem.at[slot])

    for t in range(n_wide):
        wide_copy(wo_ref, layer, t, t).start()
    for t in range(up_slots):
        up_copy(t).start()
        down_copy(t).start()
    pl.semaphore_wait(barrier, n - 1)

    def send(j):
        return pltpu.make_async_remote_copy(
            src_ref=sums_ref.at[lax.rem(chip + j, chips)], dst_ref=held.at[chip], send_sem=send_sem.at[j], recv_sem=recv_sem.at[chip],
            device_id={"kv": peer(j)}, device_id_type=MESH,
        )

    def send_pages(j):
        return pltpu.make_async_remote_copy(
            src_ref=chunk_ref.at[anyone(j)], dst_ref=got_ref.at[me], send_sem=page_send.at[j], recv_sem=page_recv.at[me],
            device_id={"kv": anyone(j)}, device_id_type=MESH,
        )

    def start(j, carry):
        send(j).start()
        return carry

    lax.fori_loop(1, chips, start, 0)

    def start_pages(j, carry):
        send_pages(j).start()
        return carry

    lax.fori_loop(1, n, start_pages, 0)
    held[chip] = sums_ref[chip]

    queries = [x_ref[0, i].astype(jnp.float32) for i in range(seq_dev)]
    second_row = lax.broadcasted_iota(jnp.int32, (rows, 1), 0) >= heads

    def twice(h, i, step):
        x = x_ref[1 + h, i, step * heads:(step + 1) * heads].astype(jnp.float32)
        return jnp.concatenate([x, x], axis=0)

    first = [jnp.sum(queries[i] * twice(0, i, 0), axis=1, keepdims=True) * scale for i in range(seq_dev)]
    second = [
        jnp.where(second_row, jnp.sum(queries[i] * twice(0, i, 1), axis=1, keepdims=True) * scale, LOW)
        for i in range(seq_dev)
    ]

    def arrive(j, carry):
        at = lax.rem(chip + chips - j, chips)
        pltpu.make_async_remote_copy(
            src_ref=sums_ref.at[at], dst_ref=held.at[at], send_sem=send_sem.at[j], recv_sem=recv_sem.at[at],
            device_id={"kv": peer(j)}, device_id_type=MESH,
        ).wait_recv()
        return carry

    lax.fori_loop(1, chips, arrive, 0)

    def highest(j, top):
        return jnp.maximum(top, held[j, seq_dev])

    top_all = lax.fori_loop(0, chips, highest, jnp.full((rows, head_dim), LOW, jnp.float32))
    tops, totals, mixed = [], [], []
    for i in range(seq_dev):
        top = jnp.maximum(jnp.maximum(top_all[:, 2 * i:2 * i + 1], first[i]), second[i])
        p_first, p_second = jnp.exp(first[i] - top), jnp.exp(second[i] - top)
        tops.append(top)
        totals.append(p_first + p_second)
        mixed.append(p_first * twice(1, i, 0) + p_second * twice(1, i, 1))

    def merge(j, carry):
        totals, mixed = carry
        stats = held[j, seq_dev]
        new_totals, new_mixed = [], []
        for i in range(seq_dev):
            weight = jnp.exp(stats[:, 2 * i:2 * i + 1] - tops[i])
            new_totals.append(totals[i] + weight * stats[:, 2 * i + 1:2 * i + 2])
            new_mixed.append(mixed[i] + weight * held[j, i])
        return tuple(new_totals), tuple(new_mixed)

    totals, mixed = lax.fori_loop(0, chips, merge, (tuple(totals), tuple(mixed)))
    for i in range(seq_dev):
        o_scr[i * rows:(i + 1) * rows] = (mixed[i] / totals[i]).astype(jnp.bfloat16).astype(jnp.float32)
    for h in range(heads):
        rows_scr[:, h * head_dim:(h + 1) * head_dim] = o_scr[pl.ds(h, hid_rows, stride=heads), :].astype(jnp.bfloat16)

    def add_out(t, carry):
        wide_copy(wo_ref, layer, t, t).wait()
        cut = pl.ds(pl.multiple_of(t * tile, tile), tile)
        part = jnp.dot(rows_scr[...], wide[t], preferred_element_type=jnp.float32)
        mid_scr[:, cut] = (hid_ref[:, cut].astype(jnp.float32) + part).astype(jnp.bfloat16)
        return carry

    lax.fori_loop(0, n_wide, add_out, 0)
    if follow:
        for t in range(wide_slots):
            wide_copy(proj[t // n_wide], layer + 1, t % n_wide, t).start()
    acc_scr[...] = jnp.zeros_like(acc_scr)

    def mlp(t, carry):
        slot = lax.rem(t, up_slots)
        up_copy(t).wait()
        inner = jax.nn.gelu(jnp.dot(mid_scr[...], up[slot], preferred_element_type=jnp.float32)).astype(jnp.bfloat16)
        down_copy(t).wait()
        acc_scr[...] += jnp.dot(inner, down[slot], preferred_element_type=jnp.float32)

        @pl.when(t + up_slots < n_up)
        def _():
            up_copy(t + up_slots).start()
            down_copy(t + up_slots).start()

        return carry

    lax.fori_loop(0, n_up, mlp, 0)
    hid_out[...] = (mid_scr[...].astype(jnp.float32) + acc_scr[...]).astype(jnp.bfloat16)

    if follow:
        xs, all_held, pass_send, pass_recv, spread_send, spread_recv, copy_sem = refs
        other = me + 1 - 2 * core
        for m in range(3):
            def project(t, carry):
                slot = lax.rem(m * n_wide + t, wide_slots)
                wide_copy(proj[m], layer + 1, t, slot).wait()
                part = jnp.dot(hid_out[...], wide[slot], preferred_element_type=jnp.float32)
                acc_scr[:, pl.ds(pl.multiple_of(t * tile, tile), tile)] = part
                if m < 2:
                    wide_copy(proj[m + 1], layer + 1, t, slot).start()
                return carry

            lax.fori_loop(0, n_wide, project, 0)
            for h in range(heads):
                o_scr[pl.ds(h, hid_rows, stride=heads), :] = acc_scr[:, h * head_dim:(h + 1) * head_dim]
            for i in range(seq_dev):
                xs[m, i] = o_scr[i * rows:(i + 1) * rows].astype(jnp.bfloat16)
        x_out[...] = xs[...]
        spread_body(n, xs, all_out, all_held, spread_send, spread_recv, pass_send, pass_recv, copy_sem)

    def finish(j, carry):
        send(j).wait_send()
        return carry

    lax.fori_loop(1, chips, finish, 0)

    def pages_came(j, carry):
        at = lax.rem(me + n - j, n)
        pltpu.make_async_remote_copy(
            src_ref=chunk_ref.at[at], dst_ref=got_ref.at[at], send_sem=page_send.at[j], recv_sem=page_recv.at[at],
            device_id={"kv": anyone(j)}, device_id_type=MESH,
        ).wait_recv()
        send_pages(j).wait_send()
        return carry

    lax.fori_loop(1, n, pages_came, 0)


def end_layer(sums, x, hidden, chunk, w_out, w_up, w_down, proj, layer, n):
    chips = n // 2
    hid_rows, width = hidden.shape
    seq_dev, rows, head_dim = x.shape[1:]
    follow = bool(proj)
    tile, up_slots = 512, 3
    wide_slots = width // tile
    out_shape = [jax.ShapeDtypeStruct(hidden.shape, hidden.dtype), jax.ShapeDtypeStruct(chunk.shape, chunk.dtype)]
    out_specs = [VMEM, ANY]
    scratch = [
        pltpu.VMEM(sums.shape, sums.dtype),
        pltpu.VMEM((seq_dev * rows, head_dim), jnp.float32),
        pltpu.VMEM(hidden.shape, jnp.bfloat16),
        pltpu.VMEM(hidden.shape, jnp.bfloat16),
        pltpu.VMEM(hidden.shape, jnp.float32),
        pltpu.VMEM((wide_slots, width, tile), w_out.dtype),
        pltpu.VMEM((up_slots, width, tile), w_up.dtype),
        pltpu.VMEM((up_slots, tile, width), w_down.dtype),
        pltpu.SemaphoreType.DMA((wide_slots,)),
        pltpu.SemaphoreType.DMA((up_slots,)),
        pltpu.SemaphoreType.DMA((up_slots,)),
        pltpu.SemaphoreType.DMA((chips,)),
        pltpu.SemaphoreType.DMA((chips,)),
        pltpu.SemaphoreType.DMA((n,)),
        pltpu.SemaphoreType.DMA((n,)),
    ]
    if follow:
        spread_shape = (2, chips) + x.shape
        out_shape += [jax.ShapeDtypeStruct(x.shape, x.dtype), jax.ShapeDtypeStruct(spread_shape, x.dtype)]
        out_specs += [VMEM, ANY]
        scratch += [pltpu.VMEM(x.shape, x.dtype), pltpu.VMEM(spread_shape, x.dtype)]
        scratch += [pltpu.SemaphoreType.DMA((chips,))] * 4 + [pltpu.SemaphoreType.DMA((n,))]
    return pl.pallas_call(
        functools.partial(layer_kernel, n, head_dim ** -0.5, layer, follow),
        out_shape=out_shape,
        in_specs=[VMEM] * 3 + [ANY] * (4 + len(proj)),
        out_specs=out_specs,
        scratch_shapes=scratch,
        compiler_params=pltpu.CompilerParams(collective_id=3 + layer, has_side_effects=True),
        cost_estimate=pl.CostEstimate(flops=10 ** 10, bytes_accessed=2 ** 27, transcendentals=0),
        name="end_layer",
    )(sums, x, hidden, chunk, w_out, w_up, w_down, *proj)


def solution(mesh):
    groups = mesh.shape['kv']
    rows_spec = P(None, ('rep', 'kv'), None)
    pool_spec = P(('rep', 'kv'))
    table_spec = P('rep', None)
    vec_spec = P('rep')
    full_spec = P()

    def device_fn(embeds, w_query, w_key, w_value, w_out, w_up, w_down, k_pool, v_pool, old_table, new_table, seq_len, finished, mig_src, mig_dst):
        me = lax.axis_index('kv')
        slots, n_layers, page_size, heads, head_dim = k_pool.shape
        steps, seq_dev, width = embeds.shape
        n_batch, pages_seq = old_table.shape
        n_mig = mig_src.shape[0]
        rounds = 4 * n_mig // (groups * groups)
        base = me * slots
        local = jnp.arange(slots, dtype=jnp.int32)
        active = finished == 0
        last = pages_seq - 1

        def find(match, value):
            return jnp.max(jnp.where(match, value, -1), axis=1)

        flat = old_table.reshape(-1)
        place = jnp.arange(n_batch * pages_seq, dtype=jnp.int32)
        seen = jnp.clip(seq_len[:, None] - jnp.arange(pages_seq, dtype=jnp.int32)[None, :] * page_size, 0, page_size).reshape(-1)
        code = find(flat[None, :] - base == local[:, None], (place * (2 * page_size) + seen)[None, :])

        src_dev, dst_dev = mig_src // slots, mig_dst // slots
        pair = src_dev * groups + dst_dev
        entry = jnp.arange(n_mig, dtype=jnp.int32)
        rank = jnp.sum((pair[None, :] == pair[:, None]) & (entry[None, :] < entry[:, None]), axis=1, dtype=jnp.int32)
        lines = jnp.arange(rounds * groups, dtype=jnp.int32)
        send_slot = find(
            ((rank * groups + dst_dev)[None, :] == lines[:, None]) & (src_dev == me)[None, :], (mig_src - src_dev * slots)[None, :]
        )
        from_page = find((mig_dst - base)[None, :] == local[:, None], (rank * groups + src_dev)[None, :])

        seq_ids = jnp.arange(n_batch, dtype=jnp.int32)
        owner_old = find((old_table[:, last] - base)[None, :] == local[:, None], seq_ids[None, :])
        owner_new = find(((new_table[:, last] - base)[None, :] == local[:, None]) & active[None, :], seq_ids[None, :])
        first_seq = jnp.where(from_page >= 0, owner_new, owner_old)
        second_seq = owner_new
        offsets = lax.rem(seq_len, page_size)

        def exchange(block):
            return lax.all_to_all(block, 'kv', 0, 0, tiled=True)

        def send_next(value, count):
            for block in packed[len(got):len(got) + count]:
                block, value = lax.optimization_barrier((block, value))
                got.append(exchange(block))
            return value

        plan = ((0, (0,)), (0, (1,))) + tuple((r, (0, 1)) for r in range(1, rounds - 1)) + ((rounds - 1, (0,)), (rounds - 1, (1,)))
        packed = list(pack_pages(plan[:1], send_slot, k_pool, v_pool, groups))
        got = [exchange(packed[0])]
        packed += list(pack_pages(plan[1:], send_slot, k_pool, v_pool, groups))
        tables = (from_page, first_seq, second_seq, offsets)
        k_out, v_out = keep_pages(from_page, k_pool, v_pool)

        hidden = jnp.transpose(embeds, (1, 0, 2)).reshape(seq_dev * steps, width)
        x = jnp.stack([
            jnp.dot(hidden, w[0], preferred_element_type=jnp.float32).astype(jnp.bfloat16).reshape(seq_dev, steps * heads, head_dim)
            for w in (w_query, w_key, w_value)
        ])
        x, k_out, v_out, packed = lax.optimization_barrier((x, k_out, v_out, packed))
        x_all = spread(x, groups)
        rows = []
        for layer in range(n_layers):
            rows.append(x_all)
            x_all = send_next(x_all, 1)
            sums = merge_chip(attend_pages(code, x_all, k_pool, v_pool, layer, pages_seq))
            if layer:
                k_out, v_out = place_pages(plan[:3], (), seq_dev, *tables, got[:3], [], k_out, v_out)
                sums, k_out, v_out = lax.optimization_barrier((sums, k_out, v_out))
            follow = (w_query, w_key, w_value) if layer + 1 < n_layers else ()
            hidden, pages, *ahead = end_layer(sums, x, hidden, packed[len(got)], w_out, w_up, w_down, follow, layer, groups)
            got.append(pages)
            if ahead:
                x, x_all = ahead
        everything = ((0, (), False), (1, (), False))
        k_out, v_out = place_pages(plan[3:], everything, seq_dev, *tables, got[3:], rows, k_out, v_out)
        hidden = jnp.transpose(hidden.reshape(seq_dev, steps, width), (1, 0, 2))
        done = lax.dynamic_slice(finished, (me * seq_dev,), (seq_dev,)) != 0
        live = jnp.stack([jnp.ones_like(done), ~done])
        hidden = jnp.where(live[:, :, None], hidden, jnp.zeros_like(hidden))
        return hidden, k_out, v_out

    in_specs = (rows_spec, full_spec, full_spec, full_spec, full_spec, full_spec, full_spec, pool_spec, pool_spec, table_spec, table_spec, vec_spec, vec_spec, vec_spec, vec_spec)
    return jax.shard_map(device_fn, mesh=mesh, in_specs=in_specs, out_specs=(rows_spec, pool_spec, pool_spec), check_vma=False)
```

```python
import functools

import jax
import jax.numpy as jnp
from jax import lax
from jax.experimental import pallas as pl
from jax.experimental.pallas import tpu as pltpu
from jax.sharding import PartitionSpec as P

MESH = pl.DeviceIdType.MESH
ANY = pl.BlockSpec(memory_space=pl.ANY)
VMEM = pl.BlockSpec(memory_space=pltpu.VMEM)
SMEM = pl.BlockSpec(memory_space=pltpu.SMEM)
LOW = -1e30


def chip_offsets(chips):
    side = 1
    while side * side < chips:
        side += 1
    if side * side != chips:
        return [(j, 0) for j in range(1, chips)], chips

    def near(d):
        d %= side
        return d if 2 * d <= side else d - side

    def cost(offset):
        x, y = near(offset[0]), near(offset[1])
        return (x == 0 or y == 0, 2 * abs(x) == side or 2 * abs(y) == side, x == 0, abs(x) + abs(y), abs(x), abs(y), x * y < 0, x)

    every = [(x, y) for x in range(side) for y in range(side) if x or y]
    return sorted(every, key=cost), side


def chip_at(chip, offset, side, chips):
    x, y = offset
    return lax.rem(chip // side + y, chips // side) * side + lax.rem(lax.rem(chip, side) + x, side)


def chip_from(chip, offset, side, chips):
    x, y = offset
    return chip_at(chip, ((side - x) % side, (chips // side - y) % (chips // side)), side, chips)


def ring(count, depth, lead, start_in, wait_in, start_out, wait_out):
    def body(i, carry):
        @pl.when(i < count)
        def _():
            @pl.when(i >= depth)
            def _():
                wait_out(i - depth)

            start_in(i)

        @pl.when(i >= lead)
        def _():
            wait_in(i - lead)
            start_out(i - lead)

        return carry

    lax.fori_loop(0, count + lead, body, 0)

    def drain(i, carry):
        wait_out(i)
        return carry

    lax.fori_loop(jnp.maximum(count - depth, 0), count, drain, 0)


def compact(total, flag, value, listed):
    def body(i, count):
        @pl.when(flag(i))
        def _():
            listed[count] = value(i)

        return count + flag(i).astype(jnp.int32)

    return lax.fori_loop(0, total, body, jnp.int32(0))


def pack_kernel(depth, lead, plan, slot_ref, *rest):
    pools = rest[:2]
    outs = rest[2:-4]
    buf, listed, sems_in, sems_out = rest[-4:]
    peers = outs[0].shape[0]
    for r, halves in plan:
        mine, outs = outs[0], outs[1:]
        count = compact(peers, lambda i: slot_ref[r * peers + i] >= 0, lambda i: i, listed)

        def ins(i):
            at = lax.rem(i, depth)
            slot = slot_ref[r * peers + listed[i]]
            return [pltpu.make_async_copy(pools[h].at[slot], buf.at[at, h], sems_in.at[at, h]) for h in halves]

        def puts(i):
            at = lax.rem(i, depth)
            return [pltpu.make_async_copy(buf.at[at, h], mine.at[listed[i], k], sems_out.at[at, h]) for k, h in enumerate(halves)]

        ring(
            count, depth, lead,
            lambda i: [c.start() for c in ins(i)],
            lambda i: [c.wait() for c in ins(i)],
            lambda i: [c.start() for c in puts(i)],
            lambda i: [c.wait() for c in puts(i)],
        )


def pack_pages(plan, send_slot, k_pool, v_pool, peers):
    page = k_pool.shape[1:]
    depth, lead = 24, 12
    total = sum(len(halves) for _, halves in plan)
    return pl.pallas_call(
        functools.partial(pack_kernel, depth, lead, plan),
        out_shape=[jax.ShapeDtypeStruct((peers, len(halves)) + page, k_pool.dtype) for _, halves in plan],
        in_specs=[SMEM, ANY, ANY],
        out_specs=[ANY] * len(plan),
        scratch_shapes=[
            pltpu.VMEM((depth, 2) + page, k_pool.dtype),
            pltpu.SMEM((peers,), jnp.int32),
            pltpu.SemaphoreType.DMA((depth, 2)),
            pltpu.SemaphoreType.DMA((depth, 2)),
        ],
        cost_estimate=pl.CostEstimate(flops=10 ** 8 * total, bytes_accessed=2 ** 21 * total, transcendentals=0),
        name="pack_pages",
    )(send_slot, k_pool, v_pool)


def keep_kernel(depth, lead, from_ref, k_ref, v_ref, k_out, v_out, buf, listed, sems_in, sems_out):
    count = compact(from_ref.shape[0], lambda i: from_ref[i] < 0, lambda i: i, listed)

    def ins(i):
        at = lax.rem(i, depth)
        return [pltpu.make_async_copy(ref.at[listed[i]], buf.at[at, h], sems_in.at[at, h]) for h, ref in enumerate((k_ref, v_ref))]

    def outs(i):
        at = lax.rem(i, depth)
        return [pltpu.make_async_copy(buf.at[at, h], ref.at[listed[i]], sems_out.at[at, h]) for h, ref in enumerate((k_out, v_out))]

    ring(
        count, depth, lead,
        lambda i: [c.start() for c in ins(i)],
        lambda i: [c.wait() for c in ins(i)],
        lambda i: [c.start() for c in outs(i)],
        lambda i: [c.wait() for c in outs(i)],
    )


def keep_pages(from_page, k_pool, v_pool):
    depth, lead = 24, 12
    return pl.pallas_call(
        functools.partial(keep_kernel, depth, lead),
        out_shape=[jax.ShapeDtypeStruct(k_pool.shape, k_pool.dtype)] * 2,
        in_specs=[SMEM] + [ANY] * 2,
        out_specs=[ANY] * 2,
        scratch_shapes=[
            pltpu.VMEM((depth, 2) + k_pool.shape[1:], k_pool.dtype),
            pltpu.SMEM((k_pool.shape[0],), jnp.int32),
            pltpu.SemaphoreType.DMA((depth, 2)),
            pltpu.SemaphoreType.DMA((depth, 2)),
        ],
        cost_estimate=pl.CostEstimate(flops=10 ** 9, bytes_accessed=2 ** 25, transcendentals=0),
        name="keep_pages",
    )(from_page, k_pool, v_pool)


def place_kernel(depth, lead, plan, from_ref, *rest):
    arrived, rest = rest[:len(plan)], rest[len(plan):]
    k_out, v_out, buf, listed, sems_in, sems_out = rest[2:]
    pools = (k_out, v_out)
    peers = arrived[0].shape[0]
    slots = from_ref.shape[0]
    for part, (r, halves) in enumerate(plan):
        count = compact(slots, lambda i: (from_ref[i] >= r * peers) & (from_ref[i] < (r + 1) * peers), lambda i: i, listed)

        def ins(i):
            at = lax.rem(i, depth)
            line = from_ref[listed[i]] - r * peers
            return [pltpu.make_async_copy(arrived[part].at[line, k], buf.at[at, h], sems_in.at[at, h]) for k, h in enumerate(halves)]

        def outs(i):
            at = lax.rem(i, depth)
            return [pltpu.make_async_copy(buf.at[at, h], pools[h].at[listed[i]], sems_out.at[at, h]) for h in halves]

        ring(
            count, depth, lead,
            lambda i: [c.start() for c in ins(i)],
            lambda i: [c.wait() for c in ins(i)],
            lambda i: [c.start() for c in outs(i)],
            lambda i: [c.wait() for c in outs(i)],
        )


def place_pages(plan, from_page, arrived, k_out, v_out):
    depth, lead = 24, 12
    return pl.pallas_call(
        functools.partial(place_kernel, depth, lead, plan),
        out_shape=[jax.ShapeDtypeStruct(k_out.shape, k_out.dtype)] * 2,
        in_specs=[SMEM] + [ANY] * (len(arrived) + 2),
        out_specs=[ANY] * 2,
        scratch_shapes=[
            pltpu.VMEM((depth, 2) + k_out.shape[1:], k_out.dtype),
            pltpu.SMEM((k_out.shape[0],), jnp.int32),
            pltpu.SemaphoreType.DMA((depth, 2)),
            pltpu.SemaphoreType.DMA((depth, 2)),
        ],
        input_output_aliases={1 + len(arrived): 0, 2 + len(arrived): 1},
        cost_estimate=pl.CostEstimate(flops=2 * 10 ** 8 * len(arrived), bytes_accessed=2 ** 22 * len(arrived), transcendentals=0),
        name="place_pages",
    )(from_page, *arrived, k_out, v_out)


def close_kernel(seq_dev, first_line, n_rows, from_ref, first_ref, second_ref, offset_ref, k_came, v_came, *rest):
    rows = rest[:n_rows]
    k_out, v_out, buf, listed, staged, early, late, sems_in, sem_out, sem_row = rest[n_rows + 2:]
    pools, arrived = (k_out, v_out), (k_came, v_came)
    peers = k_came.shape[0]
    slots, n_batch = from_ref.shape[0], offset_ref.shape[0]
    heads = k_out.shape[3]
    most = early.shape[0]

    def ins(i, line):
        return [pltpu.make_async_copy(ref.at[line], buf.at[i, h], sems_in.at[i]) for h, ref in enumerate(arrived)]

    def outs(i, slot):
        return [pltpu.make_async_copy(buf.at[i, h], pools[h].at[slot], sem_out.at[0]) for h in range(2)]

    def fetch(at, seq, step):
        home, place = seq // seq_dev, lax.rem(seq, seq_dev)
        return [
            pltpu.make_async_copy(
                x.at[lax.rem(home, 2), home // 2, 1 + h, place, pl.ds(step * heads, heads)], staged.at[at, layer, h], sem_row.at[0]
            )
            for layer, x in enumerate(rows) for h in range(2)
        ]

    def write(at, slot, layer_offset, sem):
        return [
            pltpu.make_async_copy(staged.at[at, layer, h], pools[h].at[slot, layer, layer_offset], sem_row.at[sem])
            for layer in range(n_rows) for h in range(2)
        ]

    def scan(slot, counts):
        pages, n_early, n_late = counts
        line = from_ref[slot] - first_line
        moved = (line >= 0) & (line < peers)

        @pl.when(moved)
        def _():
            listed[pages] = slot
            for c in ins(pages, line):
                c.start()

        for step, ref in enumerate((first_ref, second_ref)):
            seq = ref[slot]
            entry = (slot * 2 + step) * n_batch + seq

            @pl.when((seq >= 0) & moved)
            def _():
                late[n_late] = entry
                for c in fetch(most - 1 - n_late, seq, step):
                    c.start()

            @pl.when((seq >= 0) & jnp.logical_not(moved))
            def _():
                early[n_early] = entry
                for c in fetch(n_early, seq, step):
                    c.start()

            n_late = n_late + ((seq >= 0) & moved).astype(jnp.int32)
            n_early = n_early + ((seq >= 0) & jnp.logical_not(moved)).astype(jnp.int32)
        return pages + moved.astype(jnp.int32), n_early, n_late

    pages, n_early, n_late = lax.fori_loop(0, slots, scan, (jnp.int32(0), jnp.int32(0), jnp.int32(0)))

    def pass_on(i, carry):
        for c in ins(i, 0):
            c.wait()
        for c in outs(i, listed[i]):
            c.start()
        return carry

    lax.fori_loop(0, pages, pass_on, 0)

    def fetched(i, carry):
        for c in fetch(0, 0, 0):
            c.wait()
        return carry

    lax.fori_loop(0, n_early + n_late, fetched, 0)

    def write_row(entries, at, sem):
        def body(i, carry):
            entry = entries[i]
            seq, where = lax.rem(entry, n_batch), entry // n_batch
            for c in write(at(i), where // 2, offset_ref[seq] + lax.rem(where, 2), sem):
                c.start()
            return carry
        return body

    lax.fori_loop(0, n_early, write_row(early, lambda i: i, 1), 0)

    def placed(i, carry):
        for c in outs(i, 0):
            c.wait()
        return carry

    lax.fori_loop(0, pages, placed, 0)
    lax.fori_loop(0, n_late, write_row(late, lambda i: most - 1 - i, 1), 0)

    def written(i, carry):
        for c in write(0, 0, 0, 1):
            c.wait()
        return carry

    lax.fori_loop(0, n_early + n_late, written, 0)


def close_pools(seq_dev, last_round, from_page, first_seq, second_seq, offsets, arrived, rows, k_out, v_out):
    peers, slots = arrived[0].shape[0], k_out.shape[0]
    first_pool = 6 + len(rows)
    return pl.pallas_call(
        functools.partial(close_kernel, seq_dev, last_round * peers, len(rows)),
        out_shape=[jax.ShapeDtypeStruct(k_out.shape, k_out.dtype)] * 2,
        in_specs=[SMEM] * 4 + [ANY] * (4 + len(rows)),
        out_specs=[ANY] * 2,
        scratch_shapes=[
            pltpu.VMEM((peers, 2) + k_out.shape[1:], k_out.dtype),
            pltpu.SMEM((peers,), jnp.int32),
            pltpu.VMEM((2 * slots, len(rows), 2) + k_out.shape[3:], k_out.dtype),
            pltpu.SMEM((2 * slots,), jnp.int32),
            pltpu.SMEM((2 * slots,), jnp.int32),
            pltpu.SemaphoreType.DMA((peers,)),
            pltpu.SemaphoreType.DMA((1,)),
            pltpu.SemaphoreType.DMA((2,)),
        ],
        input_output_aliases={first_pool: 0, first_pool + 1: 1},
        cost_estimate=pl.CostEstimate(flops=4 * 10 ** 8, bytes_accessed=2 ** 23, transcendentals=0),
        name="close_pools",
    )(from_page, first_seq, second_seq, offsets, *[a.reshape((peers,) + a.shape[2:]) for a in arrived], *rows, k_out, v_out)


def attend_kernel(block, pages_seq, seq_dev, page_size, scale, code_ref, x_ref, k_ref, v_ref, acc_ref):
    rows, head_dim = x_ref.shape[-2:]
    heads = k_ref.shape[3]
    chips = acc_ref.shape[1]
    step = pl.program_id(0)

    @pl.when(step == 0)
    def _():
        for core in range(2):
            acc_ref[core, :, :seq_dev] = jnp.zeros((chips, seq_dev, rows, head_dim), jnp.float32)
            lane = lax.broadcasted_iota(jnp.int32, (chips, 1, rows, head_dim), 3)
            acc_ref[core, :, seq_dev:] = jnp.where(lax.rem(lane, 2) == 0, LOW, 0.0)

    row = lax.broadcasted_iota(jnp.int32, (rows, page_size * heads), 0)
    column = lax.broadcasted_iota(jnp.int32, (rows, page_size * heads), 1)
    same_head = lax.rem(row, heads) == lax.rem(column, heads)
    position = jnp.where(same_head, column // heads, page_size)
    lane = lax.broadcasted_iota(jnp.int32, (rows, head_dim), 1)
    found = []
    for s in range(block):
        code = code_ref[step * block + s]
        held = jnp.maximum(code, 0)
        seen = jnp.where(code >= 0, lax.rem(held, 2 * page_size), 0)
        seq = held // (2 * page_size * pages_seq)
        home, place = seq // seq_dev, lax.rem(seq, seq_dev)
        core, chip = lax.rem(home, 2), home // 2
        q = x_ref[core, chip, 0, place]
        keys = k_ref[s, 0].reshape(page_size * heads, head_dim)
        values = v_ref[s, 0].reshape(page_size * heads, head_dim)
        scores = lax.dot_general(q, keys, (((1,), (1,)), ((), ())), preferred_element_type=jnp.float32) * scale
        mask = position < seen
        scores = jnp.where(mask, scores, LOW)
        top = jnp.max(scores, axis=1, keepdims=True)
        weights = jnp.where(mask, jnp.exp(scores - top), 0.0)
        total = jnp.sum(weights, axis=1, keepdims=True)
        high = weights.astype(jnp.bfloat16)
        low = (weights - high.astype(jnp.float32)).astype(jnp.bfloat16)
        mixed = jnp.dot(high, values, preferred_element_type=jnp.float32) + jnp.dot(low, values, preferred_element_type=jnp.float32)
        found.append((core, chip, place, top, total, mixed))
    for core, chip, place, top, total, mixed in found:
        stats = acc_ref[core, chip, seq_dev]
        old_top = jnp.max(jnp.where(lane == 2 * place, stats, LOW), axis=1, keepdims=True)
        old_total = jnp.sum(jnp.where(lane == 2 * place + 1, stats, 0.0), axis=1, keepdims=True)
        new_top = jnp.maximum(top, old_top)
        old_part, new_part = jnp.exp(old_top - new_top), jnp.exp(top - new_top)
        acc_ref[core, chip, place] = acc_ref[core, chip, place] * old_part + mixed * new_part
        new_total = old_total * old_part + total * new_part
        acc_ref[core, chip, seq_dev] = jnp.where(lane == 2 * place, new_top, jnp.where(lane == 2 * place + 1, new_total, stats))


def attend_pages(code, x_all, k_pool, v_pool, layer, pages_seq):
    slots, _, page_size, heads, head_dim = k_pool.shape
    cores, chips, _, seq_dev, rows, _ = x_all.shape
    block = 8
    page_spec = pl.BlockSpec((block, 1, page_size, heads, head_dim), lambda i, c: (i, layer, 0, 0, 0))
    query_spec = pl.BlockSpec((cores, chips, 1, seq_dev, rows, head_dim), lambda i, c: (0,) * 6)
    acc_shape = (cores, chips, seq_dev + 1, rows, head_dim)
    return pl.pallas_call(
        functools.partial(attend_kernel, block, pages_seq, seq_dev, page_size, head_dim ** -0.5),
        out_shape=jax.ShapeDtypeStruct(acc_shape, jnp.float32),
        grid_spec=pltpu.PrefetchScalarGridSpec(
            num_scalar_prefetch=1,
            grid=(slots // block,),
            in_specs=[query_spec, page_spec, page_spec],
            out_specs=pl.BlockSpec(acc_shape, lambda i, c: (0,) * 5),
        ),
        compiler_params=pltpu.CompilerParams(dimension_semantics=("arbitrary",)),
        cost_estimate=pl.CostEstimate(flops=10 ** 9, bytes_accessed=2 * slots * page_size * heads * head_dim * 2, transcendentals=0),
        name="attend_pages",
    )(code, x_all, k_pool, v_pool)


def spread_kernel(n, x_ref, out_ref, held, send_sem, recv_sem, pass_sem, got_sem, copy_sem):
    me = lax.axis_index("kv")
    chips = n // 2
    core, chip = lax.rem(me, 2), me // 2
    barrier = pltpu.get_barrier_semaphore()

    def greet(j, carry):
        pl.semaphore_signal(barrier, inc=1, device_id={"kv": 2 * lax.rem(chip + j, chips) + core}, device_id_type=MESH)
        return carry

    lax.fori_loop(1, chips, greet, 0)
    pl.semaphore_signal(barrier, inc=1, device_id={"kv": me + 1 - 2 * core}, device_id_type=MESH)
    pl.semaphore_wait(barrier, chips)
    spread_body(n, x_ref, out_ref, held, send_sem, recv_sem, pass_sem, got_sem, copy_sem)


def spread_body(n, x_ref, out_ref, held, send_sem, recv_sem, pass_sem, got_sem, copy_sem):
    me = lax.axis_index("kv")
    chips = n // 2
    core, chip = lax.rem(me, 2), me // 2
    other = me + 1 - 2 * core

    def peer(j):
        return 2 * lax.rem(chip + j, chips) + core

    def send(j):
        return pltpu.make_async_remote_copy(
            src_ref=x_ref, dst_ref=held.at[core, chip], send_sem=send_sem.at[j], recv_sem=recv_sem.at[chip],
            device_id={"kv": peer(j)}, device_id_type=MESH,
        )

    def forward(source, at):
        return pltpu.make_async_remote_copy(
            src_ref=source, dst_ref=held.at[core, at], send_sem=pass_sem.at[at], recv_sem=got_sem.at[at],
            device_id={"kv": other}, device_id_type=MESH,
        )

    offsets, side = chip_offsets(chips)
    for offset in offsets:
        send(lax.rem(chip_at(chip, offset, side, chips) + chips - chip, chips)).start()
    own = forward(x_ref, chip)
    own.start()
    mine = pltpu.make_async_copy(x_ref, out_ref.at[core, chip], copy_sem.at[0])
    mine.start()

    for offset in offsets:
        at = chip_from(chip, offset, side, chips)
        j = lax.rem(chip + chips - at, chips)
        pltpu.make_async_remote_copy(
            src_ref=x_ref, dst_ref=held.at[core, at], send_sem=send_sem.at[j], recv_sem=recv_sem.at[at],
            device_id={"kv": other}, device_id_type=MESH,
        ).wait_recv()
        forward(held.at[core, at], at).start()
        pltpu.make_async_copy(held.at[core, at], out_ref.at[core, at], copy_sem.at[j]).start()

    def passed(j, carry):
        at = lax.rem(chip + j, chips)
        pltpu.make_async_remote_copy(
            src_ref=x_ref, dst_ref=held.at[1 - core, at], send_sem=pass_sem.at[at], recv_sem=got_sem.at[at],
            device_id={"kv": other}, device_id_type=MESH,
        ).wait_recv()
        pltpu.make_async_copy(held.at[1 - core, at], out_ref.at[1 - core, at], copy_sem.at[chips + j]).start()
        return carry

    lax.fori_loop(0, chips, passed, 0)

    own.wait_send()
    mine.wait()

    def finish(j, carry):
        at = lax.rem(chip + chips - j, chips)
        send(j).wait_send()
        forward(held.at[core, at], at).wait_send()
        pltpu.make_async_copy(held.at[core, at], out_ref.at[core, at], copy_sem.at[j]).wait()
        return carry

    lax.fori_loop(1, chips, finish, 0)

    def written(j, carry):
        at = lax.rem(chip + j, chips)
        pltpu.make_async_copy(held.at[1 - core, at], out_ref.at[1 - core, at], copy_sem.at[chips + j]).wait()
        return carry

    lax.fori_loop(0, chips, written, 0)


def spread(x, n):
    chips = n // 2
    return pl.pallas_call(
        functools.partial(spread_kernel, n),
        out_shape=jax.ShapeDtypeStruct((2, chips) + x.shape, x.dtype),
        in_specs=[VMEM],
        out_specs=ANY,
        scratch_shapes=[
            pltpu.VMEM((2, chips) + x.shape, x.dtype),
            pltpu.SemaphoreType.DMA((chips,)),
            pltpu.SemaphoreType.DMA((chips,)),
            pltpu.SemaphoreType.DMA((chips,)),
            pltpu.SemaphoreType.DMA((chips,)),
            pltpu.SemaphoreType.DMA((n,)),
        ],
        compiler_params=pltpu.CompilerParams(collective_id=0, has_side_effects=True),
        name="spread_queries",
    )(x)


def lane_before(x):
    return pltpu.roll(x, x.shape[1] - 1, 1)


def merge_chip_kernel(acc_ref, sums_ref, near, send_sem, recv_sem):
    me = lax.axis_index("kv")
    core = lax.rem(me, 2)
    other = me + 1 - 2 * core
    chips, blocks, rows, head_dim = near.shape
    seq_dev = blocks - 1

    barrier = pltpu.get_barrier_semaphore()
    pl.semaphore_signal(barrier, inc=1, device_id={"kv": other}, device_id_type=MESH)
    pl.semaphore_wait(barrier, 1)

    swap = pltpu.make_async_remote_copy(
        src_ref=acc_ref.at[1 - core], dst_ref=near, send_sem=send_sem.at[0], recv_sem=recv_sem.at[0],
        device_id={"kv": other}, device_id_type=MESH,
    )
    swap.start()
    even = lax.rem(lax.broadcasted_iota(jnp.int32, (rows, head_dim), 1), 2) == 0
    swap.wait_recv()

    def merge(at, carry):
        mine, theirs = acc_ref[core, at, seq_dev], near[at, seq_dev]
        top = jnp.maximum(mine, theirs)
        a, b = jnp.exp(mine - top), jnp.exp(theirs - top)
        total = a * lane_before(mine) + b * lane_before(theirs)
        sums_ref[at, seq_dev] = jnp.where(even, top, pltpu.roll(total, 1, 1))
        for i in range(seq_dev):
            sums_ref[at, i] = a[:, 2 * i:2 * i + 1] * acc_ref[core, at, i] + b[:, 2 * i:2 * i + 1] * near[at, i]
        return carry

    lax.fori_loop(0, chips, merge, 0)
    swap.wait_send()


def merge_chip(acc):
    blocks = acc.shape[1:]
    return pl.pallas_call(
        merge_chip_kernel,
        out_shape=jax.ShapeDtypeStruct(blocks, acc.dtype),
        in_specs=[VMEM],
        out_specs=VMEM,
        scratch_shapes=[
            pltpu.VMEM(blocks, acc.dtype),
            pltpu.SemaphoreType.DMA((1,)),
            pltpu.SemaphoreType.DMA((1,)),
        ],
        compiler_params=pltpu.CompilerParams(collective_id=2, has_side_effects=True),
        cost_estimate=pl.CostEstimate(flops=10 ** 9, bytes_accessed=2 ** 23, transcendentals=0),
        name="merge_chip",
    )(acc)


def layer_kernel(n, scale, layer, follow, *refs):
    sums_ref, x_ref, hid_ref, chunk_ref, wo_ref, wu_ref, wd_ref = refs[:7]
    refs = refs[7:]
    if follow:
        proj, refs = refs[:3], refs[3:]
    hid_out, got_ref = refs[:2]
    refs = refs[2:]
    if follow:
        x_out, all_out = refs[:2]
        refs = refs[2:]
    held, o_scr, rows_scr, mid_scr, acc_scr, wide, up, down, wide_sem, up_sem, down_sem, send_sem, recv_sem, page_send, page_recv = refs[:15]
    refs = refs[15:]
    me = lax.axis_index("kv")
    _, seq_dev, rows, head_dim = x_ref.shape
    heads = rows // 2
    chips = n // 2
    core, chip = lax.rem(me, 2), me // 2
    hid_rows, width = hid_ref.shape
    tile, up_tile = wide.shape[2], up.shape[2]
    wide_slots, up_slots = wide.shape[0], up.shape[0]
    n_wide, n_up = width // tile, wu_ref.shape[2] // up_tile

    def peer(j):
        return 2 * lax.rem(chip + j, chips) + core

    def anyone(j):
        return lax.rem(me + j, n)

    barrier = pltpu.get_barrier_semaphore()

    def greet(j, carry):
        pl.semaphore_signal(barrier, inc=1, device_id={"kv": anyone(j)}, device_id_type=MESH)
        return carry

    lax.fori_loop(1, n, greet, 0)

    def wide_copy(w, at, t, slot):
        return pltpu.make_async_copy(w.at[at, :, pl.ds(pl.multiple_of(t * tile, tile), tile)], wide.at[slot], wide_sem.at[slot])

    def up_copy(t):
        slot = lax.rem(t, up_slots)
        return pltpu.make_async_copy(wu_ref.at[layer, :, pl.ds(pl.multiple_of(t * up_tile, up_tile), up_tile)], up.at[slot], up_sem.at[slot])

    def down_copy(t):
        slot = lax.rem(t, up_slots)
        return pltpu.make_async_copy(wd_ref.at[layer, pl.ds(pl.multiple_of(t * up_tile, up_tile), up_tile)], down.at[slot], down_sem.at[slot])

    for t in range(n_wide):
        wide_copy(wo_ref, layer, t, t).start()
    for t in range(up_slots):
        up_copy(t).start()
        down_copy(t).start()
    pl.semaphore_wait(barrier, n - 1)

    def send(j):
        return pltpu.make_async_remote_copy(
            src_ref=sums_ref.at[lax.rem(chip + j, chips)], dst_ref=held.at[chip], send_sem=send_sem.at[j], recv_sem=recv_sem.at[chip],
            device_id={"kv": peer(j)}, device_id_type=MESH,
        )

    def send_pages(j):
        return pltpu.make_async_remote_copy(
            src_ref=chunk_ref.at[anyone(j)], dst_ref=got_ref.at[me], send_sem=page_send.at[j], recv_sem=page_recv.at[me],
            device_id={"kv": anyone(j)}, device_id_type=MESH,
        )

    offsets, side = chip_offsets(chips)
    for offset in offsets:
        send(lax.rem(chip_at(chip, offset, side, chips) + chips - chip, chips)).start()
    for offset in offsets:
        for other_core in range(2):
            to = 2 * chip_at(chip, offset, side, chips) + lax.rem(core + other_core, 2)
            send_pages(lax.rem(to + n - me, n)).start()
    send_pages(lax.rem(me + 1 - 2 * core + n - me, n)).start()
    held[chip] = sums_ref[chip]

    queries = [x_ref[0, i].astype(jnp.float32) for i in range(seq_dev)]
    second_row = lax.broadcasted_iota(jnp.int32, (rows, 1), 0) >= heads

    def twice(h, i, step):
        x = x_ref[1 + h, i, step * heads:(step + 1) * heads].astype(jnp.float32)
        return jnp.concatenate([x, x], axis=0)

    first = [jnp.sum(queries[i] * twice(0, i, 0), axis=1, keepdims=True) * scale for i in range(seq_dev)]
    second = [
        jnp.where(second_row, jnp.sum(queries[i] * twice(0, i, 1), axis=1, keepdims=True) * scale, LOW)
        for i in range(seq_dev)
    ]

    def arrive(j, carry):
        at = lax.rem(chip + chips - j, chips)
        pltpu.make_async_remote_copy(
            src_ref=sums_ref.at[at], dst_ref=held.at[at], send_sem=send_sem.at[j], recv_sem=recv_sem.at[at],
            device_id={"kv": peer(j)}, device_id_type=MESH,
        ).wait_recv()
        return carry

    lax.fori_loop(1, chips, arrive, 0)

    def highest(j, top):
        return jnp.maximum(top, held[j, seq_dev])

    top_all = lax.fori_loop(0, chips, highest, jnp.full((rows, head_dim), LOW, jnp.float32))
    tops, totals, mixed = [], [], []
    for i in range(seq_dev):
        top = jnp.maximum(jnp.maximum(top_all[:, 2 * i:2 * i + 1], first[i]), second[i])
        p_first, p_second = jnp.exp(first[i] - top), jnp.exp(second[i] - top)
        tops.append(top)
        totals.append(p_first + p_second)
        mixed.append(p_first * twice(1, i, 0) + p_second * twice(1, i, 1))

    def merge(j, carry):
        totals, mixed = carry
        stats = held[j, seq_dev]
        new_totals, new_mixed = [], []
        for i in range(seq_dev):
            weight = jnp.exp(stats[:, 2 * i:2 * i + 1] - tops[i])
            new_totals.append(totals[i] + weight * stats[:, 2 * i + 1:2 * i + 2])
            new_mixed.append(mixed[i] + weight * held[j, i])
        return tuple(new_totals), tuple(new_mixed)

    totals, mixed = lax.fori_loop(0, chips, merge, (tuple(totals), tuple(mixed)))
    for i in range(seq_dev):
        o_scr[i * rows:(i + 1) * rows] = (mixed[i] / totals[i]).astype(jnp.bfloat16).astype(jnp.float32)
    for h in range(heads):
        rows_scr[:, h * head_dim:(h + 1) * head_dim] = o_scr[pl.ds(h, hid_rows, stride=heads), :].astype(jnp.bfloat16)

    def add_out(t, carry):
        wide_copy(wo_ref, layer, t, t).wait()
        cut = pl.ds(pl.multiple_of(t * tile, tile), tile)
        part = jnp.dot(rows_scr[...], wide[t], preferred_element_type=jnp.float32)
        mid_scr[:, cut] = (hid_ref[:, cut].astype(jnp.float32) + part).astype(jnp.bfloat16)
        return carry

    lax.fori_loop(0, n_wide, add_out, 0)
    if follow:
        for t in range(wide_slots):
            wide_copy(proj[t // n_wide], layer + 1, t % n_wide, t).start()
    acc_scr[...] = jnp.zeros_like(acc_scr)

    def mlp(t, carry):
        slot = lax.rem(t, up_slots)
        up_copy(t).wait()
        inner = jax.nn.gelu(jnp.dot(mid_scr[...], up[slot], preferred_element_type=jnp.float32)).astype(jnp.bfloat16)
        down_copy(t).wait()
        acc_scr[...] += jnp.dot(inner, down[slot], preferred_element_type=jnp.float32)

        @pl.when(t + up_slots < n_up)
        def _():
            up_copy(t + up_slots).start()
            down_copy(t + up_slots).start()

        return carry

    lax.fori_loop(0, n_up, mlp, 0)
    hid_out[...] = (mid_scr[...].astype(jnp.float32) + acc_scr[...]).astype(jnp.bfloat16)

    if follow:
        xs, all_held, pass_send, pass_recv, spread_send, spread_recv, copy_sem = refs
        other = me + 1 - 2 * core
        for m in range(3):
            def project(t, carry):
                slot = lax.rem(m * n_wide + t, wide_slots)
                wide_copy(proj[m], layer + 1, t, slot).wait()
                part = jnp.dot(hid_out[...], wide[slot], preferred_element_type=jnp.float32)
                acc_scr[:, pl.ds(pl.multiple_of(t * tile, tile), tile)] = part
                if m < 2:
                    wide_copy(proj[m + 1], layer + 1, t, slot).start()
                return carry

            lax.fori_loop(0, n_wide, project, 0)
            for h in range(heads):
                o_scr[pl.ds(h, hid_rows, stride=heads), :] = acc_scr[:, h * head_dim:(h + 1) * head_dim]
            for i in range(seq_dev):
                xs[m, i] = o_scr[i * rows:(i + 1) * rows].astype(jnp.bfloat16)
        x_out[...] = xs[...]
        spread_body(n, xs, all_out, all_held, spread_send, spread_recv, pass_send, pass_recv, copy_sem)

    def finish(j, carry):
        send(j).wait_send()
        return carry

    lax.fori_loop(1, chips, finish, 0)

    def pages_came(j, carry):
        at = lax.rem(me + n - j, n)
        pltpu.make_async_remote_copy(
            src_ref=chunk_ref.at[at], dst_ref=got_ref.at[at], send_sem=page_send.at[j], recv_sem=page_recv.at[at],
            device_id={"kv": anyone(j)}, device_id_type=MESH,
        ).wait_recv()
        send_pages(j).wait_send()
        return carry

    lax.fori_loop(1, n, pages_came, 0)


def end_layer(sums, x, hidden, chunk, w_out, w_up, w_down, proj, layer, n):
    chips = n // 2
    hid_rows, width = hidden.shape
    seq_dev, rows, head_dim = x.shape[1:]
    follow = bool(proj)
    tile, up_slots = 512, 3
    wide_slots = width // tile
    out_shape = [jax.ShapeDtypeStruct(hidden.shape, hidden.dtype), jax.ShapeDtypeStruct(chunk.shape, chunk.dtype)]
    out_specs = [VMEM, ANY]
    scratch = [
        pltpu.VMEM(sums.shape, sums.dtype),
        pltpu.VMEM((seq_dev * rows, head_dim), jnp.float32),
        pltpu.VMEM(hidden.shape, jnp.bfloat16),
        pltpu.VMEM(hidden.shape, jnp.bfloat16),
        pltpu.VMEM(hidden.shape, jnp.float32),
        pltpu.VMEM((wide_slots, width, tile), w_out.dtype),
        pltpu.VMEM((up_slots, width, tile), w_up.dtype),
        pltpu.VMEM((up_slots, tile, width), w_down.dtype),
        pltpu.SemaphoreType.DMA((wide_slots,)),
        pltpu.SemaphoreType.DMA((up_slots,)),
        pltpu.SemaphoreType.DMA((up_slots,)),
        pltpu.SemaphoreType.DMA((chips,)),
        pltpu.SemaphoreType.DMA((chips,)),
        pltpu.SemaphoreType.DMA((n,)),
        pltpu.SemaphoreType.DMA((n,)),
    ]
    if follow:
        spread_shape = (2, chips) + x.shape
        out_shape += [jax.ShapeDtypeStruct(x.shape, x.dtype), jax.ShapeDtypeStruct(spread_shape, x.dtype)]
        out_specs += [VMEM, ANY]
        scratch += [pltpu.VMEM(x.shape, x.dtype), pltpu.VMEM(spread_shape, x.dtype)]
        scratch += [pltpu.SemaphoreType.DMA((chips,))] * 4 + [pltpu.SemaphoreType.DMA((n,))]
    return pl.pallas_call(
        functools.partial(layer_kernel, n, head_dim ** -0.5, layer, follow),
        out_shape=out_shape,
        in_specs=[VMEM] * 3 + [ANY] * (4 + len(proj)),
        out_specs=out_specs,
        scratch_shapes=scratch,
        compiler_params=pltpu.CompilerParams(collective_id=3 + layer, has_side_effects=True),
        cost_estimate=pl.CostEstimate(flops=10 ** 10, bytes_accessed=2 ** 27, transcendentals=0),
        name="end_layer",
    )(sums, x, hidden, chunk, w_out, w_up, w_down, *proj)


def solution(mesh):
    groups = mesh.shape['kv']
    rows_spec = P(None, ('rep', 'kv'), None)
    pool_spec = P(('rep', 'kv'))
    table_spec = P('rep', None)
    vec_spec = P('rep')
    full_spec = P()

    def device_fn(embeds, w_query, w_key, w_value, w_out, w_up, w_down, k_pool, v_pool, old_table, new_table, seq_len, finished, mig_src, mig_dst):
        me = lax.axis_index('kv')
        slots, n_layers, page_size, heads, head_dim = k_pool.shape
        steps, seq_dev, width = embeds.shape
        n_batch, pages_seq = old_table.shape
        n_mig = mig_src.shape[0]
        rounds = 4 * n_mig // (groups * groups)
        base = me * slots
        local = jnp.arange(slots, dtype=jnp.int32)
        active = finished == 0
        last = pages_seq - 1

        def find(match, value):
            return jnp.max(jnp.where(match, value, -1), axis=1)

        flat = old_table.reshape(-1)
        place = jnp.arange(n_batch * pages_seq, dtype=jnp.int32)
        seen = jnp.clip(seq_len[:, None] - jnp.arange(pages_seq, dtype=jnp.int32)[None, :] * page_size, 0, page_size).reshape(-1)
        code = find(flat[None, :] - base == local[:, None], (place * (2 * page_size) + seen)[None, :])

        src_dev, dst_dev = mig_src // slots, mig_dst // slots
        pair = src_dev * groups + dst_dev
        entry = jnp.arange(n_mig, dtype=jnp.int32)
        rank = jnp.sum((pair[None, :] == pair[:, None]) & (entry[None, :] < entry[:, None]), axis=1, dtype=jnp.int32)
        lines = jnp.arange(rounds * groups, dtype=jnp.int32)
        send_slot = find(
            ((rank * groups + dst_dev)[None, :] == lines[:, None]) & (src_dev == me)[None, :], (mig_src - src_dev * slots)[None, :]
        )
        from_page = find((mig_dst - base)[None, :] == local[:, None], (rank * groups + src_dev)[None, :])

        seq_ids = jnp.arange(n_batch, dtype=jnp.int32)
        owner_old = find((old_table[:, last] - base)[None, :] == local[:, None], seq_ids[None, :])
        owner_new = find(((new_table[:, last] - base)[None, :] == local[:, None]) & active[None, :], seq_ids[None, :])
        first_seq = jnp.where(from_page >= 0, owner_new, owner_old)
        second_seq = owner_new
        offsets = lax.rem(seq_len, page_size)

        def exchange(block):
            return lax.all_to_all(block, 'kv', 0, 0, tiled=True)

        def send_next(value, count):
            for block in packed[len(got):len(got) + count]:
                block, value = lax.optimization_barrier((block, value))
                got.append(exchange(block))
            return value

        plan = ((0, (0,)), (0, (1,))) + tuple((r, (0, 1)) for r in range(1, rounds - 1)) + ((rounds - 1, (0,)), (rounds - 1, (1,)))
        packed = list(pack_pages(plan[:1], send_slot, k_pool, v_pool, groups))
        packed[0], send_slot = lax.optimization_barrier((packed[0], send_slot))
        got = [exchange(packed[0])]
        packed += list(pack_pages(plan[1:], send_slot, k_pool, v_pool, groups))
        tables = (from_page, first_seq, second_seq, offsets)
        k_out, v_out = keep_pages(from_page, k_pool, v_pool)

        hidden = jnp.transpose(embeds, (1, 0, 2)).reshape(seq_dev * steps, width)
        x = jnp.stack([
            jnp.dot(hidden, w[0], preferred_element_type=jnp.float32).astype(jnp.bfloat16).reshape(seq_dev, steps * heads, head_dim)
            for w in (w_query, w_key, w_value)
        ])
        x, k_out, v_out, packed, got = lax.optimization_barrier((x, k_out, v_out, packed, got))
        x_all = spread(x, groups)
        rows = []
        for layer in range(n_layers):
            rows.append(x_all)
            x_all = send_next(x_all, 1)
            sums = merge_chip(attend_pages(code, x_all, k_pool, v_pool, layer, pages_seq))
            if layer:
                k_out, v_out = place_pages(plan[:3], from_page, got[:3], k_out, v_out)
                sums, k_out, v_out = lax.optimization_barrier((sums, k_out, v_out))
            follow = (w_query, w_key, w_value) if layer + 1 < n_layers else ()
            hidden, pages, *ahead = end_layer(sums, x, hidden, packed[len(got)], w_out, w_up, w_down, follow, layer, groups)
            got.append(pages)
            if ahead:
                x, x_all = ahead
        k_out, v_out = close_pools(seq_dev, rounds - 1, *tables, got[3:], rows, k_out, v_out)
        hidden = jnp.transpose(hidden.reshape(seq_dev, steps, width), (1, 0, 2))
        done = lax.dynamic_slice(finished, (me * seq_dev,), (seq_dev,)) != 0
        live = jnp.stack([jnp.ones_like(done), ~done])
        hidden = jnp.where(live[:, :, None], hidden, jnp.zeros_like(hidden))
        return hidden, k_out, v_out

    in_specs = (rows_spec, full_spec, full_spec, full_spec, full_spec, full_spec, full_spec, pool_spec, pool_spec, table_spec, table_spec, vec_spec, vec_spec, vec_spec, vec_spec)
    return jax.shard_map(device_fn, mesh=mesh, in_specs=in_specs, out_specs=(rows_spec, pool_spec, pool_spec), check_vma=False)
```

```python
import functools

import jax
import jax.numpy as jnp
from jax import lax
from jax.experimental import pallas as pl
from jax.experimental.pallas import tpu as pltpu
from jax.sharding import PartitionSpec as P

MESH = pl.DeviceIdType.MESH
ANY = pl.BlockSpec(memory_space=pl.ANY)
VMEM = pl.BlockSpec(memory_space=pltpu.VMEM)
SMEM = pl.BlockSpec(memory_space=pltpu.SMEM)
LOW = -1e30


def chip_offsets(chips):
    side = 1
    while side * side < chips:
        side += 1
    if side * side != chips:
        return [(j, 0) for j in range(1, chips)], chips

    def near(d):
        d %= side
        return d if 2 * d <= side else d - side

    def cost(offset):
        x, y = near(offset[0]), near(offset[1])
        return (x == 0 or y == 0, 2 * abs(x) == side or 2 * abs(y) == side, x == 0, abs(x) + abs(y), abs(x), abs(y), x * y < 0, x)

    every = [(x, y) for x in range(side) for y in range(side) if x or y]
    return sorted(every, key=cost), side


def chip_at(chip, offset, side, chips):
    x, y = offset
    return lax.rem(chip // side + y, chips // side) * side + lax.rem(lax.rem(chip, side) + x, side)


def chip_from(chip, offset, side, chips):
    x, y = offset
    return chip_at(chip, ((side - x) % side, (chips // side - y) % (chips // side)), side, chips)


def ring(count, depth, lead, start_in, wait_in, start_out, wait_out):
    def body(i, carry):
        @pl.when(i < count)
        def _():
            @pl.when(i >= depth)
            def _():
                wait_out(i - depth)

            start_in(i)

        @pl.when(i >= lead)
        def _():
            wait_in(i - lead)
            start_out(i - lead)

        return carry

    lax.fori_loop(0, count + lead, body, 0)

    def drain(i, carry):
        wait_out(i)
        return carry

    lax.fori_loop(jnp.maximum(count - depth, 0), count, drain, 0)


def compact(total, flag, value, listed):
    def body(i, count):
        @pl.when(flag(i))
        def _():
            listed[count] = value(i)

        return count + flag(i).astype(jnp.int32)

    return lax.fori_loop(0, total, body, jnp.int32(0))


def pack_kernel(depth, lead, plan, slot_ref, *rest):
    pools = rest[:2]
    outs = rest[2:-4]
    buf, listed, sems_in, sems_out = rest[-4:]
    peers = outs[0].shape[0]
    for r, halves in plan:
        mine, outs = outs[0], outs[1:]
        count = compact(peers, lambda i: slot_ref[r * peers + i] >= 0, lambda i: i, listed)

        def ins(i):
            at = lax.rem(i, depth)
            slot = slot_ref[r * peers + listed[i]]
            return [pltpu.make_async_copy(pools[h].at[slot], buf.at[at, h], sems_in.at[at, h]) for h in halves]

        def puts(i):
            at = lax.rem(i, depth)
            return [pltpu.make_async_copy(buf.at[at, h], mine.at[listed[i], k], sems_out.at[at, h]) for k, h in enumerate(halves)]

        ring(
            count, depth, lead,
            lambda i: [c.start() for c in ins(i)],
            lambda i: [c.wait() for c in ins(i)],
            lambda i: [c.start() for c in puts(i)],
            lambda i: [c.wait() for c in puts(i)],
        )


def pack_pages(plan, send_slot, k_pool, v_pool, peers):
    page = k_pool.shape[1:]
    depth, lead = 24, 12
    total = sum(len(halves) for _, halves in plan)
    return pl.pallas_call(
        functools.partial(pack_kernel, depth, lead, plan),
        out_shape=[jax.ShapeDtypeStruct((peers, len(halves)) + page, k_pool.dtype) for _, halves in plan],
        in_specs=[SMEM, ANY, ANY],
        out_specs=[ANY] * len(plan),
        scratch_shapes=[
            pltpu.VMEM((depth, 2) + page, k_pool.dtype),
            pltpu.SMEM((peers,), jnp.int32),
            pltpu.SemaphoreType.DMA((depth, 2)),
            pltpu.SemaphoreType.DMA((depth, 2)),
        ],
        cost_estimate=pl.CostEstimate(flops=10 ** 6, bytes_accessed=2 ** 21 * total, transcendentals=0),
        name="pack_pages",
    )(send_slot, k_pool, v_pool)


def keep_kernel(depth, lead, from_ref, k_ref, v_ref, k_out, v_out, buf, listed, sems_in, sems_out):
    count = compact(from_ref.shape[0], lambda i: from_ref[i] < 0, lambda i: i, listed)

    def ins(i):
        at = lax.rem(i, depth)
        return [pltpu.make_async_copy(ref.at[listed[i]], buf.at[at, h], sems_in.at[at, h]) for h, ref in enumerate((k_ref, v_ref))]

    def outs(i):
        at = lax.rem(i, depth)
        return [pltpu.make_async_copy(buf.at[at, h], ref.at[listed[i]], sems_out.at[at, h]) for h, ref in enumerate((k_out, v_out))]

    ring(
        count, depth, lead,
        lambda i: [c.start() for c in ins(i)],
        lambda i: [c.wait() for c in ins(i)],
        lambda i: [c.start() for c in outs(i)],
        lambda i: [c.wait() for c in outs(i)],
    )


def keep_pages(from_page, k_pool, v_pool):
    depth, lead = 24, 12
    return pl.pallas_call(
        functools.partial(keep_kernel, depth, lead),
        out_shape=[jax.ShapeDtypeStruct(k_pool.shape, k_pool.dtype)] * 2,
        in_specs=[SMEM] + [ANY] * 2,
        out_specs=[ANY] * 2,
        scratch_shapes=[
            pltpu.VMEM((depth, 2) + k_pool.shape[1:], k_pool.dtype),
            pltpu.SMEM((k_pool.shape[0],), jnp.int32),
            pltpu.SemaphoreType.DMA((depth, 2)),
            pltpu.SemaphoreType.DMA((depth, 2)),
        ],
        cost_estimate=pl.CostEstimate(flops=10 ** 6, bytes_accessed=2 ** 25, transcendentals=0),
        name="keep_pages",
    )(from_page, k_pool, v_pool)


def place_kernel(depth, lead, plan, from_ref, *rest):
    arrived, rest = rest[:len(plan)], rest[len(plan):]
    k_out, v_out, buf, listed, sems_in, sems_out = rest[2:]
    pools = (k_out, v_out)
    peers = arrived[0].shape[0]
    slots = from_ref.shape[0]
    for part, (r, halves) in enumerate(plan):
        count = compact(slots, lambda i: (from_ref[i] >= r * peers) & (from_ref[i] < (r + 1) * peers), lambda i: i, listed)

        def ins(i):
            at = lax.rem(i, depth)
            line = from_ref[listed[i]] - r * peers
            return [pltpu.make_async_copy(arrived[part].at[line, k], buf.at[at, h], sems_in.at[at, h]) for k, h in enumerate(halves)]

        def outs(i):
            at = lax.rem(i, depth)
            return [pltpu.make_async_copy(buf.at[at, h], pools[h].at[listed[i]], sems_out.at[at, h]) for h in halves]

        ring(
            count, depth, lead,
            lambda i: [c.start() for c in ins(i)],
            lambda i: [c.wait() for c in ins(i)],
            lambda i: [c.start() for c in outs(i)],
            lambda i: [c.wait() for c in outs(i)],
        )


def place_pages(plan, from_page, arrived, k_out, v_out):
    depth, lead = 24, 12
    return pl.pallas_call(
        functools.partial(place_kernel, depth, lead, plan),
        out_shape=[jax.ShapeDtypeStruct(k_out.shape, k_out.dtype)] * 2,
        in_specs=[SMEM] + [ANY] * (len(arrived) + 2),
        out_specs=[ANY] * 2,
        scratch_shapes=[
            pltpu.VMEM((depth, 2) + k_out.shape[1:], k_out.dtype),
            pltpu.SMEM((k_out.shape[0],), jnp.int32),
            pltpu.SemaphoreType.DMA((depth, 2)),
            pltpu.SemaphoreType.DMA((depth, 2)),
        ],
        input_output_aliases={1 + len(arrived): 0, 2 + len(arrived): 1},
        cost_estimate=pl.CostEstimate(flops=10 ** 6, bytes_accessed=2 ** 22 * len(arrived), transcendentals=0),
        name="place_pages",
    )(from_page, *arrived, k_out, v_out)


def close_kernel(seq_dev, first_line, n_layers, from_ref, first_ref, second_ref, offset_ref, k_came, v_came, *rest):
    rows = rest[:2 * n_layers]
    k_out, v_out, buf, listed, staged, early, late, sems_in, sem_out, sem_row = rest[2 * n_layers + 2:]
    pools, arrived = (k_out, v_out), (k_came, v_came)
    peers = k_came.shape[0]
    slots, n_batch = from_ref.shape[0], offset_ref.shape[0]
    heads = k_out.shape[3]
    most = early.shape[0]

    def ins(i, line):
        return [pltpu.make_async_copy(ref.at[line], buf.at[i, h], sems_in.at[i]) for h, ref in enumerate(arrived)]

    def outs(i, slot):
        return [pltpu.make_async_copy(buf.at[i, h], pools[h].at[slot], sem_out.at[0]) for h in range(2)]

    def fetch(at, seq, step):
        home, place = seq // seq_dev, lax.rem(seq, seq_dev)
        return [
            pltpu.make_async_copy(
                rows[2 * layer + h].at[lax.rem(home, 2), home // 2, place, pl.ds(step * heads, heads)], staged.at[at, layer, h], sem_row.at[0]
            )
            for layer in range(n_layers) for h in range(2)
        ]

    def write(at, slot, layer_offset, sem):
        return [
            pltpu.make_async_copy(staged.at[at, layer, h], pools[h].at[slot, layer, layer_offset], sem_row.at[sem])
            for layer in range(n_layers) for h in range(2)
        ]

    def scan(slot, counts):
        pages, n_early, n_late = counts
        line = from_ref[slot] - first_line
        moved = (line >= 0) & (line < peers)

        @pl.when(moved)
        def _():
            listed[pages] = slot
            for c in ins(pages, line):
                c.start()

        for step, ref in enumerate((first_ref, second_ref)):
            seq = ref[slot]
            entry = (slot * 2 + step) * n_batch + seq

            @pl.when((seq >= 0) & moved)
            def _():
                late[n_late] = entry
                for c in fetch(most - 1 - n_late, seq, step):
                    c.start()

            @pl.when((seq >= 0) & jnp.logical_not(moved))
            def _():
                early[n_early] = entry
                for c in fetch(n_early, seq, step):
                    c.start()

            n_late = n_late + ((seq >= 0) & moved).astype(jnp.int32)
            n_early = n_early + ((seq >= 0) & jnp.logical_not(moved)).astype(jnp.int32)
        return pages + moved.astype(jnp.int32), n_early, n_late

    pages, n_early, n_late = lax.fori_loop(0, slots, scan, (jnp.int32(0), jnp.int32(0), jnp.int32(0)))

    def pass_on(i, carry):
        for c in ins(i, 0):
            c.wait()
        for c in outs(i, listed[i]):
            c.start()
        return carry

    lax.fori_loop(0, pages, pass_on, 0)

    def fetched(i, carry):
        for c in fetch(0, 0, 0):
            c.wait()
        return carry

    lax.fori_loop(0, n_early + n_late, fetched, 0)

    def write_row(entries, at, sem):
        def body(i, carry):
            entry = entries[i]
            seq, where = lax.rem(entry, n_batch), entry // n_batch
            for c in write(at(i), where // 2, offset_ref[seq] + lax.rem(where, 2), sem):
                c.start()
            return carry
        return body

    lax.fori_loop(0, n_early, write_row(early, lambda i: i, 1), 0)

    def placed(i, carry):
        for c in outs(i, 0):
            c.wait()
        return carry

    lax.fori_loop(0, pages, placed, 0)
    lax.fori_loop(0, n_late, write_row(late, lambda i: most - 1 - i, 1), 0)

    def written(i, carry):
        for c in write(0, 0, 0, 1):
            c.wait()
        return carry

    lax.fori_loop(0, n_early + n_late, written, 0)


def close_pools(seq_dev, last_round, from_page, first_seq, second_seq, offsets, arrived, rows, k_out, v_out):
    peers, slots = arrived[0].shape[0], k_out.shape[0]
    first_pool = 6 + len(rows)
    return pl.pallas_call(
        functools.partial(close_kernel, seq_dev, last_round * peers, len(rows) // 2),
        out_shape=[jax.ShapeDtypeStruct(k_out.shape, k_out.dtype)] * 2,
        in_specs=[SMEM] * 4 + [ANY] * (4 + len(rows)),
        out_specs=[ANY] * 2,
        scratch_shapes=[
            pltpu.VMEM((peers, 2) + k_out.shape[1:], k_out.dtype),
            pltpu.SMEM((peers,), jnp.int32),
            pltpu.VMEM((2 * slots, len(rows) // 2, 2) + k_out.shape[3:], k_out.dtype),
            pltpu.SMEM((2 * slots,), jnp.int32),
            pltpu.SMEM((2 * slots,), jnp.int32),
            pltpu.SemaphoreType.DMA((peers,)),
            pltpu.SemaphoreType.DMA((1,)),
            pltpu.SemaphoreType.DMA((2,)),
        ],
        input_output_aliases={first_pool: 0, first_pool + 1: 1},
        cost_estimate=pl.CostEstimate(flops=10 ** 6, bytes_accessed=2 ** 23, transcendentals=0),
        name="close_pools",
    )(from_page, first_seq, second_seq, offsets, *[a.reshape((peers,) + a.shape[2:]) for a in arrived], *rows, k_out, v_out)


def attend_kernel(block, pages_seq, seq_dev, page_size, scale, code_ref, q_ref, k_ref, v_ref, acc_ref):
    rows, head_dim = q_ref.shape[-2:]
    heads = k_ref.shape[3]
    chips = acc_ref.shape[1]
    step = pl.program_id(0)

    @pl.when(step == 0)
    def _():
        for core in range(2):
            acc_ref[core, :, :seq_dev] = jnp.zeros((chips, seq_dev, rows, head_dim), jnp.float32)
            lane = lax.broadcasted_iota(jnp.int32, (chips, 1, rows, head_dim), 3)
            acc_ref[core, :, seq_dev:] = jnp.where(lax.rem(lane, 2) == 0, LOW, 0.0)

    row = lax.broadcasted_iota(jnp.int32, (rows, page_size * heads), 0)
    column = lax.broadcasted_iota(jnp.int32, (rows, page_size * heads), 1)
    same_head = lax.rem(row, heads) == lax.rem(column, heads)
    position = jnp.where(same_head, column // heads, page_size)
    lane = lax.broadcasted_iota(jnp.int32, (rows, head_dim), 1)
    found = []
    for s in range(block):
        code = code_ref[step * block + s]
        held = jnp.maximum(code, 0)
        seen = jnp.where(code >= 0, lax.rem(held, 2 * page_size), 0)
        seq = held // (2 * page_size * pages_seq)
        home, place = seq // seq_dev, lax.rem(seq, seq_dev)
        core, chip = lax.rem(home, 2), home // 2
        q = q_ref[core, chip, place]
        keys = k_ref[s, 0].reshape(page_size * heads, head_dim)
        values = v_ref[s, 0].reshape(page_size * heads, head_dim)
        scores = lax.dot_general(q, keys, (((1,), (1,)), ((), ())), preferred_element_type=jnp.float32) * scale
        mask = position < seen
        scores = jnp.where(mask, scores, LOW)
        top = jnp.max(scores, axis=1, keepdims=True)
        weights = jnp.where(mask, jnp.exp(scores - top), 0.0)
        total = jnp.sum(weights, axis=1, keepdims=True)
        high = weights.astype(jnp.bfloat16)
        low = (weights - high.astype(jnp.float32)).astype(jnp.bfloat16)
        mixed = jnp.dot(high, values, preferred_element_type=jnp.float32) + jnp.dot(low, values, preferred_element_type=jnp.float32)
        found.append((core, chip, place, top, total, mixed))
    for core, chip, place, top, total, mixed in found:
        stats = acc_ref[core, chip, seq_dev]
        old_top = jnp.max(jnp.where(lane == 2 * place, stats, LOW), axis=1, keepdims=True)
        old_total = jnp.sum(jnp.where(lane == 2 * place + 1, stats, 0.0), axis=1, keepdims=True)
        new_top = jnp.maximum(top, old_top)
        old_part, new_part = jnp.exp(old_top - new_top), jnp.exp(top - new_top)
        acc_ref[core, chip, place] = acc_ref[core, chip, place] * old_part + mixed * new_part
        new_total = old_total * old_part + total * new_part
        acc_ref[core, chip, seq_dev] = jnp.where(lane == 2 * place, new_top, jnp.where(lane == 2 * place + 1, new_total, stats))


def attend_pages(code, q_all, k_pool, v_pool, layer, pages_seq):
    slots, _, page_size, heads, head_dim = k_pool.shape
    cores, chips, seq_dev, rows, _ = q_all.shape
    block = 8
    page_spec = pl.BlockSpec((block, 1, page_size, heads, head_dim), lambda i, c: (i, layer, 0, 0, 0))
    query_spec = pl.BlockSpec(q_all.shape, lambda i, c: (0,) * 5)
    acc_shape = (cores, chips, seq_dev + 1, rows, head_dim)
    return pl.pallas_call(
        functools.partial(attend_kernel, block, pages_seq, seq_dev, page_size, head_dim ** -0.5),
        out_shape=jax.ShapeDtypeStruct(acc_shape, jnp.float32),
        grid_spec=pltpu.PrefetchScalarGridSpec(
            num_scalar_prefetch=1,
            grid=(slots // block,),
            in_specs=[query_spec, page_spec, page_spec],
            out_specs=pl.BlockSpec(acc_shape, lambda i, c: (0,) * 5),
        ),
        compiler_params=pltpu.CompilerParams(dimension_semantics=("arbitrary",)),
        cost_estimate=pl.CostEstimate(flops=10 ** 6, bytes_accessed=2 * slots * page_size * heads * head_dim * 2, transcendentals=0),
        name="attend_pages",
    )(code, q_all, k_pool, v_pool)


def spread_kernel(n, x_ref, out_ref, held, send_sem, recv_sem, pass_sem, got_sem, copy_sem):
    me = lax.axis_index("kv")
    chips = n // 2
    core, chip = lax.rem(me, 2), me // 2
    barrier = pltpu.get_barrier_semaphore()

    def greet(j, carry):
        pl.semaphore_signal(barrier, inc=1, device_id={"kv": 2 * lax.rem(chip + j, chips) + core}, device_id_type=MESH)
        return carry

    lax.fori_loop(1, chips, greet, 0)
    pl.semaphore_signal(barrier, inc=1, device_id={"kv": me + 1 - 2 * core}, device_id_type=MESH)
    pl.semaphore_wait(barrier, chips)
    spread_body(n, x_ref, out_ref, held, send_sem, recv_sem, pass_sem, got_sem, copy_sem)


def spread_body(n, x_ref, out_ref, held, send_sem, recv_sem, pass_sem, got_sem, copy_sem):
    me = lax.axis_index("kv")
    chips = n // 2
    core, chip = lax.rem(me, 2), me // 2
    other = me + 1 - 2 * core

    def peer(j):
        return 2 * lax.rem(chip + j, chips) + core

    def send(j):
        return pltpu.make_async_remote_copy(
            src_ref=x_ref, dst_ref=held.at[core, chip], send_sem=send_sem.at[j], recv_sem=recv_sem.at[chip],
            device_id={"kv": peer(j)}, device_id_type=MESH,
        )

    def forward(source, at):
        return pltpu.make_async_remote_copy(
            src_ref=source, dst_ref=held.at[core, at], send_sem=pass_sem.at[at], recv_sem=got_sem.at[at],
            device_id={"kv": other}, device_id_type=MESH,
        )

    offsets, side = chip_offsets(chips)
    for offset in offsets:
        send(lax.rem(chip_at(chip, offset, side, chips) + chips - chip, chips)).start()
    own = forward(x_ref, chip)
    own.start()
    mine = pltpu.make_async_copy(x_ref, out_ref.at[core, chip], copy_sem.at[0])
    mine.start()

    for offset in offsets:
        at = chip_from(chip, offset, side, chips)
        j = lax.rem(chip + chips - at, chips)
        pltpu.make_async_remote_copy(
            src_ref=x_ref, dst_ref=held.at[core, at], send_sem=send_sem.at[j], recv_sem=recv_sem.at[at],
            device_id={"kv": other}, device_id_type=MESH,
        ).wait_recv()
        forward(held.at[core, at], at).start()
        pltpu.make_async_copy(held.at[core, at], out_ref.at[core, at], copy_sem.at[j]).start()

    def passed(j, carry):
        at = lax.rem(chip + j, chips)
        pltpu.make_async_remote_copy(
            src_ref=x_ref, dst_ref=held.at[1 - core, at], send_sem=pass_sem.at[at], recv_sem=got_sem.at[at],
            device_id={"kv": other}, device_id_type=MESH,
        ).wait_recv()
        pltpu.make_async_copy(held.at[1 - core, at], out_ref.at[1 - core, at], copy_sem.at[chips + j]).start()
        return carry

    lax.fori_loop(0, chips, passed, 0)

    own.wait_send()
    mine.wait()

    def finish(j, carry):
        at = lax.rem(chip + chips - j, chips)
        send(j).wait_send()
        forward(held.at[core, at], at).wait_send()
        pltpu.make_async_copy(held.at[core, at], out_ref.at[core, at], copy_sem.at[j]).wait()
        return carry

    lax.fori_loop(1, chips, finish, 0)

    def written(j, carry):
        at = lax.rem(chip + j, chips)
        pltpu.make_async_copy(held.at[1 - core, at], out_ref.at[1 - core, at], copy_sem.at[chips + j]).wait()
        return carry

    lax.fori_loop(0, chips, written, 0)


def spread(x, n):
    chips = n // 2
    return pl.pallas_call(
        functools.partial(spread_kernel, n),
        out_shape=jax.ShapeDtypeStruct((2, chips) + x.shape, x.dtype),
        in_specs=[VMEM],
        out_specs=ANY,
        scratch_shapes=[
            pltpu.VMEM((2, chips) + x.shape, x.dtype),
            pltpu.SemaphoreType.DMA((chips,)),
            pltpu.SemaphoreType.DMA((chips,)),
            pltpu.SemaphoreType.DMA((chips,)),
            pltpu.SemaphoreType.DMA((chips,)),
            pltpu.SemaphoreType.DMA((n,)),
        ],
        compiler_params=pltpu.CompilerParams(collective_id=0, has_side_effects=True),
        name="spread_rows",
    )(x)


def lane_before(x):
    return pltpu.roll(x, x.shape[1] - 1, 1)


def merge_chip_kernel(acc_ref, sums_ref, near, send_sem, recv_sem):
    me = lax.axis_index("kv")
    core = lax.rem(me, 2)
    other = me + 1 - 2 * core
    chips, blocks, rows, head_dim = near.shape
    seq_dev = blocks - 1

    barrier = pltpu.get_barrier_semaphore()
    pl.semaphore_signal(barrier, inc=1, device_id={"kv": other}, device_id_type=MESH)
    pl.semaphore_wait(barrier, 1)

    swap = pltpu.make_async_remote_copy(
        src_ref=acc_ref.at[1 - core], dst_ref=near, send_sem=send_sem.at[0], recv_sem=recv_sem.at[0],
        device_id={"kv": other}, device_id_type=MESH,
    )
    swap.start()
    even = lax.rem(lax.broadcasted_iota(jnp.int32, (rows, head_dim), 1), 2) == 0
    swap.wait_recv()

    def merge(at, carry):
        mine, theirs = acc_ref[core, at, seq_dev], near[at, seq_dev]
        top = jnp.maximum(mine, theirs)
        a, b = jnp.exp(mine - top), jnp.exp(theirs - top)
        total = a * lane_before(mine) + b * lane_before(theirs)
        sums_ref[at, seq_dev] = jnp.where(even, top, pltpu.roll(total, 1, 1))
        for i in range(seq_dev):
            sums_ref[at, i] = a[:, 2 * i:2 * i + 1] * acc_ref[core, at, i] + b[:, 2 * i:2 * i + 1] * near[at, i]
        return carry

    lax.fori_loop(0, chips, merge, 0)
    swap.wait_send()


def merge_chip(acc):
    blocks = acc.shape[1:]
    return pl.pallas_call(
        merge_chip_kernel,
        out_shape=jax.ShapeDtypeStruct(blocks, acc.dtype),
        in_specs=[VMEM],
        out_specs=VMEM,
        scratch_shapes=[
            pltpu.VMEM(blocks, acc.dtype),
            pltpu.SemaphoreType.DMA((1,)),
            pltpu.SemaphoreType.DMA((1,)),
        ],
        compiler_params=pltpu.CompilerParams(collective_id=2, has_side_effects=True),
        cost_estimate=pl.CostEstimate(flops=10 ** 6, bytes_accessed=2 ** 23, transcendentals=0),
        name="merge_chip",
    )(acc)


def layer_kernel(n, scale, layer, follow, *refs):
    sums_ref, x_ref, hid_ref, chunk_ref, wo_ref, wu_ref, wd_ref = refs[:7]
    refs = refs[7:]
    hid_out, got_ref = refs[:2]
    refs = refs[2:]
    if follow:
        all_out, refs = refs[0], refs[1:]
    held, o_scr, rows_scr, mid_scr, acc_scr, wide, up, down, wide_sem, up_sem, down_sem, send_sem, recv_sem, page_send, page_recv = refs[:15]
    refs = refs[15:]
    me = lax.axis_index("kv")
    _, seq_dev, rows, head_dim = x_ref.shape
    heads = rows // 2
    chips = n // 2
    core, chip = lax.rem(me, 2), me // 2
    hid_rows, width = hid_ref.shape
    tile, up_tile = wide.shape[2], up.shape[2]
    up_slots = up.shape[0]
    n_wide, n_up = width // tile, wu_ref.shape[2] // up_tile

    def peer(j):
        return 2 * lax.rem(chip + j, chips) + core

    def anyone(j):
        return lax.rem(me + j, n)

    barrier = pltpu.get_barrier_semaphore()

    def greet(j, carry):
        pl.semaphore_signal(barrier, inc=1, device_id={"kv": anyone(j)}, device_id_type=MESH)
        return carry

    lax.fori_loop(1, n, greet, 0)

    def wide_copy(w, at, t, slot):
        return pltpu.make_async_copy(w.at[at, :, pl.ds(pl.multiple_of(t * tile, tile), tile)], wide.at[slot], wide_sem.at[slot])

    def up_copy(t):
        slot = lax.rem(t, up_slots)
        return pltpu.make_async_copy(wu_ref.at[layer, :, pl.ds(pl.multiple_of(t * up_tile, up_tile), up_tile)], up.at[slot], up_sem.at[slot])

    def down_copy(t):
        slot = lax.rem(t, up_slots)
        return pltpu.make_async_copy(wd_ref.at[layer, pl.ds(pl.multiple_of(t * up_tile, up_tile), up_tile)], down.at[slot], down_sem.at[slot])

    for t in range(n_wide):
        wide_copy(wo_ref, layer, t, t).start()
    for t in range(up_slots):
        up_copy(t).start()
        down_copy(t).start()
    pl.semaphore_wait(barrier, n - 1)

    def send(j):
        return pltpu.make_async_remote_copy(
            src_ref=sums_ref.at[lax.rem(chip + j, chips)], dst_ref=held.at[chip], send_sem=send_sem.at[j], recv_sem=recv_sem.at[chip],
            device_id={"kv": peer(j)}, device_id_type=MESH,
        )

    def send_pages(j):
        return pltpu.make_async_remote_copy(
            src_ref=chunk_ref.at[anyone(j)], dst_ref=got_ref.at[me], send_sem=page_send.at[j], recv_sem=page_recv.at[me],
            device_id={"kv": anyone(j)}, device_id_type=MESH,
        )

    offsets, side = chip_offsets(chips)
    for offset in offsets:
        send(lax.rem(chip_at(chip, offset, side, chips) + chips - chip, chips)).start()
    for offset in offsets:
        for other_core in range(2):
            to = 2 * chip_at(chip, offset, side, chips) + lax.rem(core + other_core, 2)
            send_pages(lax.rem(to + n - me, n)).start()
    send_pages(lax.rem(me + 1 - 2 * core + n - me, n)).start()
    held[chip] = sums_ref[chip]

    queries = [x_ref[0, i].astype(jnp.float32) for i in range(seq_dev)]
    second_row = lax.broadcasted_iota(jnp.int32, (rows, 1), 0) >= heads

    def twice(h, i, step):
        x = x_ref[1 + h, i, step * heads:(step + 1) * heads].astype(jnp.float32)
        return jnp.concatenate([x, x], axis=0)

    first = [jnp.sum(queries[i] * twice(0, i, 0), axis=1, keepdims=True) * scale for i in range(seq_dev)]
    second = [
        jnp.where(second_row, jnp.sum(queries[i] * twice(0, i, 1), axis=1, keepdims=True) * scale, LOW)
        for i in range(seq_dev)
    ]

    def arrive(j, carry):
        at = lax.rem(chip + chips - j, chips)
        pltpu.make_async_remote_copy(
            src_ref=sums_ref.at[at], dst_ref=held.at[at], send_sem=send_sem.at[j], recv_sem=recv_sem.at[at],
            device_id={"kv": peer(j)}, device_id_type=MESH,
        ).wait_recv()
        return carry

    lax.fori_loop(1, chips, arrive, 0)

    def highest(j, top):
        return jnp.maximum(top, held[j, seq_dev])

    top_all = lax.fori_loop(0, chips, highest, jnp.full((rows, head_dim), LOW, jnp.float32))
    tops, totals, mixed = [], [], []
    for i in range(seq_dev):
        top = jnp.maximum(jnp.maximum(top_all[:, 2 * i:2 * i + 1], first[i]), second[i])
        p_first, p_second = jnp.exp(first[i] - top), jnp.exp(second[i] - top)
        tops.append(top)
        totals.append(p_first + p_second)
        mixed.append(p_first * twice(1, i, 0) + p_second * twice(1, i, 1))

    def merge(j, carry):
        totals, mixed = carry
        stats = held[j, seq_dev]
        new_totals, new_mixed = [], []
        for i in range(seq_dev):
            weight = jnp.exp(stats[:, 2 * i:2 * i + 1] - tops[i])
            new_totals.append(totals[i] + weight * stats[:, 2 * i + 1:2 * i + 2])
            new_mixed.append(mixed[i] + weight * held[j, i])
        return tuple(new_totals), tuple(new_mixed)

    totals, mixed = lax.fori_loop(0, chips, merge, (tuple(totals), tuple(mixed)))
    for i in range(seq_dev):
        o_scr[i * rows:(i + 1) * rows] = (mixed[i] / totals[i]).astype(jnp.bfloat16).astype(jnp.float32)
    for h in range(heads):
        rows_scr[:, h * head_dim:(h + 1) * head_dim] = o_scr[pl.ds(h, hid_rows, stride=heads), :].astype(jnp.bfloat16)

    def add_out(t, carry):
        wide_copy(wo_ref, layer, t, t).wait()
        cut = pl.ds(pl.multiple_of(t * tile, tile), tile)
        part = jnp.dot(rows_scr[...], wide[t], preferred_element_type=jnp.float32)
        mid_scr[:, cut] = (hid_ref[:, cut].astype(jnp.float32) + part).astype(jnp.bfloat16)
        return carry

    lax.fori_loop(0, n_wide, add_out, 0)
    acc_scr[...] = jnp.zeros_like(acc_scr)

    def mlp(t, carry):
        slot = lax.rem(t, up_slots)
        up_copy(t).wait()
        inner = jax.nn.gelu(jnp.dot(mid_scr[...], up[slot], preferred_element_type=jnp.float32)).astype(jnp.bfloat16)
        down_copy(t).wait()
        acc_scr[...] += jnp.dot(inner, down[slot], preferred_element_type=jnp.float32)

        @pl.when(t + up_slots < n_up)
        def _():
            up_copy(t + up_slots).start()
            down_copy(t + up_slots).start()

        return carry

    lax.fori_loop(0, n_up, mlp, 0)
    hid_out[...] = (mid_scr[...].astype(jnp.float32) + acc_scr[...]).astype(jnp.bfloat16)

    def finish(j, carry):
        send(j).wait_send()
        return carry

    lax.fori_loop(1, chips, finish, 0)
    if follow:
        all_held, pass_send, pass_recv, spread_send, spread_recv, copy_sem = refs
        spread_body(n, hid_out, all_out, all_held, spread_send, spread_recv, pass_send, pass_recv, copy_sem)

    def pages_came(j, carry):
        at = lax.rem(me + n - j, n)
        pltpu.make_async_remote_copy(
            src_ref=chunk_ref.at[at], dst_ref=got_ref.at[at], send_sem=page_send.at[j], recv_sem=page_recv.at[at],
            device_id={"kv": anyone(j)}, device_id_type=MESH,
        ).wait_recv()
        send_pages(j).wait_send()
        return carry

    lax.fori_loop(1, n, pages_came, 0)


def end_layer(sums, x, hidden, chunk, w_out, w_up, w_down, layer, follow, n):
    chips = n // 2
    hid_rows, width = hidden.shape
    seq_dev, rows, head_dim = x.shape[1:]
    tile, up_slots = 512, 3
    wide_slots = width // tile
    out_shape = [jax.ShapeDtypeStruct(hidden.shape, hidden.dtype), jax.ShapeDtypeStruct(chunk.shape, chunk.dtype)]
    out_specs = [VMEM, ANY]
    scratch = [
        pltpu.VMEM(sums.shape, sums.dtype),
        pltpu.VMEM((seq_dev * rows, head_dim), jnp.float32),
        pltpu.VMEM(hidden.shape, jnp.bfloat16),
        pltpu.VMEM(hidden.shape, jnp.bfloat16),
        pltpu.VMEM(hidden.shape, jnp.float32),
        pltpu.VMEM((wide_slots, width, tile), w_out.dtype),
        pltpu.VMEM((up_slots, width, tile), w_up.dtype),
        pltpu.VMEM((up_slots, tile, width), w_down.dtype),
        pltpu.SemaphoreType.DMA((wide_slots,)),
        pltpu.SemaphoreType.DMA((up_slots,)),
        pltpu.SemaphoreType.DMA((up_slots,)),
        pltpu.SemaphoreType.DMA((chips,)),
        pltpu.SemaphoreType.DMA((chips,)),
        pltpu.SemaphoreType.DMA((n,)),
        pltpu.SemaphoreType.DMA((n,)),
    ]
    if follow:
        spread_shape = (2, chips) + hidden.shape
        out_shape += [jax.ShapeDtypeStruct(spread_shape, hidden.dtype)]
        out_specs += [ANY]
        scratch += [pltpu.VMEM(spread_shape, hidden.dtype)]
        scratch += [pltpu.SemaphoreType.DMA((chips,))] * 4 + [pltpu.SemaphoreType.DMA((n,))]
    return pl.pallas_call(
        functools.partial(layer_kernel, n, head_dim ** -0.5, layer, follow),
        out_shape=out_shape,
        in_specs=[VMEM] * 3 + [ANY] * 4,
        out_specs=out_specs,
        scratch_shapes=scratch,
        compiler_params=pltpu.CompilerParams(collective_id=3 + layer, has_side_effects=True),
        cost_estimate=pl.CostEstimate(flops=10 ** 10, bytes_accessed=2 ** 27, transcendentals=0),
        name="end_layer",
    )(sums, x, hidden, chunk, w_out, w_up, w_down)


def solution(mesh):
    groups = mesh.shape['kv']
    rows_spec = P(None, ('rep', 'kv'), None)
    pool_spec = P(('rep', 'kv'))
    table_spec = P('rep', None)
    vec_spec = P('rep')
    full_spec = P()

    def device_fn(embeds, w_query, w_key, w_value, w_out, w_up, w_down, k_pool, v_pool, old_table, new_table, seq_len, finished, mig_src, mig_dst):
        me = lax.axis_index('kv')
        slots, n_layers, page_size, heads, head_dim = k_pool.shape
        steps, seq_dev, width = embeds.shape
        n_batch, pages_seq = old_table.shape
        n_mig = mig_src.shape[0]
        rounds = 4 * n_mig // (groups * groups)
        base = me * slots
        local = jnp.arange(slots, dtype=jnp.int32)
        active = finished == 0
        last = pages_seq - 1

        def find(match, value):
            return jnp.max(jnp.where(match, value, -1), axis=1)

        flat = old_table.reshape(-1)
        place = jnp.arange(n_batch * pages_seq, dtype=jnp.int32)
        seen = jnp.clip(seq_len[:, None] - jnp.arange(pages_seq, dtype=jnp.int32)[None, :] * page_size, 0, page_size).reshape(-1)
        code = find(flat[None, :] - base == local[:, None], (place * (2 * page_size) + seen)[None, :])

        src_dev, dst_dev = mig_src // slots, mig_dst // slots
        pair = src_dev * groups + dst_dev
        entry = jnp.arange(n_mig, dtype=jnp.int32)
        rank = jnp.sum((pair[None, :] == pair[:, None]) & (entry[None, :] < entry[:, None]), axis=1, dtype=jnp.int32)
        lines = jnp.arange(rounds * groups, dtype=jnp.int32)
        send_slot = find(
            ((rank * groups + dst_dev)[None, :] == lines[:, None]) & (src_dev == me)[None, :], (mig_src - src_dev * slots)[None, :]
        )
        from_page = find((mig_dst - base)[None, :] == local[:, None], (rank * groups + src_dev)[None, :])

        seq_ids = jnp.arange(n_batch, dtype=jnp.int32)
        owner_old = find((old_table[:, last] - base)[None, :] == local[:, None], seq_ids[None, :])
        owner_new = find(((new_table[:, last] - base)[None, :] == local[:, None]) & active[None, :], seq_ids[None, :])
        first_seq = jnp.where(from_page >= 0, owner_new, owner_old)
        second_seq = owner_new
        offsets = lax.rem(seq_len, page_size)

        def exchange(block):
            return lax.all_to_all(block, 'kv', 0, 0, tiled=True)

        def send_next(value, count):
            for block in packed[len(got):len(got) + count]:
                block, value = lax.optimization_barrier((block, value))
                got.append(exchange(block))
            return value

        plan = tuple((r, (0, 1)) for r in range(rounds - 1)) + ((rounds - 1, (0,)), (rounds - 1, (1,)))
        packed = list(pack_pages(plan[:1], send_slot, k_pool, v_pool, groups))
        packed[0], send_slot = lax.optimization_barrier((packed[0], send_slot))
        packed += list(pack_pages(plan[1:], send_slot, k_pool, v_pool, groups))
        got = []
        tables = (from_page, first_seq, second_seq, offsets)
        k_out, v_out = keep_pages(from_page, k_pool, v_pool)

        hidden = jnp.transpose(embeds, (1, 0, 2)).reshape(seq_dev * steps, width)
        every = spread(hidden, groups)
        rows = []
        for layer in range(n_layers):
            every, got = lax.optimization_barrier((every, got))
            every = send_next(every, 1)
            flat_rows = every.reshape(groups * seq_dev * steps, width)
            every_x = [
                jnp.dot(flat_rows, w[layer], preferred_element_type=jnp.float32).astype(jnp.bfloat16)
                .reshape(2, groups // 2, seq_dev, steps * heads, head_dim)
                for w in (w_query, w_key, w_value)
            ]
            rows += every_x[1:]
            x = jnp.stack([y[lax.rem(me, 2), me // 2] for y in every_x])
            sums = merge_chip(attend_pages(code, every_x[0], k_pool, v_pool, layer, pages_seq))
            if layer:
                k_out, v_out = place_pages(plan[:2], from_page, got[:2], k_out, v_out)
            sums, k_out, v_out, packed = lax.optimization_barrier((sums, k_out, v_out, packed))
            hidden, pages, *ahead = end_layer(
                sums, x, hidden, packed[len(got)], w_out, w_up, w_down, layer, layer + 1 < n_layers, groups
            )
            got.append(pages)
            if ahead:
                (every,) = ahead
        k_out, v_out = close_pools(seq_dev, rounds - 1, *tables, got[2:], rows, k_out, v_out)
        hidden = jnp.transpose(hidden.reshape(seq_dev, steps, width), (1, 0, 2))
        done = lax.dynamic_slice(finished, (me * seq_dev,), (seq_dev,)) != 0
        live = jnp.stack([jnp.ones_like(done), ~done])
        hidden = jnp.where(live[:, :, None], hidden, jnp.zeros_like(hidden))
        return hidden, k_out, v_out

    in_specs = (rows_spec, full_spec, full_spec, full_spec, full_spec, full_spec, full_spec, pool_spec, pool_spec, table_spec, table_spec, vec_spec, vec_spec, vec_spec, vec_spec)
    return jax.shard_map(device_fn, mesh=mesh, in_specs=in_specs, out_specs=(rows_spec, pool_spec, pool_spec), check_vma=False)
```

```python
import functools

import jax
import jax.numpy as jnp
from jax import lax
from jax.experimental import pallas as pl
from jax.experimental.pallas import tpu as pltpu
from jax.sharding import PartitionSpec as P

MESH = pl.DeviceIdType.MESH
ANY = pl.BlockSpec(memory_space=pl.ANY)
VMEM = pl.BlockSpec(memory_space=pltpu.VMEM)
SMEM = pl.BlockSpec(memory_space=pltpu.SMEM)
LOW = -1e30


def chip_offsets(chips):
    side = 1
    while side * side < chips:
        side += 1
    if side * side != chips:
        return [(j, 0) for j in range(1, chips)], chips

    def near(d):
        d %= side
        return d if 2 * d <= side else d - side

    def cost(offset):
        x, y = near(offset[0]), near(offset[1])
        return (x == 0 or y == 0, 2 * abs(x) == side or 2 * abs(y) == side, x == 0, abs(x) + abs(y), abs(x), abs(y), x * y < 0, x)

    every = [(x, y) for x in range(side) for y in range(side) if x or y]
    return sorted(every, key=cost), side


def chip_at(chip, offset, side, chips):
    x, y = offset
    return lax.rem(chip // side + y, chips // side) * side + lax.rem(lax.rem(chip, side) + x, side)


def chip_from(chip, offset, side, chips):
    x, y = offset
    return chip_at(chip, ((side - x) % side, (chips // side - y) % (chips // side)), side, chips)


def ring(count, depth, lead, start_in, wait_in, start_out, wait_out):
    def body(i, carry):
        @pl.when(i < count)
        def _():
            @pl.when(i >= depth)
            def _():
                wait_out(i - depth)

            start_in(i)

        @pl.when(i >= lead)
        def _():
            wait_in(i - lead)
            start_out(i - lead)

        return carry

    lax.fori_loop(0, count + lead, body, 0)

    def drain(i, carry):
        wait_out(i)
        return carry

    lax.fori_loop(jnp.maximum(count - depth, 0), count, drain, 0)


def compact(total, flag, value, listed):
    def body(i, count):
        @pl.when(flag(i))
        def _():
            listed[count] = value(i)

        return count + flag(i).astype(jnp.int32)

    return lax.fori_loop(0, total, body, jnp.int32(0))


def pack_kernel(depth, lead, plan, slot_ref, *rest):
    pools = rest[:2]
    outs = rest[2:-4]
    buf, listed, sems_in, sems_out = rest[-4:]
    peers = outs[0].shape[0]
    for r, halves in plan:
        mine, outs = outs[0], outs[1:]
        count = compact(peers, lambda i: slot_ref[r * peers + i] >= 0, lambda i: i, listed)

        def ins(i):
            at = lax.rem(i, depth)
            slot = slot_ref[r * peers + listed[i]]
            return [pltpu.make_async_copy(pools[h].at[slot], buf.at[at, h], sems_in.at[at, h]) for h in halves]

        def puts(i):
            at = lax.rem(i, depth)
            return [pltpu.make_async_copy(buf.at[at, h], mine.at[listed[i], k], sems_out.at[at, h]) for k, h in enumerate(halves)]

        ring(
            count, depth, lead,
            lambda i: [c.start() for c in ins(i)],
            lambda i: [c.wait() for c in ins(i)],
            lambda i: [c.start() for c in puts(i)],
            lambda i: [c.wait() for c in puts(i)],
        )


def pack_pages(plan, send_slot, k_pool, v_pool, peers):
    page = k_pool.shape[1:]
    depth, lead = 24, 12
    total = sum(len(halves) for _, halves in plan)
    return pl.pallas_call(
        functools.partial(pack_kernel, depth, lead, plan),
        out_shape=[jax.ShapeDtypeStruct((peers, len(halves)) + page, k_pool.dtype) for _, halves in plan],
        in_specs=[SMEM, ANY, ANY],
        out_specs=[ANY] * len(plan),
        scratch_shapes=[
            pltpu.VMEM((depth, 2) + page, k_pool.dtype),
            pltpu.SMEM((peers,), jnp.int32),
            pltpu.SemaphoreType.DMA((depth, 2)),
            pltpu.SemaphoreType.DMA((depth, 2)),
        ],
        cost_estimate=pl.CostEstimate(flops=10 ** 6, bytes_accessed=2 ** 21 * total, transcendentals=0),
        name="pack_pages",
    )(send_slot, k_pool, v_pool)


def keep_kernel(depth, lead, from_ref, k_ref, v_ref, k_out, v_out, buf, listed, sems_in, sems_out):
    count = compact(from_ref.shape[0], lambda i: from_ref[i] < 0, lambda i: i, listed)

    def ins(i):
        at = lax.rem(i, depth)
        return [pltpu.make_async_copy(ref.at[listed[i]], buf.at[at, h], sems_in.at[at, h]) for h, ref in enumerate((k_ref, v_ref))]

    def outs(i):
        at = lax.rem(i, depth)
        return [pltpu.make_async_copy(buf.at[at, h], ref.at[listed[i]], sems_out.at[at, h]) for h, ref in enumerate((k_out, v_out))]

    ring(
        count, depth, lead,
        lambda i: [c.start() for c in ins(i)],
        lambda i: [c.wait() for c in ins(i)],
        lambda i: [c.start() for c in outs(i)],
        lambda i: [c.wait() for c in outs(i)],
    )


def keep_pages(from_page, k_pool, v_pool):
    depth, lead = 24, 12
    return pl.pallas_call(
        functools.partial(keep_kernel, depth, lead),
        out_shape=[jax.ShapeDtypeStruct(k_pool.shape, k_pool.dtype)] * 2,
        in_specs=[SMEM] + [ANY] * 2,
        out_specs=[ANY] * 2,
        scratch_shapes=[
            pltpu.VMEM((depth, 2) + k_pool.shape[1:], k_pool.dtype),
            pltpu.SMEM((k_pool.shape[0],), jnp.int32),
            pltpu.SemaphoreType.DMA((depth, 2)),
            pltpu.SemaphoreType.DMA((depth, 2)),
        ],
        cost_estimate=pl.CostEstimate(flops=10 ** 6, bytes_accessed=2 ** 25, transcendentals=0),
        name="keep_pages",
    )(from_page, k_pool, v_pool)


def place_kernel(depth, lead, plan, from_ref, *rest):
    arrived, rest = rest[:len(plan)], rest[len(plan):]
    k_out, v_out, buf, listed, sems_in, sems_out = rest[2:]
    pools = (k_out, v_out)
    peers = arrived[0].shape[0]
    slots = from_ref.shape[0]
    for part, (r, halves) in enumerate(plan):
        count = compact(slots, lambda i: (from_ref[i] >= r * peers) & (from_ref[i] < (r + 1) * peers), lambda i: i, listed)

        def ins(i):
            at = lax.rem(i, depth)
            line = from_ref[listed[i]] - r * peers
            return [pltpu.make_async_copy(arrived[part].at[line, k], buf.at[at, h], sems_in.at[at, h]) for k, h in enumerate(halves)]

        def outs(i):
            at = lax.rem(i, depth)
            return [pltpu.make_async_copy(buf.at[at, h], pools[h].at[listed[i]], sems_out.at[at, h]) for h in halves]

        ring(
            count, depth, lead,
            lambda i: [c.start() for c in ins(i)],
            lambda i: [c.wait() for c in ins(i)],
            lambda i: [c.start() for c in outs(i)],
            lambda i: [c.wait() for c in outs(i)],
        )


def place_pages(plan, from_page, arrived, k_out, v_out):
    depth, lead = 24, 12
    return pl.pallas_call(
        functools.partial(place_kernel, depth, lead, plan),
        out_shape=[jax.ShapeDtypeStruct(k_out.shape, k_out.dtype)] * 2,
        in_specs=[SMEM] + [ANY] * (len(arrived) + 2),
        out_specs=[ANY] * 2,
        scratch_shapes=[
            pltpu.VMEM((depth, 2) + k_out.shape[1:], k_out.dtype),
            pltpu.SMEM((k_out.shape[0],), jnp.int32),
            pltpu.SemaphoreType.DMA((depth, 2)),
            pltpu.SemaphoreType.DMA((depth, 2)),
        ],
        input_output_aliases={1 + len(arrived): 0, 2 + len(arrived): 1},
        cost_estimate=pl.CostEstimate(flops=10 ** 6, bytes_accessed=2 ** 22 * len(arrived), transcendentals=0),
        name="place_pages",
    )(from_page, *arrived, k_out, v_out)


def close_kernel(seq_dev, first_line, n_layers, from_ref, first_ref, second_ref, offset_ref, k_came, v_came, *rest):
    rows = rest[:2 * n_layers]
    k_out, v_out, buf, listed, staged, early, late, sems_in, sem_out, sem_row = rest[2 * n_layers + 2:]
    pools, arrived = (k_out, v_out), (k_came, v_came)
    peers = k_came.shape[0]
    slots, n_batch = from_ref.shape[0], offset_ref.shape[0]
    heads = k_out.shape[3]
    most = early.shape[0]

    def ins(i, line):
        return [pltpu.make_async_copy(ref.at[line], buf.at[i, h], sems_in.at[i]) for h, ref in enumerate(arrived)]

    def outs(i, slot):
        return [pltpu.make_async_copy(buf.at[i, h], pools[h].at[slot], sem_out.at[0]) for h in range(2)]

    def fetch(at, seq, step):
        home, place = seq // seq_dev, lax.rem(seq, seq_dev)
        return [
            pltpu.make_async_copy(
                rows[2 * layer + h].at[lax.rem(home, 2), home // 2, place, pl.ds(step * heads, heads)], staged.at[at, layer, h], sem_row.at[0]
            )
            for layer in range(n_layers) for h in range(2)
        ]

    def write(at, slot, layer_offset, sem):
        return [
            pltpu.make_async_copy(staged.at[at, layer, h], pools[h].at[slot, layer, layer_offset], sem_row.at[sem])
            for layer in range(n_layers) for h in range(2)
        ]

    def scan(slot, counts):
        pages, n_early, n_late = counts
        line = from_ref[slot] - first_line
        moved = (line >= 0) & (line < peers)

        @pl.when(moved)
        def _():
            listed[pages] = slot
            for c in ins(pages, line):
                c.start()

        for step, ref in enumerate((first_ref, second_ref)):
            seq = ref[slot]
            entry = (slot * 2 + step) * n_batch + seq

            @pl.when((seq >= 0) & moved)
            def _():
                late[n_late] = entry
                for c in fetch(most - 1 - n_late, seq, step):
                    c.start()

            @pl.when((seq >= 0) & jnp.logical_not(moved))
            def _():
                early[n_early] = entry
                for c in fetch(n_early, seq, step):
                    c.start()

            n_late = n_late + ((seq >= 0) & moved).astype(jnp.int32)
            n_early = n_early + ((seq >= 0) & jnp.logical_not(moved)).astype(jnp.int32)
        return pages + moved.astype(jnp.int32), n_early, n_late

    pages, n_early, n_late = lax.fori_loop(0, slots, scan, (jnp.int32(0), jnp.int32(0), jnp.int32(0)))

    def pass_on(i, carry):
        for c in ins(i, 0):
            c.wait()
        for c in outs(i, listed[i]):
            c.start()
        return carry

    lax.fori_loop(0, pages, pass_on, 0)

    def fetched(i, carry):
        for c in fetch(0, 0, 0):
            c.wait()
        return carry

    lax.fori_loop(0, n_early + n_late, fetched, 0)

    def write_row(entries, at, sem):
        def body(i, carry):
            entry = entries[i]
            seq, where = lax.rem(entry, n_batch), entry // n_batch
            for c in write(at(i), where // 2, offset_ref[seq] + lax.rem(where, 2), sem):
                c.start()
            return carry
        return body

    lax.fori_loop(0, n_early, write_row(early, lambda i: i, 1), 0)

    def placed(i, carry):
        for c in outs(i, 0):
            c.wait()
        return carry

    lax.fori_loop(0, pages, placed, 0)
    lax.fori_loop(0, n_late, write_row(late, lambda i: most - 1 - i, 1), 0)

    def written(i, carry):
        for c in write(0, 0, 0, 1):
            c.wait()
        return carry

    lax.fori_loop(0, n_early + n_late, written, 0)


def close_pools(seq_dev, last_round, from_page, first_seq, second_seq, offsets, arrived, rows, k_out, v_out):
    peers, slots = arrived[0].shape[0], k_out.shape[0]
    first_pool = 6 + len(rows)
    return pl.pallas_call(
        functools.partial(close_kernel, seq_dev, last_round * peers, len(rows) // 2),
        out_shape=[jax.ShapeDtypeStruct(k_out.shape, k_out.dtype)] * 2,
        in_specs=[SMEM] * 4 + [ANY] * (4 + len(rows)),
        out_specs=[ANY] * 2,
        scratch_shapes=[
            pltpu.VMEM((peers, 2) + k_out.shape[1:], k_out.dtype),
            pltpu.SMEM((peers,), jnp.int32),
            pltpu.VMEM((2 * slots, len(rows) // 2, 2) + k_out.shape[3:], k_out.dtype),
            pltpu.SMEM((2 * slots,), jnp.int32),
            pltpu.SMEM((2 * slots,), jnp.int32),
            pltpu.SemaphoreType.DMA((peers,)),
            pltpu.SemaphoreType.DMA((1,)),
            pltpu.SemaphoreType.DMA((2,)),
        ],
        input_output_aliases={first_pool: 0, first_pool + 1: 1},
        cost_estimate=pl.CostEstimate(flops=10 ** 6, bytes_accessed=2 ** 23, transcendentals=0),
        name="close_pools",
    )(from_page, first_seq, second_seq, offsets, *[a.reshape((peers,) + a.shape[2:]) for a in arrived], *rows, k_out, v_out)


def attend_kernel(block, pages_seq, seq_dev, page_size, scale, code_ref, q_ref, k_ref, v_ref, acc_ref):
    rows, head_dim = q_ref.shape[-2:]
    heads = k_ref.shape[3]
    chips = acc_ref.shape[1]
    step = pl.program_id(0)

    @pl.when(step == 0)
    def _():
        for core in range(2):
            acc_ref[core, :, :seq_dev] = jnp.zeros((chips, seq_dev, rows, head_dim), jnp.float32)
            lane = lax.broadcasted_iota(jnp.int32, (chips, 1, rows, head_dim), 3)
            acc_ref[core, :, seq_dev:] = jnp.where(lax.rem(lane, 2) == 0, LOW, 0.0)

    row = lax.broadcasted_iota(jnp.int32, (rows, page_size * heads), 0)
    column = lax.broadcasted_iota(jnp.int32, (rows, page_size * heads), 1)
    same_head = lax.rem(row, heads) == lax.rem(column, heads)
    position = jnp.where(same_head, column // heads, page_size)
    lane = lax.broadcasted_iota(jnp.int32, (rows, head_dim), 1)
    found = []
    for s in range(block):
        code = code_ref[step * block + s]
        held = jnp.maximum(code, 0)
        seen = jnp.where(code >= 0, lax.rem(held, 2 * page_size), 0)
        seq = held // (2 * page_size * pages_seq)
        home, place = seq // seq_dev, lax.rem(seq, seq_dev)
        core, chip = lax.rem(home, 2), home // 2
        q = q_ref[core, chip, place]
        keys = k_ref[s, 0].reshape(page_size * heads, head_dim)
        values = v_ref[s, 0].reshape(page_size * heads, head_dim)
        scores = lax.dot_general(q, keys, (((1,), (1,)), ((), ())), preferred_element_type=jnp.float32) * scale
        mask = position < seen
        scores = jnp.where(mask, scores, LOW)
        top = jnp.max(scores, axis=1, keepdims=True)
        weights = jnp.where(mask, jnp.exp(scores - top), 0.0)
        total = jnp.sum(weights, axis=1, keepdims=True)
        high = weights.astype(jnp.bfloat16)
        low = (weights - high.astype(jnp.float32)).astype(jnp.bfloat16)
        mixed = jnp.dot(high, values, preferred_element_type=jnp.float32) + jnp.dot(low, values, preferred_element_type=jnp.float32)
        found.append((core, chip, place, top, total, mixed))
    for core, chip, place, top, total, mixed in found:
        stats = acc_ref[core, chip, seq_dev]
        old_top = jnp.max(jnp.where(lane == 2 * place, stats, LOW), axis=1, keepdims=True)
        old_total = jnp.sum(jnp.where(lane == 2 * place + 1, stats, 0.0), axis=1, keepdims=True)
        new_top = jnp.maximum(top, old_top)
        old_part, new_part = jnp.exp(old_top - new_top), jnp.exp(top - new_top)
        acc_ref[core, chip, place] = acc_ref[core, chip, place] * old_part + mixed * new_part
        new_total = old_total * old_part + total * new_part
        acc_ref[core, chip, seq_dev] = jnp.where(lane == 2 * place, new_top, jnp.where(lane == 2 * place + 1, new_total, stats))


def attend_pages(code, q_all, k_pool, v_pool, layer, pages_seq):
    slots, _, page_size, heads, head_dim = k_pool.shape
    cores, chips, seq_dev, rows, _ = q_all.shape
    block = 8
    page_spec = pl.BlockSpec((block, 1, page_size, heads, head_dim), lambda i, c: (i, layer, 0, 0, 0))
    query_spec = pl.BlockSpec(q_all.shape, lambda i, c: (0,) * 5)
    acc_shape = (cores, chips, seq_dev + 1, rows, head_dim)
    return pl.pallas_call(
        functools.partial(attend_kernel, block, pages_seq, seq_dev, page_size, head_dim ** -0.5),
        out_shape=jax.ShapeDtypeStruct(acc_shape, jnp.float32),
        grid_spec=pltpu.PrefetchScalarGridSpec(
            num_scalar_prefetch=1,
            grid=(slots // block,),
            in_specs=[query_spec, page_spec, page_spec],
            out_specs=pl.BlockSpec(acc_shape, lambda i, c: (0,) * 5),
        ),
        compiler_params=pltpu.CompilerParams(dimension_semantics=("arbitrary",)),
        cost_estimate=pl.CostEstimate(flops=10 ** 6, bytes_accessed=2 * slots * page_size * heads * head_dim * 2, transcendentals=0),
        name="attend_pages",
    )(code, q_all, k_pool, v_pool)


def spread_kernel(n, x_ref, out_ref, held, send_sem, recv_sem, pass_sem, got_sem, copy_sem):
    me = lax.axis_index("kv")
    chips = n // 2
    core, chip = lax.rem(me, 2), me // 2
    barrier = pltpu.get_barrier_semaphore()

    def greet(j, carry):
        pl.semaphore_signal(barrier, inc=1, device_id={"kv": 2 * lax.rem(chip + j, chips) + core}, device_id_type=MESH)
        return carry

    lax.fori_loop(1, chips, greet, 0)
    pl.semaphore_signal(barrier, inc=1, device_id={"kv": me + 1 - 2 * core}, device_id_type=MESH)
    pl.semaphore_wait(barrier, chips)
    spread_body(n, x_ref, out_ref, held, send_sem, recv_sem, pass_sem, got_sem, copy_sem)


def spread_body(n, x_ref, out_ref, held, send_sem, recv_sem, pass_sem, got_sem, copy_sem, behind=lambda: None):
    me = lax.axis_index("kv")
    chips = n // 2
    core, chip = lax.rem(me, 2), me // 2
    other = me + 1 - 2 * core

    def peer(j):
        return 2 * lax.rem(chip + j, chips) + core

    def send(j):
        return pltpu.make_async_remote_copy(
            src_ref=x_ref, dst_ref=held.at[core, chip], send_sem=send_sem.at[j], recv_sem=recv_sem.at[chip],
            device_id={"kv": peer(j)}, device_id_type=MESH,
        )

    def forward(source, at):
        return pltpu.make_async_remote_copy(
            src_ref=source, dst_ref=held.at[core, at], send_sem=pass_sem.at[at], recv_sem=got_sem.at[at],
            device_id={"kv": other}, device_id_type=MESH,
        )

    offsets, side = chip_offsets(chips)
    for offset in offsets:
        send(lax.rem(chip_at(chip, offset, side, chips) + chips - chip, chips)).start()
    own = forward(x_ref, chip)
    own.start()
    mine = pltpu.make_async_copy(x_ref, out_ref.at[core, chip], copy_sem.at[0])
    mine.start()
    behind()

    for offset in offsets:
        at = chip_from(chip, offset, side, chips)
        j = lax.rem(chip + chips - at, chips)
        pltpu.make_async_remote_copy(
            src_ref=x_ref, dst_ref=held.at[core, at], send_sem=send_sem.at[j], recv_sem=recv_sem.at[at],
            device_id={"kv": other}, device_id_type=MESH,
        ).wait_recv()
        forward(held.at[core, at], at).start()
        pltpu.make_async_copy(held.at[core, at], out_ref.at[core, at], copy_sem.at[j]).start()

    def passed(j, carry):
        at = lax.rem(chip + j, chips)
        pltpu.make_async_remote_copy(
            src_ref=x_ref, dst_ref=held.at[1 - core, at], send_sem=pass_sem.at[at], recv_sem=got_sem.at[at],
            device_id={"kv": other}, device_id_type=MESH,
        ).wait_recv()
        pltpu.make_async_copy(held.at[1 - core, at], out_ref.at[1 - core, at], copy_sem.at[chips + j]).start()
        return carry

    lax.fori_loop(0, chips, passed, 0)

    own.wait_send()
    mine.wait()

    def finish(j, carry):
        at = lax.rem(chip + chips - j, chips)
        send(j).wait_send()
        forward(held.at[core, at], at).wait_send()
        pltpu.make_async_copy(held.at[core, at], out_ref.at[core, at], copy_sem.at[j]).wait()
        return carry

    lax.fori_loop(1, chips, finish, 0)

    def written(j, carry):
        at = lax.rem(chip + j, chips)
        pltpu.make_async_copy(held.at[1 - core, at], out_ref.at[1 - core, at], copy_sem.at[chips + j]).wait()
        return carry

    lax.fori_loop(0, chips, written, 0)


def spread(x, n):
    chips = n // 2
    return pl.pallas_call(
        functools.partial(spread_kernel, n),
        out_shape=jax.ShapeDtypeStruct((2, chips) + x.shape, x.dtype),
        in_specs=[VMEM],
        out_specs=ANY,
        scratch_shapes=[
            pltpu.VMEM((2, chips) + x.shape, x.dtype),
            pltpu.SemaphoreType.DMA((chips,)),
            pltpu.SemaphoreType.DMA((chips,)),
            pltpu.SemaphoreType.DMA((chips,)),
            pltpu.SemaphoreType.DMA((chips,)),
            pltpu.SemaphoreType.DMA((n,)),
        ],
        compiler_params=pltpu.CompilerParams(collective_id=0, has_side_effects=True),
        name="spread_rows",
    )(x)


def pack_stats(x):
    parts = x.shape[0] // 8
    span = x.shape[1] // parts
    lane = lax.broadcasted_iota(jnp.int32, (8, x.shape[1]), 1)
    out = x[:8]
    for g in range(1, parts):
        out = jnp.where(lane // span == g, pltpu.roll(x[8 * g:8 * g + 8], span * g, 1), out)
    return out


def unpack_stats(x, rows):
    span = x.shape[1] // (rows // 8)
    return jnp.concatenate([x] + [pltpu.roll(x, x.shape[1] - span * g, 1) for g in range(1, rows // 8)], axis=0)


def lane_before(x):
    return pltpu.roll(x, x.shape[1] - 1, 1)


def merge_chip_kernel(acc_ref, sums_ref, near, send_sem, recv_sem):
    me = lax.axis_index("kv")
    core = lax.rem(me, 2)
    other = me + 1 - 2 * core
    chips, blocks, rows, head_dim = near.shape
    seq_dev = blocks - 1

    barrier = pltpu.get_barrier_semaphore()
    pl.semaphore_signal(barrier, inc=1, device_id={"kv": other}, device_id_type=MESH)
    pl.semaphore_wait(barrier, 1)

    swap = pltpu.make_async_remote_copy(
        src_ref=acc_ref.at[1 - core], dst_ref=near, send_sem=send_sem.at[0], recv_sem=recv_sem.at[0],
        device_id={"kv": other}, device_id_type=MESH,
    )
    swap.start()
    even = lax.rem(lax.broadcasted_iota(jnp.int32, (rows, head_dim), 1), 2) == 0
    swap.wait_recv()

    def merge(at, carry):
        mine, theirs = acc_ref[core, at, seq_dev], near[at, seq_dev]
        top = jnp.maximum(mine, theirs)
        a, b = jnp.exp(mine - top), jnp.exp(theirs - top)
        total = a * lane_before(mine) + b * lane_before(theirs)
        sums_ref[at, seq_dev * rows:] = pack_stats(jnp.where(even, top, pltpu.roll(total, 1, 1)))
        for i in range(seq_dev):
            sums_ref[at, i * rows:(i + 1) * rows] = a[:, 2 * i:2 * i + 1] * acc_ref[core, at, i] + b[:, 2 * i:2 * i + 1] * near[at, i]
        return carry

    lax.fori_loop(0, chips, merge, 0)
    swap.wait_send()


def merge_chip(acc):
    blocks = acc.shape[1:]
    return pl.pallas_call(
        merge_chip_kernel,
        out_shape=jax.ShapeDtypeStruct((blocks[0], (blocks[1] - 1) * blocks[2] + 8, blocks[3]), acc.dtype),
        in_specs=[VMEM],
        out_specs=VMEM,
        scratch_shapes=[
            pltpu.VMEM(blocks, acc.dtype),
            pltpu.SemaphoreType.DMA((1,)),
            pltpu.SemaphoreType.DMA((1,)),
        ],
        compiler_params=pltpu.CompilerParams(collective_id=2, has_side_effects=True),
        cost_estimate=pl.CostEstimate(flops=10 ** 6, bytes_accessed=2 ** 23, transcendentals=0),
        name="merge_chip",
    )(acc)


def layer_kernel(n, scale, layer, follow, *refs):
    sums_ref, x_ref, hid_ref, chunk_ref, wo_ref, wu_ref, wd_ref = refs[:7]
    refs = refs[7:]
    hid_out, got_ref = refs[:2]
    refs = refs[2:]
    if follow:
        all_out, refs = refs[0], refs[1:]
    held, o_scr, rows_scr, mid_scr, acc_scr, wide, up, down, wide_sem, up_sem, down_sem, send_sem, recv_sem, page_send, page_recv = refs[:15]
    refs = refs[15:]
    me = lax.axis_index("kv")
    _, seq_dev, rows, head_dim = x_ref.shape
    heads = rows // 2
    chips = n // 2
    core, chip = lax.rem(me, 2), me // 2
    hid_rows, width = hid_ref.shape
    tile, up_tile = wide.shape[2], up.shape[2]
    up_slots = up.shape[0]
    n_wide, n_up = width // tile, wu_ref.shape[2] // up_tile

    def peer(j):
        return 2 * lax.rem(chip + j, chips) + core

    def anyone(j):
        return lax.rem(me + j, n)

    barrier = pltpu.get_barrier_semaphore()

    def greet(j, carry):
        pl.semaphore_signal(barrier, inc=1, device_id={"kv": anyone(j)}, device_id_type=MESH)
        return carry

    lax.fori_loop(1, n, greet, 0)

    def wide_copy(w, at, t, slot):
        return pltpu.make_async_copy(w.at[at, :, pl.ds(pl.multiple_of(t * tile, tile), tile)], wide.at[slot], wide_sem.at[slot])

    def up_copy(t):
        slot = lax.rem(t, up_slots)
        return pltpu.make_async_copy(wu_ref.at[layer, :, pl.ds(pl.multiple_of(t * up_tile, up_tile), up_tile)], up.at[slot], up_sem.at[slot])

    def down_copy(t):
        slot = lax.rem(t, up_slots)
        return pltpu.make_async_copy(wd_ref.at[layer, pl.ds(pl.multiple_of(t * up_tile, up_tile), up_tile)], down.at[slot], down_sem.at[slot])

    for t in range(n_wide):
        wide_copy(wo_ref, layer, t, t).start()
    for t in range(up_slots):
        up_copy(t).start()
        down_copy(t).start()
    pl.semaphore_wait(barrier, n - 1)

    def send(j):
        return pltpu.make_async_remote_copy(
            src_ref=sums_ref.at[lax.rem(chip + j, chips)], dst_ref=held.at[chip], send_sem=send_sem.at[j], recv_sem=recv_sem.at[chip],
            device_id={"kv": peer(j)}, device_id_type=MESH,
        )

    def send_pages(j):
        return pltpu.make_async_remote_copy(
            src_ref=chunk_ref.at[anyone(j)], dst_ref=got_ref.at[me], send_sem=page_send.at[j], recv_sem=page_recv.at[me],
            device_id={"kv": anyone(j)}, device_id_type=MESH,
        )

    offsets, side = chip_offsets(chips)
    for offset in offsets:
        send(lax.rem(chip_at(chip, offset, side, chips) + chips - chip, chips)).start()
    def send_chunk(some):
        for offset in some:
            for other_core in range(2):
                to = 2 * chip_at(chip, offset, side, chips) + lax.rem(core + other_core, 2)
                send_pages(lax.rem(to + n - me, n)).start()

    at_once = 3 * len(offsets) // 5 if follow else len(offsets)
    send_chunk(offsets[:at_once])
    send_pages(lax.rem(me + 1 - 2 * core + n - me, n)).start()
    held[chip] = sums_ref[chip]

    queries = [x_ref[0, i].astype(jnp.float32) for i in range(seq_dev)]
    second_row = lax.broadcasted_iota(jnp.int32, (rows, 1), 0) >= heads

    def twice(h, i, step):
        x = x_ref[1 + h, i, step * heads:(step + 1) * heads].astype(jnp.float32)
        return jnp.concatenate([x, x], axis=0)

    first = [jnp.sum(queries[i] * twice(0, i, 0), axis=1, keepdims=True) * scale for i in range(seq_dev)]
    second = [
        jnp.where(second_row, jnp.sum(queries[i] * twice(0, i, 1), axis=1, keepdims=True) * scale, LOW)
        for i in range(seq_dev)
    ]

    def arrive(j, carry):
        at = lax.rem(chip + chips - j, chips)
        pltpu.make_async_remote_copy(
            src_ref=sums_ref.at[at], dst_ref=held.at[at], send_sem=send_sem.at[j], recv_sem=recv_sem.at[at],
            device_id={"kv": peer(j)}, device_id_type=MESH,
        ).wait_recv()
        return carry

    lax.fori_loop(1, chips, arrive, 0)

    def highest(j, top):
        return jnp.maximum(top, held[j, seq_dev * rows:])

    top_all = unpack_stats(lax.fori_loop(0, chips, highest, jnp.full((8, head_dim), LOW, jnp.float32)), rows)
    tops, totals, mixed = [], [], []
    for i in range(seq_dev):
        top = jnp.maximum(jnp.maximum(top_all[:, 2 * i:2 * i + 1], first[i]), second[i])
        p_first, p_second = jnp.exp(first[i] - top), jnp.exp(second[i] - top)
        tops.append(top)
        totals.append(p_first + p_second)
        mixed.append(p_first * twice(1, i, 0) + p_second * twice(1, i, 1))

    def merge(j, carry):
        totals, mixed = carry
        stats = unpack_stats(held[j, seq_dev * rows:], rows)
        new_totals, new_mixed = [], []
        for i in range(seq_dev):
            weight = jnp.exp(stats[:, 2 * i:2 * i + 1] - tops[i])
            new_totals.append(totals[i] + weight * stats[:, 2 * i + 1:2 * i + 2])
            new_mixed.append(mixed[i] + weight * held[j, i * rows:(i + 1) * rows])
        return tuple(new_totals), tuple(new_mixed)

    totals, mixed = lax.fori_loop(0, chips, merge, (tuple(totals), tuple(mixed)))
    for i in range(seq_dev):
        o_scr[i * rows:(i + 1) * rows] = (mixed[i] / totals[i]).astype(jnp.bfloat16).astype(jnp.float32)
    for h in range(heads):
        rows_scr[:, h * head_dim:(h + 1) * head_dim] = o_scr[pl.ds(h, hid_rows, stride=heads), :].astype(jnp.bfloat16)

    def add_out(t, carry):
        wide_copy(wo_ref, layer, t, t).wait()
        cut = pl.ds(pl.multiple_of(t * tile, tile), tile)
        part = jnp.dot(rows_scr[...], wide[t], preferred_element_type=jnp.float32)
        mid_scr[:, cut] = (hid_ref[:, cut].astype(jnp.float32) + part).astype(jnp.bfloat16)
        return carry

    lax.fori_loop(0, n_wide, add_out, 0)
    acc_scr[...] = jnp.zeros_like(acc_scr)

    def mlp(t, carry):
        slot = lax.rem(t, up_slots)
        up_copy(t).wait()
        inner = jax.nn.gelu(jnp.dot(mid_scr[...], up[slot], preferred_element_type=jnp.float32)).astype(jnp.bfloat16)
        down_copy(t).wait()
        acc_scr[...] += jnp.dot(inner, down[slot], preferred_element_type=jnp.float32)

        @pl.when(t + up_slots < n_up)
        def _():
            up_copy(t + up_slots).start()
            down_copy(t + up_slots).start()

        return carry

    lax.fori_loop(0, n_up, mlp, 0)
    hid_out[...] = (mid_scr[...].astype(jnp.float32) + acc_scr[...]).astype(jnp.bfloat16)

    def finish(j, carry):
        send(j).wait_send()
        return carry

    lax.fori_loop(1, chips, finish, 0)
    if follow:
        all_held, pass_send, pass_recv, spread_send, spread_recv, copy_sem = refs
        spread_body(
            n, hid_out, all_out, all_held, spread_send, spread_recv, pass_send, pass_recv, copy_sem, lambda: send_chunk(offsets[at_once:])
        )

    def pages_came(j, carry):
        at = lax.rem(me + n - j, n)
        pltpu.make_async_remote_copy(
            src_ref=chunk_ref.at[at], dst_ref=got_ref.at[at], send_sem=page_send.at[j], recv_sem=page_recv.at[at],
            device_id={"kv": anyone(j)}, device_id_type=MESH,
        ).wait_recv()
        send_pages(j).wait_send()
        return carry

    lax.fori_loop(1, n, pages_came, 0)


def end_layer(sums, x, hidden, chunk, w_out, w_up, w_down, layer, follow, n):
    chips = n // 2
    hid_rows, width = hidden.shape
    seq_dev, rows, head_dim = x.shape[1:]
    tile, up_slots = 512, 3
    wide_slots = width // tile
    out_shape = [jax.ShapeDtypeStruct(hidden.shape, hidden.dtype), jax.ShapeDtypeStruct(chunk.shape, chunk.dtype)]
    out_specs = [VMEM, ANY]
    scratch = [
        pltpu.VMEM(sums.shape, sums.dtype),
        pltpu.VMEM((seq_dev * rows, head_dim), jnp.float32),
        pltpu.VMEM(hidden.shape, jnp.bfloat16),
        pltpu.VMEM(hidden.shape, jnp.bfloat16),
        pltpu.VMEM(hidden.shape, jnp.float32),
        pltpu.VMEM((wide_slots, width, tile), w_out.dtype),
        pltpu.VMEM((up_slots, width, tile), w_up.dtype),
        pltpu.VMEM((up_slots, tile, width), w_down.dtype),
        pltpu.SemaphoreType.DMA((wide_slots,)),
        pltpu.SemaphoreType.DMA((up_slots,)),
        pltpu.SemaphoreType.DMA((up_slots,)),
        pltpu.SemaphoreType.DMA((chips,)),
        pltpu.SemaphoreType.DMA((chips,)),
        pltpu.SemaphoreType.DMA((n,)),
        pltpu.SemaphoreType.DMA((n,)),
    ]
    if follow:
        spread_shape = (2, chips) + hidden.shape
        out_shape += [jax.ShapeDtypeStruct(spread_shape, hidden.dtype)]
        out_specs += [ANY]
        scratch += [pltpu.VMEM(spread_shape, hidden.dtype)]
        scratch += [pltpu.SemaphoreType.DMA((chips,))] * 4 + [pltpu.SemaphoreType.DMA((n,))]
    return pl.pallas_call(
        functools.partial(layer_kernel, n, head_dim ** -0.5, layer, follow),
        out_shape=out_shape,
        in_specs=[VMEM] * 3 + [ANY] * 4,
        out_specs=out_specs,
        scratch_shapes=scratch,
        compiler_params=pltpu.CompilerParams(collective_id=3 + layer, has_side_effects=True),
        cost_estimate=pl.CostEstimate(flops=10 ** 10, bytes_accessed=2 ** 27, transcendentals=0),
        name="end_layer",
    )(sums, x, hidden, chunk, w_out, w_up, w_down)


def solution(mesh):
    groups = mesh.shape['kv']
    rows_spec = P(None, ('rep', 'kv'), None)
    pool_spec = P(('rep', 'kv'))
    table_spec = P('rep', None)
    vec_spec = P('rep')
    full_spec = P()

    def device_fn(embeds, w_query, w_key, w_value, w_out, w_up, w_down, k_pool, v_pool, old_table, new_table, seq_len, finished, mig_src, mig_dst):
        me = lax.axis_index('kv')
        slots, n_layers, page_size, heads, head_dim = k_pool.shape
        steps, seq_dev, width = embeds.shape
        n_batch, pages_seq = old_table.shape
        n_mig = mig_src.shape[0]
        rounds = 4 * n_mig // (groups * groups)
        base = me * slots
        local = jnp.arange(slots, dtype=jnp.int32)
        active = finished == 0
        last = pages_seq - 1

        def find(match, value):
            return jnp.max(jnp.where(match, value, -1), axis=1)

        flat = old_table.reshape(-1)
        place = jnp.arange(n_batch * pages_seq, dtype=jnp.int32)
        seen = jnp.clip(seq_len[:, None] - jnp.arange(pages_seq, dtype=jnp.int32)[None, :] * page_size, 0, page_size).reshape(-1)
        code = find(flat[None, :] - base == local[:, None], (place * (2 * page_size) + seen)[None, :])

        src_dev, dst_dev = mig_src // slots, mig_dst // slots
        pair = src_dev * groups + dst_dev
        entry = jnp.arange(n_mig, dtype=jnp.int32)
        rank = jnp.sum((pair[None, :] == pair[:, None]) & (entry[None, :] < entry[:, None]), axis=1, dtype=jnp.int32)
        lines = jnp.arange(rounds * groups, dtype=jnp.int32)
        send_slot = find(
            ((rank * groups + dst_dev)[None, :] == lines[:, None]) & (src_dev == me)[None, :], (mig_src - src_dev * slots)[None, :]
        )
        from_page = find((mig_dst - base)[None, :] == local[:, None], (rank * groups + src_dev)[None, :])

        seq_ids = jnp.arange(n_batch, dtype=jnp.int32)
        owner_old = find((old_table[:, last] - base)[None, :] == local[:, None], seq_ids[None, :])
        owner_new = find(((new_table[:, last] - base)[None, :] == local[:, None]) & active[None, :], seq_ids[None, :])
        first_seq = jnp.where(from_page >= 0, owner_new, owner_old)
        second_seq = owner_new
        offsets = lax.rem(seq_len, page_size)

        def exchange(block):
            return lax.all_to_all(block, 'kv', 0, 0, tiled=True)

        def send_next(value, count):
            for block in packed[len(got):len(got) + count]:
                block, value = lax.optimization_barrier((block, value))
                got.append(exchange(block))
            return value

        plan = tuple((r, (0, 1)) for r in range(rounds - 1)) + ((rounds - 1, (0,)), (rounds - 1, (1,)))
        packed = list(pack_pages(plan[:1], send_slot, k_pool, v_pool, groups))
        packed[0], send_slot = lax.optimization_barrier((packed[0], send_slot))
        packed += list(pack_pages(plan[1:], send_slot, k_pool, v_pool, groups))
        got = []
        tables = (from_page, first_seq, second_seq, offsets)
        k_out, v_out = keep_pages(from_page, k_pool, v_pool)

        hidden = jnp.transpose(embeds, (1, 0, 2)).reshape(seq_dev * steps, width)
        every = spread(hidden, groups)
        rows = []
        for layer in range(n_layers):
            every, got = lax.optimization_barrier((every, got))
            every = send_next(every, 1)
            flat_rows = every.reshape(groups * seq_dev * steps, width)
            every_x = [
                jnp.dot(flat_rows, w[layer], preferred_element_type=jnp.float32).astype(jnp.bfloat16)
                .reshape(2, groups // 2, seq_dev, steps * heads, head_dim)
                for w in (w_query, w_key, w_value)
            ]
            rows += every_x[1:]
            x = jnp.stack([y[lax.rem(me, 2), me // 2] for y in every_x])
            sums = merge_chip(attend_pages(code, every_x[0], k_pool, v_pool, layer, pages_seq))
            if layer:
                k_out, v_out = place_pages(plan[:2], from_page, got[:2], k_out, v_out)
            sums, k_out, v_out, packed = lax.optimization_barrier((sums, k_out, v_out, packed))
            hidden, pages, *ahead = end_layer(
                sums, x, hidden, packed[len(got)], w_out, w_up, w_down, layer, layer + 1 < n_layers, groups
            )
            got.append(pages)
            if ahead:
                (every,) = ahead
        k_out, v_out = close_pools(seq_dev, rounds - 1, *tables, got[2:], rows, k_out, v_out)
        hidden = jnp.transpose(hidden.reshape(seq_dev, steps, width), (1, 0, 2))
        done = lax.dynamic_slice(finished, (me * seq_dev,), (seq_dev,)) != 0
        live = jnp.stack([jnp.ones_like(done), ~done])
        hidden = jnp.where(live[:, :, None], hidden, jnp.zeros_like(hidden))
        return hidden, k_out, v_out

    in_specs = (rows_spec, full_spec, full_spec, full_spec, full_spec, full_spec, full_spec, pool_spec, pool_spec, table_spec, table_spec, vec_spec, vec_spec, vec_spec, vec_spec)
    return jax.shard_map(device_fn, mesh=mesh, in_specs=in_specs, out_specs=(rows_spec, pool_spec, pool_spec), check_vma=False)
```

```python
import functools

import jax
import jax.numpy as jnp
from jax import lax
from jax.experimental import pallas as pl
from jax.experimental.pallas import tpu as pltpu
from jax.sharding import PartitionSpec as P

MESH = pl.DeviceIdType.MESH
ANY = pl.BlockSpec(memory_space=pl.ANY)
VMEM = pl.BlockSpec(memory_space=pltpu.VMEM)
SMEM = pl.BlockSpec(memory_space=pltpu.SMEM)
LOW = -1e30


def chip_offsets(chips):
    side = 1
    while side * side < chips:
        side += 1
    if side * side != chips:
        return [(j, 0) for j in range(1, chips)], chips

    def near(d):
        d %= side
        return d if 2 * d <= side else d - side

    def cost(offset):
        x, y = near(offset[0]), near(offset[1])
        return (x == 0 or y == 0, 2 * abs(x) == side or 2 * abs(y) == side, x == 0, abs(x) + abs(y), abs(x), abs(y), x * y < 0, x)

    every = [(x, y) for x in range(side) for y in range(side) if x or y]
    return sorted(every, key=cost), side


def chip_at(chip, offset, side, chips):
    x, y = offset
    return lax.rem(chip // side + y, chips // side) * side + lax.rem(lax.rem(chip, side) + x, side)


def chip_from(chip, offset, side, chips):
    x, y = offset
    return chip_at(chip, ((side - x) % side, (chips // side - y) % (chips // side)), side, chips)


def ring(count, depth, lead, start_in, wait_in, start_out, wait_out):
    def body(i, carry):
        @pl.when(i < count)
        def _():
            @pl.when(i >= depth)
            def _():
                wait_out(i - depth)

            start_in(i)

        @pl.when(i >= lead)
        def _():
            wait_in(i - lead)
            start_out(i - lead)

        return carry

    lax.fori_loop(0, count + lead, body, 0)

    def drain(i, carry):
        wait_out(i)
        return carry

    lax.fori_loop(jnp.maximum(count - depth, 0), count, drain, 0)


def compact(total, flag, value, listed):
    def body(i, count):
        @pl.when(flag(i))
        def _():
            listed[count] = value(i)

        return count + flag(i).astype(jnp.int32)

    return lax.fori_loop(0, total, body, jnp.int32(0))


def pack_kernel(depth, lead, plan, slot_ref, *rest):
    pools = rest[:2]
    outs = rest[2:-4]
    buf, listed, sems_in, sems_out = rest[-4:]
    peers = outs[0].shape[0]
    for r, halves in plan:
        mine, outs = outs[0], outs[1:]
        count = compact(peers, lambda i: slot_ref[r * peers + i] >= 0, lambda i: i, listed)

        def ins(i):
            at = lax.rem(i, depth)
            slot = slot_ref[r * peers + listed[i]]
            return [pltpu.make_async_copy(pools[h].at[slot], buf.at[at, h], sems_in.at[at, h]) for h in halves]

        def puts(i):
            at = lax.rem(i, depth)
            return [pltpu.make_async_copy(buf.at[at, h], mine.at[listed[i], k], sems_out.at[at, h]) for k, h in enumerate(halves)]

        ring(
            count, depth, lead,
            lambda i: [c.start() for c in ins(i)],
            lambda i: [c.wait() for c in ins(i)],
            lambda i: [c.start() for c in puts(i)],
            lambda i: [c.wait() for c in puts(i)],
        )


def pack_pages(plan, send_slot, k_pool, v_pool, peers):
    page = k_pool.shape[1:]
    depth, lead = 24, 12
    total = sum(len(halves) for _, halves in plan)
    return pl.pallas_call(
        functools.partial(pack_kernel, depth, lead, plan),
        out_shape=[jax.ShapeDtypeStruct((peers, len(halves)) + page, k_pool.dtype) for _, halves in plan],
        in_specs=[SMEM, ANY, ANY],
        out_specs=[ANY] * len(plan),
        scratch_shapes=[
            pltpu.VMEM((depth, 2) + page, k_pool.dtype),
            pltpu.SMEM((peers,), jnp.int32),
            pltpu.SemaphoreType.DMA((depth, 2)),
            pltpu.SemaphoreType.DMA((depth, 2)),
        ],
        cost_estimate=pl.CostEstimate(flops=10 ** 6, bytes_accessed=2 ** 21 * total, transcendentals=0),
        name="pack_pages",
    )(send_slot, k_pool, v_pool)


def keep_kernel(depth, lead, from_ref, k_ref, v_ref, k_out, v_out, buf, listed, sems_in, sems_out):
    count = compact(from_ref.shape[0], lambda i: from_ref[i] < 0, lambda i: i, listed)

    def ins(i):
        at = lax.rem(i, depth)
        return [pltpu.make_async_copy(ref.at[listed[i]], buf.at[at, h], sems_in.at[at, h]) for h, ref in enumerate((k_ref, v_ref))]

    def outs(i):
        at = lax.rem(i, depth)
        return [pltpu.make_async_copy(buf.at[at, h], ref.at[listed[i]], sems_out.at[at, h]) for h, ref in enumerate((k_out, v_out))]

    ring(
        count, depth, lead,
        lambda i: [c.start() for c in ins(i)],
        lambda i: [c.wait() for c in ins(i)],
        lambda i: [c.start() for c in outs(i)],
        lambda i: [c.wait() for c in outs(i)],
    )


def keep_pages(from_page, k_pool, v_pool):
    depth, lead = 24, 12
    return pl.pallas_call(
        functools.partial(keep_kernel, depth, lead),
        out_shape=[jax.ShapeDtypeStruct(k_pool.shape, k_pool.dtype)] * 2,
        in_specs=[SMEM] + [ANY] * 2,
        out_specs=[ANY] * 2,
        scratch_shapes=[
            pltpu.VMEM((depth, 2) + k_pool.shape[1:], k_pool.dtype),
            pltpu.SMEM((k_pool.shape[0],), jnp.int32),
            pltpu.SemaphoreType.DMA((depth, 2)),
            pltpu.SemaphoreType.DMA((depth, 2)),
        ],
        cost_estimate=pl.CostEstimate(flops=10 ** 6, bytes_accessed=2 ** 25, transcendentals=0),
        name="keep_pages",
    )(from_page, k_pool, v_pool)


def place_kernel(depth, lead, plan, from_ref, *rest):
    arrived, rest = rest[:len(plan)], rest[len(plan):]
    k_out, v_out, buf, listed, sems_in, sems_out = rest[2:]
    pools = (k_out, v_out)
    peers = arrived[0].shape[0]
    slots = from_ref.shape[0]
    for part, (r, halves) in enumerate(plan):
        count = compact(slots, lambda i: (from_ref[i] >= r * peers) & (from_ref[i] < (r + 1) * peers), lambda i: i, listed)

        def ins(i):
            at = lax.rem(i, depth)
            line = from_ref[listed[i]] - r * peers
            return [pltpu.make_async_copy(arrived[part].at[line, k], buf.at[at, h], sems_in.at[at, h]) for k, h in enumerate(halves)]

        def outs(i):
            at = lax.rem(i, depth)
            return [pltpu.make_async_copy(buf.at[at, h], pools[h].at[listed[i]], sems_out.at[at, h]) for h in halves]

        ring(
            count, depth, lead,
            lambda i: [c.start() for c in ins(i)],
            lambda i: [c.wait() for c in ins(i)],
            lambda i: [c.start() for c in outs(i)],
            lambda i: [c.wait() for c in outs(i)],
        )


def place_pages(plan, from_page, arrived, k_out, v_out):
    depth, lead = 24, 12
    return pl.pallas_call(
        functools.partial(place_kernel, depth, lead, plan),
        out_shape=[jax.ShapeDtypeStruct(k_out.shape, k_out.dtype)] * 2,
        in_specs=[SMEM] + [ANY] * (len(arrived) + 2),
        out_specs=[ANY] * 2,
        scratch_shapes=[
            pltpu.VMEM((depth, 2) + k_out.shape[1:], k_out.dtype),
            pltpu.SMEM((k_out.shape[0],), jnp.int32),
            pltpu.SemaphoreType.DMA((depth, 2)),
            pltpu.SemaphoreType.DMA((depth, 2)),
        ],
        input_output_aliases={1 + len(arrived): 0, 2 + len(arrived): 1},
        cost_estimate=pl.CostEstimate(flops=10 ** 6, bytes_accessed=2 ** 22 * len(arrived), transcendentals=0),
        name="place_pages",
    )(from_page, *arrived, k_out, v_out)


def close_kernel(seq_dev, first_line, n_layers, from_ref, first_ref, second_ref, offset_ref, k_came, v_came, *rest):
    rows = rest[:2 * n_layers]
    k_out, v_out, buf, listed, staged, early, late, sems_in, sem_out, sem_row = rest[2 * n_layers + 2:]
    pools, arrived = (k_out, v_out), (k_came, v_came)
    peers = k_came.shape[0]
    slots, n_batch = from_ref.shape[0], offset_ref.shape[0]
    heads = k_out.shape[3]
    most = early.shape[0]

    def ins(i, line):
        return [pltpu.make_async_copy(ref.at[line], buf.at[i, h], sems_in.at[i]) for h, ref in enumerate(arrived)]

    def outs(i, slot):
        return [pltpu.make_async_copy(buf.at[i, h], pools[h].at[slot], sem_out.at[0]) for h in range(2)]

    def fetch(at, seq, step):
        home, place = seq // seq_dev, lax.rem(seq, seq_dev)
        return [
            pltpu.make_async_copy(
                rows[2 * layer + h].at[lax.rem(home, 2), home // 2, place, pl.ds(step * heads, heads)], staged.at[at, layer, h], sem_row.at[0]
            )
            for layer in range(n_layers) for h in range(2)
        ]

    def write(at, slot, layer_offset, sem):
        return [
            pltpu.make_async_copy(staged.at[at, layer, h], pools[h].at[slot, layer, layer_offset], sem_row.at[sem])
            for layer in range(n_layers) for h in range(2)
        ]

    def scan(slot, counts):
        pages, n_early, n_late = counts
        line = from_ref[slot] - first_line
        moved = (line >= 0) & (line < peers)

        @pl.when(moved)
        def _():
            listed[pages] = slot
            for c in ins(pages, line):
                c.start()

        for step, ref in enumerate((first_ref, second_ref)):
            seq = ref[slot]
            entry = (slot * 2 + step) * n_batch + seq

            @pl.when((seq >= 0) & moved)
            def _():
                late[n_late] = entry
                for c in fetch(most - 1 - n_late, seq, step):
                    c.start()

            @pl.when((seq >= 0) & jnp.logical_not(moved))
            def _():
                early[n_early] = entry
                for c in fetch(n_early, seq, step):
                    c.start()

            n_late = n_late + ((seq >= 0) & moved).astype(jnp.int32)
            n_early = n_early + ((seq >= 0) & jnp.logical_not(moved)).astype(jnp.int32)
        return pages + moved.astype(jnp.int32), n_early, n_late

    pages, n_early, n_late = lax.fori_loop(0, slots, scan, (jnp.int32(0), jnp.int32(0), jnp.int32(0)))

    def pass_on(i, carry):
        for c in ins(i, 0):
            c.wait()
        for c in outs(i, listed[i]):
            c.start()
        return carry

    lax.fori_loop(0, pages, pass_on, 0)

    def fetched(i, carry):
        for c in fetch(0, 0, 0):
            c.wait()
        return carry

    lax.fori_loop(0, n_early + n_late, fetched, 0)

    def write_row(entries, at, sem):
        def body(i, carry):
            entry = entries[i]
            seq, where = lax.rem(entry, n_batch), entry // n_batch
            for c in write(at(i), where // 2, offset_ref[seq] + lax.rem(where, 2), sem):
                c.start()
            return carry
        return body

    lax.fori_loop(0, n_early, write_row(early, lambda i: i, 1), 0)

    def placed(i, carry):
        for c in outs(i, 0):
            c.wait()
        return carry

    lax.fori_loop(0, pages, placed, 0)
    lax.fori_loop(0, n_late, write_row(late, lambda i: most - 1 - i, 1), 0)

    def written(i, carry):
        for c in write(0, 0, 0, 1):
            c.wait()
        return carry

    lax.fori_loop(0, n_early + n_late, written, 0)


def close_pools(seq_dev, last_round, from_page, first_seq, second_seq, offsets, arrived, rows, k_out, v_out):
    peers, slots = arrived[0].shape[0], k_out.shape[0]
    first_pool = 6 + len(rows)
    return pl.pallas_call(
        functools.partial(close_kernel, seq_dev, last_round * peers, len(rows) // 2),
        out_shape=[jax.ShapeDtypeStruct(k_out.shape, k_out.dtype)] * 2,
        in_specs=[SMEM] * 4 + [ANY] * (4 + len(rows)),
        out_specs=[ANY] * 2,
        scratch_shapes=[
            pltpu.VMEM((peers, 2) + k_out.shape[1:], k_out.dtype),
            pltpu.SMEM((peers,), jnp.int32),
            pltpu.VMEM((2 * slots, len(rows) // 2, 2) + k_out.shape[3:], k_out.dtype),
            pltpu.SMEM((2 * slots,), jnp.int32),
            pltpu.SMEM((2 * slots,), jnp.int32),
            pltpu.SemaphoreType.DMA((peers,)),
            pltpu.SemaphoreType.DMA((1,)),
            pltpu.SemaphoreType.DMA((2,)),
        ],
        input_output_aliases={first_pool: 0, first_pool + 1: 1},
        cost_estimate=pl.CostEstimate(flops=10 ** 6, bytes_accessed=2 ** 23, transcendentals=0),
        name="close_pools",
    )(from_page, first_seq, second_seq, offsets, *[a.reshape((peers,) + a.shape[2:]) for a in arrived], *rows, k_out, v_out)


def attend_kernel(block, pages_seq, seq_dev, page_size, scale, code_ref, q_ref, k_ref, v_ref, acc_ref):
    rows, head_dim = q_ref.shape[-2:]
    heads = k_ref.shape[3]
    chips = acc_ref.shape[1]
    step = pl.program_id(0)

    @pl.when(step == 0)
    def _():
        for core in range(2):
            acc_ref[core, :, :seq_dev] = jnp.zeros((chips, seq_dev, rows, head_dim), jnp.float32)
            lane = lax.broadcasted_iota(jnp.int32, (chips, 1, rows, head_dim), 3)
            acc_ref[core, :, seq_dev:] = jnp.where(lax.rem(lane, 2) == 0, LOW, 0.0)

    row = lax.broadcasted_iota(jnp.int32, (rows, page_size * heads), 0)
    column = lax.broadcasted_iota(jnp.int32, (rows, page_size * heads), 1)
    same_head = lax.rem(row, heads) == lax.rem(column, heads)
    position = jnp.where(same_head, column // heads, page_size)
    lane = lax.broadcasted_iota(jnp.int32, (rows, head_dim), 1)
    found = []
    for s in range(block):
        code = code_ref[step * block + s]
        held = jnp.maximum(code, 0)
        seen = jnp.where(code >= 0, lax.rem(held, 2 * page_size), 0)
        seq = held // (2 * page_size * pages_seq)
        home, place = seq // seq_dev, lax.rem(seq, seq_dev)
        core, chip = lax.rem(home, 2), home // 2
        q = q_ref[core, chip, place]
        keys = k_ref[s, 0].reshape(page_size * heads, head_dim)
        values = v_ref[s, 0].reshape(page_size * heads, head_dim)
        scores = lax.dot_general(q, keys, (((1,), (1,)), ((), ())), preferred_element_type=jnp.float32) * scale
        mask = position < seen
        scores = jnp.where(mask, scores, LOW)
        top = jnp.max(scores, axis=1, keepdims=True)
        weights = jnp.where(mask, jnp.exp(scores - top), 0.0)
        total = jnp.sum(weights, axis=1, keepdims=True)
        high = weights.astype(jnp.bfloat16)
        low = (weights - high.astype(jnp.float32)).astype(jnp.bfloat16)
        both = jnp.dot(jnp.concatenate([high, low], axis=0), values, preferred_element_type=jnp.float32)
        mixed = both[:rows] + both[rows:]
        found.append((core, chip, place, top, total, mixed))
    for core, chip, place, top, total, mixed in found:
        stats = acc_ref[core, chip, seq_dev]
        old_top = jnp.max(jnp.where(lane == 2 * place, stats, LOW), axis=1, keepdims=True)
        old_total = jnp.sum(jnp.where(lane == 2 * place + 1, stats, 0.0), axis=1, keepdims=True)
        new_top = jnp.maximum(top, old_top)
        old_part, new_part = jnp.exp(old_top - new_top), jnp.exp(top - new_top)
        acc_ref[core, chip, place] = acc_ref[core, chip, place] * old_part + mixed * new_part
        new_total = old_total * old_part + total * new_part
        acc_ref[core, chip, seq_dev] = jnp.where(lane == 2 * place, new_top, jnp.where(lane == 2 * place + 1, new_total, stats))


def attend_pages(code, q_all, k_pool, v_pool, layer, pages_seq):
    slots, _, page_size, heads, head_dim = k_pool.shape
    cores, chips, seq_dev, rows, _ = q_all.shape
    block = 8
    page_spec = pl.BlockSpec((block, 1, page_size, heads, head_dim), lambda i, c: (i, layer, 0, 0, 0))
    query_spec = pl.BlockSpec(q_all.shape, lambda i, c: (0,) * 5)
    acc_shape = (cores, chips, seq_dev + 1, rows, head_dim)
    return pl.pallas_call(
        functools.partial(attend_kernel, block, pages_seq, seq_dev, page_size, head_dim ** -0.5),
        out_shape=jax.ShapeDtypeStruct(acc_shape, jnp.float32),
        grid_spec=pltpu.PrefetchScalarGridSpec(
            num_scalar_prefetch=1,
            grid=(slots // block,),
            in_specs=[query_spec, page_spec, page_spec],
            out_specs=pl.BlockSpec(acc_shape, lambda i, c: (0,) * 5),
        ),
        compiler_params=pltpu.CompilerParams(dimension_semantics=("arbitrary",)),
        cost_estimate=pl.CostEstimate(flops=10 ** 6, bytes_accessed=2 * slots * page_size * heads * head_dim * 2, transcendentals=0),
        name="attend_pages",
    )(code, q_all, k_pool, v_pool)


def spread_kernel(n, x_ref, out_ref, held, send_sem, recv_sem, pass_sem, got_sem, copy_sem):
    me = lax.axis_index("kv")
    chips = n // 2
    core, chip = lax.rem(me, 2), me // 2
    barrier = pltpu.get_barrier_semaphore()

    def greet(j, carry):
        pl.semaphore_signal(barrier, inc=1, device_id={"kv": 2 * lax.rem(chip + j, chips) + core}, device_id_type=MESH)
        return carry

    lax.fori_loop(1, chips, greet, 0)
    pl.semaphore_signal(barrier, inc=1, device_id={"kv": me + 1 - 2 * core}, device_id_type=MESH)
    pl.semaphore_wait(barrier, chips)
    spread_body(n, x_ref, out_ref, held, send_sem, recv_sem, pass_sem, got_sem, copy_sem)


def spread_body(n, x_ref, out_ref, held, send_sem, recv_sem, pass_sem, got_sem, copy_sem, behind=lambda: None):
    me = lax.axis_index("kv")
    chips = n // 2
    core, chip = lax.rem(me, 2), me // 2
    other = me + 1 - 2 * core

    def peer(j):
        return 2 * lax.rem(chip + j, chips) + core

    def send(j):
        return pltpu.make_async_remote_copy(
            src_ref=x_ref, dst_ref=held.at[core, chip], send_sem=send_sem.at[j], recv_sem=recv_sem.at[chip],
            device_id={"kv": peer(j)}, device_id_type=MESH,
        )

    def forward(source, at):
        return pltpu.make_async_remote_copy(
            src_ref=source, dst_ref=held.at[core, at], send_sem=pass_sem.at[at], recv_sem=got_sem.at[at],
            device_id={"kv": other}, device_id_type=MESH,
        )

    offsets, side = chip_offsets(chips)
    for offset in offsets:
        send(lax.rem(chip_at(chip, offset, side, chips) + chips - chip, chips)).start()
    own = forward(x_ref, chip)
    own.start()
    mine = pltpu.make_async_copy(x_ref, out_ref.at[core, chip], copy_sem.at[0])
    mine.start()
    behind()

    for offset in offsets:
        at = chip_from(chip, offset, side, chips)
        j = lax.rem(chip + chips - at, chips)
        pltpu.make_async_remote_copy(
            src_ref=x_ref, dst_ref=held.at[core, at], send_sem=send_sem.at[j], recv_sem=recv_sem.at[at],
            device_id={"kv": other}, device_id_type=MESH,
        ).wait_recv()
        forward(held.at[core, at], at).start()
        pltpu.make_async_copy(held.at[core, at], out_ref.at[core, at], copy_sem.at[j]).start()

    def passed(j, carry):
        at = lax.rem(chip + j, chips)
        pltpu.make_async_remote_copy(
            src_ref=x_ref, dst_ref=held.at[1 - core, at], send_sem=pass_sem.at[at], recv_sem=got_sem.at[at],
            device_id={"kv": other}, device_id_type=MESH,
        ).wait_recv()
        pltpu.make_async_copy(held.at[1 - core, at], out_ref.at[1 - core, at], copy_sem.at[chips + j]).start()
        return carry

    lax.fori_loop(0, chips, passed, 0)

    own.wait_send()
    mine.wait()

    def finish(j, carry):
        at = lax.rem(chip + chips - j, chips)
        send(j).wait_send()
        forward(held.at[core, at], at).wait_send()
        pltpu.make_async_copy(held.at[core, at], out_ref.at[core, at], copy_sem.at[j]).wait()
        return carry

    lax.fori_loop(1, chips, finish, 0)

    def written(j, carry):
        at = lax.rem(chip + j, chips)
        pltpu.make_async_copy(held.at[1 - core, at], out_ref.at[1 - core, at], copy_sem.at[chips + j]).wait()
        return carry

    lax.fori_loop(0, chips, written, 0)


def spread(x, n):
    chips = n // 2
    return pl.pallas_call(
        functools.partial(spread_kernel, n),
        out_shape=jax.ShapeDtypeStruct((2, chips) + x.shape, x.dtype),
        in_specs=[VMEM],
        out_specs=ANY,
        scratch_shapes=[
            pltpu.VMEM((2, chips) + x.shape, x.dtype),
            pltpu.SemaphoreType.DMA((chips,)),
            pltpu.SemaphoreType.DMA((chips,)),
            pltpu.SemaphoreType.DMA((chips,)),
            pltpu.SemaphoreType.DMA((chips,)),
            pltpu.SemaphoreType.DMA((n,)),
        ],
        compiler_params=pltpu.CompilerParams(collective_id=0, has_side_effects=True),
        name="spread_rows",
    )(x)


def pack_stats(x):
    parts = x.shape[0] // 8
    span = x.shape[1] // parts
    lane = lax.broadcasted_iota(jnp.int32, (8, x.shape[1]), 1)
    out = x[:8]
    for g in range(1, parts):
        out = jnp.where(lane // span == g, pltpu.roll(x[8 * g:8 * g + 8], span * g, 1), out)
    return out


def unpack_stats(x, rows):
    span = x.shape[1] // (rows // 8)
    return jnp.concatenate([x] + [pltpu.roll(x, x.shape[1] - span * g, 1) for g in range(1, rows // 8)], axis=0)


def lane_before(x):
    return pltpu.roll(x, x.shape[1] - 1, 1)


def merge_chip_kernel(acc_ref, sums_ref, near, send_sem, recv_sem):
    me = lax.axis_index("kv")
    core = lax.rem(me, 2)
    other = me + 1 - 2 * core
    chips, blocks, rows, head_dim = near.shape
    seq_dev = blocks - 1

    barrier = pltpu.get_barrier_semaphore()
    pl.semaphore_signal(barrier, inc=1, device_id={"kv": other}, device_id_type=MESH)
    pl.semaphore_wait(barrier, 1)

    swap = pltpu.make_async_remote_copy(
        src_ref=acc_ref.at[1 - core], dst_ref=near, send_sem=send_sem.at[0], recv_sem=recv_sem.at[0],
        device_id={"kv": other}, device_id_type=MESH,
    )
    swap.start()
    even = lax.rem(lax.broadcasted_iota(jnp.int32, (rows, head_dim), 1), 2) == 0
    swap.wait_recv()

    def merge(at, carry):
        mine, theirs = acc_ref[core, at, seq_dev], near[at, seq_dev]
        top = jnp.maximum(mine, theirs)
        a, b = jnp.exp(mine - top), jnp.exp(theirs - top)
        total = a * lane_before(mine) + b * lane_before(theirs)
        sums_ref[at, seq_dev * rows:] = pack_stats(jnp.where(even, top, pltpu.roll(total, 1, 1)))
        for i in range(seq_dev):
            sums_ref[at, i * rows:(i + 1) * rows] = a[:, 2 * i:2 * i + 1] * acc_ref[core, at, i] + b[:, 2 * i:2 * i + 1] * near[at, i]
        return carry

    lax.fori_loop(0, chips, merge, 0)
    swap.wait_send()


def merge_chip(acc):
    blocks = acc.shape[1:]
    return pl.pallas_call(
        merge_chip_kernel,
        out_shape=jax.ShapeDtypeStruct((blocks[0], (blocks[1] - 1) * blocks[2] + 8, blocks[3]), acc.dtype),
        in_specs=[VMEM],
        out_specs=VMEM,
        scratch_shapes=[
            pltpu.VMEM(blocks, acc.dtype),
            pltpu.SemaphoreType.DMA((1,)),
            pltpu.SemaphoreType.DMA((1,)),
        ],
        compiler_params=pltpu.CompilerParams(collective_id=2, has_side_effects=True),
        cost_estimate=pl.CostEstimate(flops=10 ** 6, bytes_accessed=2 ** 23, transcendentals=0),
        name="merge_chip",
    )(acc)


def layer_kernel(n, scale, layer, follow, *refs):
    sums_ref, x_ref, hid_ref, chunk_ref, wo_ref, wu_ref, wd_ref = refs[:7]
    refs = refs[7:]
    hid_out, got_ref = refs[:2]
    refs = refs[2:]
    if follow:
        all_out, refs = refs[0], refs[1:]
    held, o_scr, rows_scr, mid_scr, acc_scr, wide, up, down, wide_sem, up_sem, down_sem, send_sem, recv_sem, page_send, page_recv = refs[:15]
    refs = refs[15:]
    me = lax.axis_index("kv")
    _, seq_dev, rows, head_dim = x_ref.shape
    heads = rows // 2
    chips = n // 2
    core, chip = lax.rem(me, 2), me // 2
    hid_rows, width = hid_ref.shape
    tile, up_tile = wide.shape[2], up.shape[2]
    up_slots = up.shape[0]
    n_wide, n_up = width // tile, wu_ref.shape[2] // up_tile

    def peer(j):
        return 2 * lax.rem(chip + j, chips) + core

    def anyone(j):
        return lax.rem(me + j, n)

    barrier = pltpu.get_barrier_semaphore()

    def greet(j, carry):
        pl.semaphore_signal(barrier, inc=1, device_id={"kv": anyone(j)}, device_id_type=MESH)
        return carry

    lax.fori_loop(1, n, greet, 0)

    def wide_copy(w, at, t, slot):
        return pltpu.make_async_copy(w.at[at, :, pl.ds(pl.multiple_of(t * tile, tile), tile)], wide.at[slot], wide_sem.at[slot])

    def up_copy(t):
        slot = lax.rem(t, up_slots)
        return pltpu.make_async_copy(wu_ref.at[layer, :, pl.ds(pl.multiple_of(t * up_tile, up_tile), up_tile)], up.at[slot], up_sem.at[slot])

    def down_copy(t):
        slot = lax.rem(t, up_slots)
        return pltpu.make_async_copy(wd_ref.at[layer, pl.ds(pl.multiple_of(t * up_tile, up_tile), up_tile)], down.at[slot], down_sem.at[slot])

    for t in range(n_wide):
        wide_copy(wo_ref, layer, t, t).start()
    for t in range(up_slots):
        up_copy(t).start()
        down_copy(t).start()
    pl.semaphore_wait(barrier, n - 1)

    def send(j):
        return pltpu.make_async_remote_copy(
            src_ref=sums_ref.at[lax.rem(chip + j, chips)], dst_ref=held.at[chip], send_sem=send_sem.at[j], recv_sem=recv_sem.at[chip],
            device_id={"kv": peer(j)}, device_id_type=MESH,
        )

    def send_pages(j):
        return pltpu.make_async_remote_copy(
            src_ref=chunk_ref.at[anyone(j)], dst_ref=got_ref.at[me], send_sem=page_send.at[j], recv_sem=page_recv.at[me],
            device_id={"kv": anyone(j)}, device_id_type=MESH,
        )

    offsets, side = chip_offsets(chips)
    for offset in offsets:
        send(lax.rem(chip_at(chip, offset, side, chips) + chips - chip, chips)).start()
    def send_chunk(some):
        for offset in some:
            for other_core in range(2):
                to = 2 * chip_at(chip, offset, side, chips) + lax.rem(core + other_core, 2)
                send_pages(lax.rem(to + n - me, n)).start()

    at_once = 3 * len(offsets) // 5 if follow else len(offsets)
    send_chunk(offsets[:at_once])
    send_pages(lax.rem(me + 1 - 2 * core + n - me, n)).start()
    held[chip] = sums_ref[chip]

    queries = [x_ref[0, i].astype(jnp.float32) for i in range(seq_dev)]
    second_row = lax.broadcasted_iota(jnp.int32, (rows, 1), 0) >= heads

    def twice(h, i, step):
        x = x_ref[1 + h, i, step * heads:(step + 1) * heads].astype(jnp.float32)
        return jnp.concatenate([x, x], axis=0)

    first = [jnp.sum(queries[i] * twice(0, i, 0), axis=1, keepdims=True) * scale for i in range(seq_dev)]
    second = [
        jnp.where(second_row, jnp.sum(queries[i] * twice(0, i, 1), axis=1, keepdims=True) * scale, LOW)
        for i in range(seq_dev)
    ]

    def arrive(j, carry):
        at = lax.rem(chip + chips - j, chips)
        pltpu.make_async_remote_copy(
            src_ref=sums_ref.at[at], dst_ref=held.at[at], send_sem=send_sem.at[j], recv_sem=recv_sem.at[at],
            device_id={"kv": peer(j)}, device_id_type=MESH,
        ).wait_recv()
        return carry

    lax.fori_loop(1, chips, arrive, 0)

    def highest(j, top):
        return jnp.maximum(top, held[j, seq_dev * rows:])

    top_all = unpack_stats(lax.fori_loop(0, chips, highest, jnp.full((8, head_dim), LOW, jnp.float32)), rows)
    tops, totals, mixed = [], [], []
    for i in range(seq_dev):
        top = jnp.maximum(jnp.maximum(top_all[:, 2 * i:2 * i + 1], first[i]), second[i])
        p_first, p_second = jnp.exp(first[i] - top), jnp.exp(second[i] - top)
        tops.append(top)
        totals.append(p_first + p_second)
        mixed.append(p_first * twice(1, i, 0) + p_second * twice(1, i, 1))

    def merge(j, carry):
        totals, mixed = carry
        stats = unpack_stats(held[j, seq_dev * rows:], rows)
        new_totals, new_mixed = [], []
        for i in range(seq_dev):
            weight = jnp.exp(stats[:, 2 * i:2 * i + 1] - tops[i])
            new_totals.append(totals[i] + weight * stats[:, 2 * i + 1:2 * i + 2])
            new_mixed.append(mixed[i] + weight * held[j, i * rows:(i + 1) * rows])
        return tuple(new_totals), tuple(new_mixed)

    totals, mixed = lax.fori_loop(0, chips, merge, (tuple(totals), tuple(mixed)))
    for i in range(seq_dev):
        o_scr[i * rows:(i + 1) * rows] = (mixed[i] / totals[i]).astype(jnp.bfloat16).astype(jnp.float32)
    for h in range(heads):
        rows_scr[:, h * head_dim:(h + 1) * head_dim] = o_scr[pl.ds(h, hid_rows, stride=heads), :].astype(jnp.bfloat16)

    def add_out(t, carry):
        wide_copy(wo_ref, layer, t, t).wait()
        cut = pl.ds(pl.multiple_of(t * tile, tile), tile)
        part = jnp.dot(rows_scr[...], wide[t], preferred_element_type=jnp.float32)
        mid_scr[:, cut] = (hid_ref[:, cut].astype(jnp.float32) + part).astype(jnp.bfloat16)
        return carry

    lax.fori_loop(0, n_wide, add_out, 0)
    acc_scr[...] = jnp.zeros_like(acc_scr)

    def mlp(t, carry):
        slot = lax.rem(t, up_slots)
        up_copy(t).wait()
        inner = jax.nn.gelu(jnp.dot(mid_scr[...], up[slot], preferred_element_type=jnp.float32)).astype(jnp.bfloat16)
        down_copy(t).wait()
        acc_scr[...] += jnp.dot(inner, down[slot], preferred_element_type=jnp.float32)

        @pl.when(t + up_slots < n_up)
        def _():
            up_copy(t + up_slots).start()
            down_copy(t + up_slots).start()

        return carry

    lax.fori_loop(0, n_up, mlp, 0)
    hid_out[...] = (mid_scr[...].astype(jnp.float32) + acc_scr[...]).astype(jnp.bfloat16)

    def finish(j, carry):
        send(j).wait_send()
        return carry

    lax.fori_loop(1, chips, finish, 0)
    if follow:
        all_held, pass_send, pass_recv, spread_send, spread_recv, copy_sem = refs
        spread_body(
            n, hid_out, all_out, all_held, spread_send, spread_recv, pass_send, pass_recv, copy_sem, lambda: send_chunk(offsets[at_once:])
        )

    def pages_came(j, carry):
        at = lax.rem(me + n - j, n)
        pltpu.make_async_remote_copy(
            src_ref=chunk_ref.at[at], dst_ref=got_ref.at[at], send_sem=page_send.at[j], recv_sem=page_recv.at[at],
            device_id={"kv": anyone(j)}, device_id_type=MESH,
        ).wait_recv()
        send_pages(j).wait_send()
        return carry

    lax.fori_loop(1, n, pages_came, 0)


def end_layer(sums, x, hidden, chunk, w_out, w_up, w_down, layer, follow, n):
    chips = n // 2
    hid_rows, width = hidden.shape
    seq_dev, rows, head_dim = x.shape[1:]
    tile, up_slots = 512, 3
    wide_slots = width // tile
    out_shape = [jax.ShapeDtypeStruct(hidden.shape, hidden.dtype), jax.ShapeDtypeStruct(chunk.shape, chunk.dtype)]
    out_specs = [VMEM, ANY]
    scratch = [
        pltpu.VMEM(sums.shape, sums.dtype),
        pltpu.VMEM((seq_dev * rows, head_dim), jnp.float32),
        pltpu.VMEM(hidden.shape, jnp.bfloat16),
        pltpu.VMEM(hidden.shape, jnp.bfloat16),
        pltpu.VMEM(hidden.shape, jnp.float32),
        pltpu.VMEM((wide_slots, width, tile), w_out.dtype),
        pltpu.VMEM((up_slots, width, tile), w_up.dtype),
        pltpu.VMEM((up_slots, tile, width), w_down.dtype),
        pltpu.SemaphoreType.DMA((wide_slots,)),
        pltpu.SemaphoreType.DMA((up_slots,)),
        pltpu.SemaphoreType.DMA((up_slots,)),
        pltpu.SemaphoreType.DMA((chips,)),
        pltpu.SemaphoreType.DMA((chips,)),
        pltpu.SemaphoreType.DMA((n,)),
        pltpu.SemaphoreType.DMA((n,)),
    ]
    if follow:
        spread_shape = (2, chips) + hidden.shape
        out_shape += [jax.ShapeDtypeStruct(spread_shape, hidden.dtype)]
        out_specs += [ANY]
        scratch += [pltpu.VMEM(spread_shape, hidden.dtype)]
        scratch += [pltpu.SemaphoreType.DMA((chips,))] * 4 + [pltpu.SemaphoreType.DMA((n,))]
    return pl.pallas_call(
        functools.partial(layer_kernel, n, head_dim ** -0.5, layer, follow),
        out_shape=out_shape,
        in_specs=[VMEM] * 3 + [ANY] * 4,
        out_specs=out_specs,
        scratch_shapes=scratch,
        compiler_params=pltpu.CompilerParams(collective_id=3 + layer, has_side_effects=True),
        cost_estimate=pl.CostEstimate(flops=10 ** 10, bytes_accessed=2 ** 27, transcendentals=0),
        name="end_layer",
    )(sums, x, hidden, chunk, w_out, w_up, w_down)


def solution(mesh):
    groups = mesh.shape['kv']
    rows_spec = P(None, ('rep', 'kv'), None)
    pool_spec = P(('rep', 'kv'))
    table_spec = P('rep', None)
    vec_spec = P('rep')
    full_spec = P()

    def device_fn(embeds, w_query, w_key, w_value, w_out, w_up, w_down, k_pool, v_pool, old_table, new_table, seq_len, finished, mig_src, mig_dst):
        me = lax.axis_index('kv')
        slots, n_layers, page_size, heads, head_dim = k_pool.shape
        steps, seq_dev, width = embeds.shape
        n_batch, pages_seq = old_table.shape
        n_mig = mig_src.shape[0]
        rounds = 4 * n_mig // (groups * groups)
        base = me * slots
        local = jnp.arange(slots, dtype=jnp.int32)
        active = finished == 0
        last = pages_seq - 1

        def find(match, value):
            return jnp.max(jnp.where(match, value, -1), axis=1)

        flat = old_table.reshape(-1)
        place = jnp.arange(n_batch * pages_seq, dtype=jnp.int32)
        seen = jnp.clip(seq_len[:, None] - jnp.arange(pages_seq, dtype=jnp.int32)[None, :] * page_size, 0, page_size).reshape(-1)
        code = find(flat[None, :] - base == local[:, None], (place * (2 * page_size) + seen)[None, :])

        src_dev, dst_dev = mig_src // slots, mig_dst // slots
        pair = src_dev * groups + dst_dev
        entry = jnp.arange(n_mig, dtype=jnp.int32)
        rank = jnp.sum((pair[None, :] == pair[:, None]) & (entry[None, :] < entry[:, None]), axis=1, dtype=jnp.int32)
        lines = jnp.arange(rounds * groups, dtype=jnp.int32)
        send_slot = find(
            ((rank * groups + dst_dev)[None, :] == lines[:, None]) & (src_dev == me)[None, :], (mig_src - src_dev * slots)[None, :]
        )
        from_page = find((mig_dst - base)[None, :] == local[:, None], (rank * groups + src_dev)[None, :])

        seq_ids = jnp.arange(n_batch, dtype=jnp.int32)
        owner_old = find((old_table[:, last] - base)[None, :] == local[:, None], seq_ids[None, :])
        owner_new = find(((new_table[:, last] - base)[None, :] == local[:, None]) & active[None, :], seq_ids[None, :])
        first_seq = jnp.where(from_page >= 0, owner_new, owner_old)
        second_seq = owner_new
        offsets = lax.rem(seq_len, page_size)

        def exchange(block):
            return lax.all_to_all(block, 'kv', 0, 0, tiled=True)

        def send_next(value, count):
            for block in packed[len(got):len(got) + count]:
                block, value = lax.optimization_barrier((block, value))
                got.append(exchange(block))
            return value

        plan = tuple((r, (0, 1)) for r in range(rounds - 1)) + ((rounds - 1, (0,)), (rounds - 1, (1,)))
        packed = list(pack_pages(plan[:1], send_slot, k_pool, v_pool, groups))
        packed[0], send_slot = lax.optimization_barrier((packed[0], send_slot))
        packed += list(pack_pages(plan[1:], send_slot, k_pool, v_pool, groups))
        got = []
        tables = (from_page, first_seq, second_seq, offsets)
        k_out, v_out = keep_pages(from_page, k_pool, v_pool)

        hidden = jnp.transpose(embeds, (1, 0, 2)).reshape(seq_dev * steps, width)
        every = spread(hidden, groups)
        rows = []
        for layer in range(n_layers):
            every, got = lax.optimization_barrier((every, got))
            every = send_next(every, 1)
            flat_rows = every.reshape(groups * seq_dev * steps, width)
            every_x = [
                jnp.dot(flat_rows, w[layer], preferred_element_type=jnp.float32).astype(jnp.bfloat16)
                .reshape(2, groups // 2, seq_dev, steps * heads, head_dim)
                for w in (w_query, w_key, w_value)
            ]
            rows += every_x[1:]
            x = jnp.stack([y[lax.rem(me, 2), me // 2] for y in every_x])
            sums = merge_chip(attend_pages(code, every_x[0], k_pool, v_pool, layer, pages_seq))
            if layer:
                k_out, v_out = place_pages(plan[:2], from_page, got[:2], k_out, v_out)
            sums, k_out, v_out, packed = lax.optimization_barrier((sums, k_out, v_out, packed))
            hidden, pages, *ahead = end_layer(
                sums, x, hidden, packed[len(got)], w_out, w_up, w_down, layer, layer + 1 < n_layers, groups
            )
            got.append(pages)
            if ahead:
                (every,) = ahead
        k_out, v_out = close_pools(seq_dev, rounds - 1, *tables, got[2:], rows, k_out, v_out)
        hidden = jnp.transpose(hidden.reshape(seq_dev, steps, width), (1, 0, 2))
        done = lax.dynamic_slice(finished, (me * seq_dev,), (seq_dev,)) != 0
        live = jnp.stack([jnp.ones_like(done), ~done])
        hidden = jnp.where(live[:, :, None], hidden, jnp.zeros_like(hidden))
        return hidden, k_out, v_out

    in_specs = (rows_spec, full_spec, full_spec, full_spec, full_spec, full_spec, full_spec, pool_spec, pool_spec, table_spec, table_spec, vec_spec, vec_spec, vec_spec, vec_spec)
    return jax.shard_map(device_fn, mesh=mesh, in_specs=in_specs, out_specs=(rows_spec, pool_spec, pool_spec), check_vma=False)
```
